32 devices in a mesh: tm: 1, space: 32 (over z, y, x, core).
Axes of the slice: x: 2, y: 2, z: 4, core: 2. Of those that a mesh axis runs over, the one named last changes fastest.
Arguments:
- links: float32 [8, 3, 2, 3, 2, 110592], P('tm', None, None, None, None, 'space'), may hold values from -1 to 1, as said below
Outputs:
- new_links: float32 [8, 3, 2, 3, 2, 110592], P('tm', None, None, None, None, 'space')
- theta: float32 [], replicated
- deficit: float32 [8], P('tm')
The draws below stay inside these ranges and needn't reach their ends.
Inputs may be any that keep to these rules, and one draw needn't show every extreme that they name: `links`: each link's two stored rows are orthonormal complex 3-vectors, the first two rows of a special unitary matrix.
All inputs are finite; a program needn't handle non-finite values.
Results may differ from the reference program's by a relative error of at most 0.00013.
Values sent between devices are 32-bit elements; how exact they have to be, the bound alone decides.
A program may use at most 128 MiB of HBM per device.

```python
import math
import jax
import jax.numpy as jnp
from jax import lax

EXTENT = 48
SLICES = 8


def draw_links(key, part):
    sites = EXTENT ** 3
    subkeys = jax.random.split(key, 1)
    site_index = jnp.arange(sites, dtype=jnp.int32)
    row_index = (site_index // EXTENT - 1) % (EXTENT * EXTENT)
    ycoord = (row_index // EXTENT).astype(jnp.float32)
    tcoord = jnp.arange(SLICES, dtype=jnp.float32)
    strength = 0.15 + 0.35 * (0.5 * tcoord[:, None] / SLICES + 0.5 * ycoord[None, :] / EXTENT)
    full_shape = (SLICES, 3, 2, 3, 2, sites)
    noise_field = jnp.clip(0.6 * jax.random.normal(subkeys[0], full_shape, jnp.float32), -1.0, 1.0)
    unit_rows = (jnp.arange(2)[:, None] == jnp.arange(3)[None, :]).astype(jnp.float32)
    unit_rows = unit_rows[:, :, None] * jnp.array([1.0, 0.0], jnp.float32)
    raw_rows = noise_field * strength[:, None, None, None, None, :] + unit_rows[None, None, :, :, :, None]
    vector_one = raw_rows[:, :, 0]
    vector_two = raw_rows[:, :, 1]
    length = jnp.sqrt(jnp.sum(vector_one * vector_one, axis=(2, 3)))
    row_one = vector_one / length[:, :, None, None, :]
    correlation_real = jnp.sum(row_one[:, :, :, 0] * vector_two[:, :, :, 0] + row_one[:, :, :, 1] * vector_two[:, :, :, 1], axis=2)
    correlation_imag = jnp.sum(row_one[:, :, :, 0] * vector_two[:, :, :, 1] - row_one[:, :, :, 1] * vector_two[:, :, :, 0], axis=2)
    rest_real = vector_two[:, :, :, 0] - (correlation_real[:, :, None] * row_one[:, :, :, 0] - correlation_imag[:, :, None] * row_one[:, :, :, 1])
    rest_imag = vector_two[:, :, :, 1] - (correlation_real[:, :, None] * row_one[:, :, :, 1] + correlation_imag[:, :, None] * row_one[:, :, :, 0])
    row_two = jnp.stack([rest_real, rest_imag], axis=3)
    length = jnp.sqrt(jnp.sum(row_two * row_two, axis=(2, 3)))
    row_two = row_two / length[:, :, None, None, :]
    return jnp.stack([row_one, row_two], axis=2).astype(jnp.float32)


def setup_inputs(seed: int = 0) -> dict:
    splits = jax.random.split(jax.random.key(seed), 2)
    links = draw_links(jax.random.fold_in(splits[1], 71), 0)
    return dict(links=links)


root_three = math.sqrt(3.0)
step_size = 0.08
top_momentum = 12.0
storage_offset = 1

def complex_mul(p, q):
    return (p[0] * q[0] - p[1] * q[1], p[0] * q[1] + p[1] * q[0])

def complex_add(p, q):
    return (p[0] + q[0], p[1] + q[1])

def complex_sub(p, q):
    return (p[0] - q[0], p[1] - q[1])

def complex_conj(p):
    return (p[0], -p[1])

def matrix_mul(left, right):
    rows_out = []
    for i in range(len(left)):
        entries = []
        for j in range(3):
            summed = complex_mul(left[i][0], right[0][j])
            for k in (1, 2):
                summed = complex_add(summed, complex_mul(left[i][k], right[k][j]))
            entries.append(summed)
        rows_out.append(entries)
    return rows_out

def dagger_of(matrix):
    return [[complex_conj(matrix[j][i]) for j in range(3)] for i in range(3)]

def cross_conj(row_one, row_two):
    row_three = []
    for k in range(3):
        a = complex_mul(row_one[(k + 1) % 3], row_two[(k + 2) % 3])
        b = complex_mul(row_one[(k + 2) % 3], row_two[(k + 1) % 3])
        row_three.append(complex_conj(complex_sub(a, b)))
    return row_three

def full_matrix(entry_of):
    row_one = [(entry_of(0, c, 0), entry_of(0, c, 1)) for c in range(3)]
    row_two = [(entry_of(1, c, 0), entry_of(1, c, 1)) for c in range(3)]
    return [row_one, row_two, cross_conj(row_one, row_two)]

def gradient_of(current, behind):
    gradient = []
    for i in range(3):
        entries = []
        for j in range(3):
            summed = complex_sub(behind[0][i][j], current[0][i][j])
            for d in (1, 2):
                summed = complex_add(summed, complex_sub(behind[d][i][j], current[d][i][j]))
            entries.append(summed)
        gradient.append(entries)
    return gradient

def algebra_of(gradient):
    g = gradient
    return [g[0][1][1] + g[1][0][1], g[0][1][0] - g[1][0][0], g[0][0][1] - g[1][1][1], g[0][2][1] + g[2][0][1], g[0][2][0] - g[2][0][0], g[1][2][1] + g[2][1][1], g[1][2][0] - g[2][1][0], (g[0][0][1] + g[1][1][1] - 2.0 * g[2][2][1]) / root_three]

def rotation_of(algebra):
    half_step = 0.5 * step_size
    zeros_like = jnp.zeros_like(algebra[0])
    diag_zero = algebra[2] + algebra[7] / root_three
    diag_one = -algebra[2] + algebra[7] / root_three
    diag_two = -2.0 * algebra[7] / root_three
    hermitian = [[(diag_zero, zeros_like), (algebra[0], -algebra[1]), (algebra[3], -algebra[4])], [(algebra[0], algebra[1]), (diag_one, zeros_like), (algebra[5], -algebra[6])], [(algebra[3], algebra[4]), (algebra[5], algebra[6]), (diag_two, zeros_like)]]
    generator = [[(-half_step * h[1], half_step * h[0]) for h in row] for row in hermitian]
    square = matrix_mul(generator[:2], generator)
    rows_two = []
    for i in range(2):
        entries = []
        for j in range(3):
            real_value = generator[i][j][0] + 0.5 * square[i][j][0]
            if i == j:
                real_value = real_value + 1.0
            entries.append((real_value, generator[i][j][1] + 0.5 * square[i][j][1]))
        rows_two.append(entries)
    length = jnp.sqrt(sum((p[0] * p[0] + p[1] * p[1] for p in rows_two[0])))
    row_one = [(p[0] / length, p[1] / length) for p in rows_two[0]]
    correlation = complex_mul(complex_conj(row_one[0]), rows_two[1][0])
    for k in (1, 2):
        correlation = complex_add(correlation, complex_mul(complex_conj(row_one[k]), rows_two[1][k]))
    row_two = [complex_sub(rows_two[1][k], complex_mul(correlation, row_one[k])) for k in range(3)]
    length = jnp.sqrt(sum((p[0] * p[0] + p[1] * p[1] for p in row_two)))
    row_two = [(p[0] / length, p[1] / length) for p in row_two]
    return [row_one, row_two, cross_conj(row_one, row_two)]

def two_rows(product, axis):
    return jnp.stack([jnp.stack([jnp.stack(product[r][c], axis=axis) for c in range(3)], axis=axis) for r in range(2)], axis=axis)

def reference(links):
    extent = EXTENT
    slice_count = links.shape[0]
    wave_number = jnp.arange(extent, dtype=jnp.int32)
    wave_term = 4.0 * jnp.sin(math.pi * wave_number.astype(jnp.float32) / extent) ** 2
    momentum = wave_term[:, None, None] + wave_term[None, :, None] + wave_term[None, None, :]
    zero_mode = wave_number[:, None, None] + wave_number[None, :, None] + wave_number[None, None, :] == 0
    factor = jnp.where(zero_mode, 0.0, top_momentum / jnp.where(zero_mode, 1.0, momentum))
    roll_axes = (-1, -3, -2)

    def one_slice(slice_links):
        ordered = jnp.roll(slice_links, -storage_offset * extent, axis=-1)
        lattice = ordered.reshape(3, 2, 3, 2, extent, extent, extent)
        current = []
        behind = []
        for d in range(3):
            here = lattice[d]
            moved = jnp.roll(here, 1, axis=roll_axes[d])
            current.append(full_matrix(lambda r, c, p, arr=here: arr[r, c, p]))
            behind.append(full_matrix(lambda r, c, p, arr=moved: arr[r, c, p]))
        algebra = algebra_of(gradient_of(current, behind))
        theta_part = sum((jnp.sum(a * a) for a in algebra))
        spectrum = jnp.fft.fftn(jnp.stack(algebra), axes=(1, 2, 3))
        smooth = jnp.real(jnp.fft.ifftn(spectrum * factor, axes=(1, 2, 3))).astype(jnp.float32)
        rotation = rotation_of([smooth[a] for a in range(8)])
        new_dirs = []
        deficit_part = jnp.zeros((), jnp.float32)
        for d in range(3):
            ahead_rot = jax.tree.map(lambda a, ax=roll_axes[d]: jnp.roll(a, -1, axis=ax), rotation)
            product = matrix_mul(matrix_mul(rotation, current[d]), dagger_of(ahead_rot))
            deficit_part = deficit_part + jnp.sum(3.0 - product[0][0][0] - product[1][1][0] - product[2][2][0])
            new_dirs.append(two_rows(product, 0))
        result = jnp.stack(new_dirs).reshape(3, 2, 3, 2, extent ** 3)
        return (jnp.roll(result, storage_offset * extent, axis=-1), theta_part, deficit_part)
    new_links, thetas, deficits = lax.map(one_slice, links)
    theta = jnp.sum(thetas) / (slice_count * extent ** 3)
    deficit = deficits / extent ** 3
    return (new_links, theta, deficit)
```

```python
import functools
import math

import jax
import jax.numpy as jnp
import numpy as np
from jax import lax
from jax.experimental import pallas as pl
from jax.experimental.pallas import tpu as pltpu
from jax.sharding import PartitionSpec as P

EXTENT = 48
LANES = 128
UNITS = 3
PIECES = 6

root_three = math.sqrt(3.0)
step_size = 0.08
top_momentum = 12.0

f32 = jnp.float32
bf16 = jnp.bfloat16
MESH = pl.DeviceIdType.MESH
VM = pl.BlockSpec(memory_space=pltpu.VMEM)
PARAMS = pltpu.CompilerParams(vmem_limit_bytes=60 * 1024 * 1024)


def cmul(p, q):
    return (p[0] * q[0] - p[1] * q[1], p[0] * q[1] + p[1] * q[0])


def cadd(p, q):
    return (p[0] + q[0], p[1] + q[1])


def csub(p, q):
    return (p[0] - q[0], p[1] - q[1])


def conj(p):
    return (p[0], -p[1])


def conj_mul(p, q):
    return (p[0] * q[0] + p[1] * q[1], p[0] * q[1] - p[1] * q[0])


def mul_conj(p, q):
    return (p[0] * q[0] + p[1] * q[1], p[1] * q[0] - p[0] * q[1])


def dot_row(row, col, mul):
    out = mul(row[0], col[0])
    for k in (1, 2):
        out = cadd(out, mul(row[k], col[k]))
    return out


def cross_conj(a, b):
    return [
        conj(csub(cmul(a[(k + 1) % 3], b[(k + 2) % 3]), cmul(a[(k + 2) % 3], b[(k + 1) % 3])))
        for k in range(3)
    ]


def algebra_of(u):
    return [
        u[0][1][1] + u[1][0][1],
        u[0][1][0] - u[1][0][0],
        u[0][0][1] - u[1][1][1],
        u[0][2][1] + u[2][0][1],
        u[0][2][0] - u[2][0][0],
        u[1][2][1] + u[2][1][1],
        u[1][2][0] - u[2][1][0],
        (u[0][0][1] + u[1][1][1] - 2.0 * u[2][2][1]) * (1.0 / root_three),
    ]


def rotation_of(s):
    h = 0.5 * step_size
    s = [v * h for v in s]
    third = s[7] * (1.0 / root_three)
    d0, d1, d2 = s[2] + third, third - s[2], -2.0 * third
    herm = [
        [(d0, None), (s[0], -s[1]), (s[3], -s[4])],
        [(s[0], s[1]), (d1, None), (s[5], -s[6])],
        [(s[3], s[4]), (s[5], s[6]), (d2, None)],
    ]

    def mul(p, q):
        if p[1] is None and q[1] is None:
            return (p[0] * q[0], jnp.zeros_like(p[0]))
        if p[1] is None:
            return (p[0] * q[0], p[0] * q[1])
        if q[1] is None:
            return (p[0] * q[0], p[1] * q[0])
        return cmul(p, q)

    rows = []
    for i in range(2):
        row = []
        for j in range(3):
            sq = dot_row(herm[i], [herm[k][j] for k in range(3)], mul)
            re, im = -0.5 * sq[0], -0.5 * sq[1]
            if herm[i][j][1] is not None:
                re = re - herm[i][j][1]
            else:
                re = re + 1.0
            row.append((re, im + herm[i][j][0]))
        rows.append(row)

    def unit(row):
        inv = lax.rsqrt(sum(p[0] * p[0] + p[1] * p[1] for p in row))
        return [(p[0] * inv, p[1] * inv) for p in row]

    one = unit(rows[0])
    corr = dot_row(one, rows[1], conj_mul)
    two = unit([csub(rows[1][k], cmul(corr, one[k])) for k in range(3)])
    return [one, two, cross_conj(one, two)]


def block(k):
    return pl.ds(pl.multiple_of(k * LANES, LANES), LANES)


def lane_ids(rows=8):
    return lax.broadcasted_iota(jnp.int32, (rows, LANES), 1)


def load_link(ref, d, sl):
    rows = [[(ref[d, r, c, 0, :, sl], ref[d, r, c, 1, :, sl]) for c in range(3)] for r in range(2)]
    return rows + [cross_conj(rows[0], rows[1])]


def algebra_kernel(links, out):
    def step(k, carry):
        sl = block(k)
        for d in range(3):
            for a, v in enumerate(algebra_of(load_link(links, d, sl))):
                out[d, a, :, sl] = v
        return carry

    lax.fori_loop(0, links.shape[-1] // LANES, step, 0)


def split3(x):
    hi = x.astype(bf16)
    lo = (x - hi.astype(f32)).astype(bf16)
    return jnp.concatenate([hi, lo, hi], axis=0)


def transform(table, parts):
    both = jnp.dot(table, split3(jnp.concatenate(parts, axis=1)), preferred_element_type=f32)
    return [both[:, i * LANES : (i + 1) * LANES] for i in range(len(parts))]


def swap(v):
    return pltpu.roll(v, 4, 0)


def flip(place, i, group):
    other = place
    for b in range(group.bit_length() - 1):
        if i >> b & 1:
            other = other + (1 << b) * (1 - 2 * lax.rem(lax.div(place, 1 << b), 2))
    return other


def spread_kernel(
    extent, group, alg, y_rim, z_below, z_above, coords, out, theta, mine, send_sem, recv_sem, edge_send, edge_recv
):
    nb = alg.shape[-1] // LANES
    yb = y_rim.shape[-1] // LANES
    half = alg.shape[2] // 2
    third = nb // UNITS
    lane = lane_ids()
    me = lax.axis_index("space")
    place = lax.rem(me, group)
    base = me - place
    beyond = group - base
    barrier = greet([base + flip(place, i, group) for i in range(1, group)] + [beyond + i for i in range(group)])

    def step(k, total):
        sl = block(k)
        before = block(jnp.maximum(k - 1, 0))
        after = block(jnp.minimum(k + 1, nb - 1))
        edge_x = coords[0, :, sl] == 0
        edge_z = coords[1, :, sl] == 0
        for a in range(8):
            x, y, z = alg[0, a, :, sl], alg[1, a, :, sl], alg[2, a, :, sl]
            near = pltpu.roll(jnp.where(lane == LANES - 1, alg[0, a, :, before], x), 1, 1)
            far = pltpu.roll(jnp.where(lane < extent - 1, alg[0, a, :, after], x), LANES - extent + 1, 1)
            bx = jnp.where(edge_x, far, near)
            by = jnp.where(
                k < yb,
                y_rim[a, :, block(jnp.minimum(k, yb - 1))],
                alg[1, a, :, block(jnp.maximum(k - yb, 0))],
            )
            prev = jnp.where(k == 0, z_below[a], alg[2, a, :, before])
            near = pltpu.roll(jnp.where(lane >= LANES - extent, prev, z), extent, 1)
            far = pltpu.roll(jnp.where(k == 0, alg[2, a, :, block(yb)], z_above[a]), extent, 1)
            bz = jnp.where(edge_z, far, near)
            b = (bx - x) + (by - y) + (bz - z)
            total = total + b * b
            mine[2 * a, k] = b[:half]
            mine[2 * a + 1, k] = b[half:]
        return total

    def edge_copy(i):
        return pltpu.make_async_remote_copy(
            src_ref=mine.at[i, pl.ds(0, 1)],
            dst_ref=out.at[pl.ds(group * nb, 1)],
            send_sem=edge_send.at[i],
            recv_sem=edge_recv.at[0],
            device_id={"space": beyond + i},
            device_id_type=MESH,
        )

    total = jnp.zeros((8, LANES), f32)
    copies = []
    for c in range(UNITS):
        total = lax.fori_loop(c * third, (c + 1) * third, step, total)
        if c == 0:
            pl.semaphore_wait(barrier, 2 * group - 1)

            @pl.when(place == 0)
            def _():
                for i in range(group):
                    edge_copy(i).start()

        for i in reversed(range(1, group)):
            other = flip(place, i, group)
            copy = pltpu.make_async_remote_copy(
                src_ref=mine.at[other, pl.ds(c * third, third)],
                dst_ref=out.at[pl.ds(place * nb + c * third, third)],
                send_sem=send_sem.at[c, i],
                recv_sem=recv_sem.at[c, i],
                device_id={"space": base + other},
                device_id_type=MESH,
            )
            copy.start()
            copies.append(copy)
    theta[...] = total

    def keep(k, carry):
        out[place * nb + k] = mine[place, k]
        return carry

    lax.fori_loop(0, nb, keep, 0)
    for copy in copies:
        copy.wait()
    edge_copy(0).wait_recv()

    @pl.when(place == 0)
    def _():
        for i in range(group):
            edge_copy(i).wait_send()


def solve_kernel(
    extent, group, fields, decay, weight, close, x_table, z_table, z_back, own_zero, far_zero,
    smooth, one, two, modes, ends, far, mode, far_mode, outgo, held, edge_held,
    end_send, end_recv, send_sem, recv_sem, edge_send, edge_recv,
):
    n = extent
    nb = smooth.shape[-1] // LANES
    planes = group * nb * LANES // (n * n)
    columns = n * n // LANES
    pairs = planes // 2
    lanes = planes * 4
    per = columns // PIECES
    unit = nb // UNITS
    me = lax.axis_index("space")
    place = lax.rem(me, group)
    base = me - place
    beyond = group - base
    upper = lax.broadcasted_iota(jnp.int32, (8, LANES), 0) >= 4
    barrier = greet([base + flip(place, i, group) for i in range(1, group)] + [beyond + i for i in range(group)])

    def rows_at(i):
        return pl.ds(pl.multiple_of(i * n, 8), n)

    def turn_in(c, extra):
        tiles = [fields[y * columns + c] for y in range(planes)] + extra
        rest = LANES - 4 * len(tiles)
        full = jnp.concatenate(tiles + [jnp.zeros((rest, LANES), f32)], axis=0)
        one[block(c), :] = full.T

    turn_in(0, [fields[planes * columns]])

    def turn_rest(c, carry):
        turn_in(c, [])
        return carry

    lax.fori_loop(1, columns, turn_rest, 0)
    one[0:n, :] = pltpu.roll(one[0:n, :], LANES - 4, 1)

    def along_x(i, carry):
        parts = [one[rows_at(2 * i + e), :] for e in range(2)]
        for e, v in enumerate(transform(x_table[...], parts)):
            two[rows_at(2 * i + e), :] = v
        return carry

    lax.fori_loop(0, n // 2, along_x, 0, unroll=4)

    def along_z(i, carry):
        parts = [two[pl.ds(2 * i + e, n, stride=n), :] for e in range(2)]
        for e, v in enumerate(transform(z_table[...], parts)):
            one[rows_at(2 * i + e), :] = v
        return carry

    def end_copy(p):
        cols = pl.ds(p * per * LANES, per * LANES)
        return pltpu.make_async_remote_copy(
            src_ref=ends.at[:, cols],
            dst_ref=far.at[:, cols],
            send_sem=end_send.at[p],
            recv_sem=end_recv.at[p],
            device_id={"space": beyond + place},
            device_id_type=MESH,
        )

    mode_copy = pltpu.make_async_remote_copy(
        src_ref=mode,
        dst_ref=far_mode,
        send_sem=end_send.at[PIECES],
        recv_sem=end_recv.at[PIECES],
        device_id={"space": beyond + place},
        device_id_type=MESH,
    )

    def reduce_ends(c, carry):
        sl = block(c)
        modes[:, sl] = one[sl, :].T[:lanes]
        mu = decay[:, sl]
        mu2 = mu * mu
        low = jnp.where(upper, 1.0, mu)
        high = jnp.where(upper, mu, 1.0)
        fwd = modes[0:8, sl]
        bwd = modes[lanes - 8 : lanes, sl]
        for i in range(1, pairs):
            fwd = fwd * mu2 + modes[8 * i : 8 * i + 8, sl]
            bwd = bwd * mu2 + modes[lanes - 8 - 8 * i : lanes - 8 * i, sl]
        ends[:, sl] = jnp.where(upper, high * bwd + low * swap(bwd), low * fwd + high * swap(fwd))
        return carry

    step_z = n // 2 // PIECES
    for p in range(PIECES):
        lax.fori_loop(p * step_z, (p + 1) * step_z, along_z, 0, unroll=4)
        if p == 0:
            mode[...] = one[0:8, :]
        lax.fori_loop(p * per, (p + 1) * per, reduce_ends, 0)
        if p == 0:
            pl.semaphore_wait(barrier, 2 * group - 1)
            mode_copy.start()
        end_copy(p).start()

    def sweep(c, carry):
        sl = block(c)
        mu = decay[:, sl]
        mu2 = mu * mu
        low = jnp.where(upper, 1.0, mu)
        high = jnp.where(upper, mu, 1.0)
        total = close[0, :, sl] * far[:, sl] + close[1, :, sl] * ends[:, sl]
        turned = swap(total)
        e = jnp.where(upper, turned, total)
        f = jnp.where(upper, total, turned) * mu
        w = weight[:, sl]
        up = mu * high
        down = jnp.where(upper, 0.0, mu)
        rising = []
        for i in range(pairs):
            v = modes[8 * i : 8 * i + 8, sl]
            s = low * v + high * swap(v)
            rising.append(jnp.where(upper, s, v) + up * e)
            e = mu2 * e + s
        done = [None] * pairs
        for i in reversed(range(pairs)):
            v = modes[8 * i : 8 * i + 8, sl]
            t = swap(v)
            done[i] = w * (rising[i] + low * f + down * t)
            f = mu2 * f + mu * (high * v + low * t)
        full = jnp.concatenate(done + [jnp.zeros((LANES - lanes, LANES), f32)], axis=0)
        one[sl, :] = full.T
        return carry

    def back_z(i, carry):
        parts = [one[rows_at(2 * i + e), :] for e in range(2)]
        for e, v in enumerate(transform(z_back[...], parts)):
            two[pl.ds(2 * i + e, n, stride=n), :] = v
        return carry

    for p in range(PIECES):
        end_copy(p).wait_recv()
        if p == 0:
            mode_copy.wait_recv()
        lax.fori_loop(p * per, (p + 1) * per, sweep, 0)
        if p == 0:
            exact = functools.partial(jnp.dot, preferred_element_type=f32, precision=lax.Precision.HIGHEST)
            flat = exact(mode[...], own_zero[...]) + exact(far_mode[...], far_zero[...])
            first = lax.broadcasted_iota(jnp.int32, (8, LANES), 0) == 0
            one[0:8, :] = jnp.where(first, flat, one[0:8, :])
        lax.fori_loop(p * step_z, (p + 1) * step_z, back_z, 0, unroll=4)

    def back_x(i, carry):
        parts = [two[rows_at(2 * i + e), :] for e in range(2)]
        for e, v in enumerate(transform(x_table[...], parts)):
            one[rows_at(2 * i + e), :] = v
        return carry

    lax.fori_loop(0, n // 2, back_x, 0, unroll=4)
    one[0:n, :] = pltpu.roll(one[0:n, :], 4, 1)

    def turn_out(c):
        full = one[block(c), :].T
        for y in range(planes):
            outgo[y * columns + c] = full[4 * y : 4 * y + 4]
        return full

    def turn_out_rest(c, carry):
        turn_out(c)
        return carry

    def unit_copy(i, v):
        other = flip(place, i, group)
        return pltpu.make_async_remote_copy(
            src_ref=outgo.at[pl.ds(other * nb + v * unit, unit)],
            dst_ref=held.at[place, pl.ds(v * unit, unit)],
            send_sem=send_sem.at[v, i],
            recv_sem=recv_sem.at[v, i],
            device_id={"space": base + other},
            device_id_type=MESH,
        )

    edge_copy = pltpu.make_async_remote_copy(
        src_ref=outgo.at[pl.ds(planes * columns, 1)],
        dst_ref=edge_held.at[place],
        send_sem=edge_send.at[0],
        recv_sem=edge_recv.at[place],
        device_id={"space": beyond},
        device_id_type=MESH,
    )

    full = turn_out(0)
    outgo[planes * columns] = full[lanes : lanes + 4]
    for side in range(2):
        lax.fori_loop(max(1, side * unit), (side + 1) * unit, turn_out_rest, 0)
        if side == 0:
            edge_copy.start()
        for i in reversed(range(1, group)):
            odd = lax.rem(place + i + side, 2)
            unit_copy(i, odd).start()

            @pl.when(odd == 0)
            def _():
                unit_copy(i, 2).start()

    def keep(k, carry):
        held[place, k] = outgo[place * nb + k]
        return carry

    lax.fori_loop(0, nb, keep, 0)
    for p in range(PIECES):
        end_copy(p).wait_send()
    mode_copy.wait_send()
    for i in reversed(range(1, group)):
        for v in range(UNITS):
            unit_copy(i, v).wait()

    def gather(k, carry):
        for a in range(8):
            smooth[a, :, block(k)] = jnp.concatenate([held[2 * a, k], held[2 * a + 1, k]], axis=0)
        return carry

    lax.fori_loop(0, nb, gather, 0)
    edge_copy.wait_send()

    @pl.when(place == 0)
    def _():
        for i in range(group):
            pltpu.make_async_remote_copy(
                src_ref=outgo.at[pl.ds(planes * columns, 1)],
                dst_ref=edge_held.at[i],
                send_sem=edge_send.at[0],
                recv_sem=edge_recv.at[i],
                device_id={"space": beyond},
                device_id_type=MESH,
            ).wait_recv()
        for a in range(8):
            row = jnp.concatenate([edge_held[2 * a, 0], edge_held[2 * a + 1, 0]], axis=0)
            smooth[a, :, 0:LANES] = jnp.where(lane_ids() < n, row, smooth[a, :, 0:LANES])


def link_kernel(extent, links, smooth, above, below, coords, out, deficit, rot):
    nb = smooth.shape[-1] // LANES
    yb = above.shape[-1] // LANES
    lane = lane_ids()

    def rotate(values, sl):
        g = rotation_of(values)
        for i in range(3):
            for j in range(3):
                for p in range(2):
                    rot[6 * i + 2 * j + p, :, sl] = g[i][j][p]

    def rotate_own(k, carry):
        rotate([smooth[a, :, block(k)] for a in range(8)], block(k))
        return carry

    def rotate_above(k, carry):
        rotate([above[a, :, block(k)] for a in range(8)], block(nb + k))
        return carry

    lax.fori_loop(0, nb, rotate_own, 0)
    lax.fori_loop(0, yb, rotate_above, 0)
    rotate([below[a] for a in range(8)], block(nb + yb))

    def step(k, total):
        sl = block(k)
        before = block(jnp.maximum(k - 1, 0))
        after = block(k + 1)
        wrap = block(jnp.where(k == yb, 0, nb + yb))
        edge_x = coords[0, :, sl] == extent - 1
        edge_z = coords[1, :, sl] == extent - 1

        def ahead_x(e):
            cur = rot[e, :, sl]
            near = pltpu.roll(jnp.where(lane == 0, rot[e, :, after], cur), LANES - 1, 1)
            far = pltpu.roll(jnp.where(lane >= LANES - extent + 1, rot[e, :, before], cur), extent - 1, 1)
            return jnp.where(edge_x, far, near)

        def ahead_y(e):
            return rot[e, :, block(k + yb)]

        def ahead_z(e):
            cur = rot[e, :, sl]
            near = pltpu.roll(jnp.where(lane < extent, rot[e, :, after], cur), LANES - extent, 1)
            far = pltpu.roll(rot[e, :, wrap], LANES - extent, 1)
            return jnp.where(edge_z, far, near)

        for d, ahead in enumerate((ahead_x, ahead_y, ahead_z)):
            u = load_link(links, d, sl)
            own = [[(rot[6 * i + 2 * j, :, sl], rot[6 * i + 2 * j + 1, :, sl]) for j in range(3)] for i in range(3)]
            left = [
                [dot_row(own[i], [u[k2][j] for k2 in range(3)], cmul) for j in range(3)]
                for i in range(3)
            ]
            for j in range(3):
                row = [(ahead(6 * j + 2 * c), ahead(6 * j + 2 * c + 1)) for c in range(3)]
                for i in range(2):
                    v = dot_row(left[i], row, mul_conj)
                    out[d, i, j, 0, :, sl] = v[0]
                    out[d, i, j, 1, :, sl] = v[1]
                    if i == j:
                        total = total + (1.0 - v[0])
                if j == 2:
                    total = total + (1.0 - dot_row(left[2], row, mul_conj)[0])
        return total

    deficit[...] = lax.fori_loop(0, nb, step, jnp.zeros((8, LANES), f32))


def greet(others):
    barrier = pltpu.get_barrier_semaphore()
    for other in others:
        pl.semaphore_signal(barrier, inc=1, device_id={"space": other}, device_id_type=MESH)
    return barrier


def halo_kernel(n, moves, source, *refs):
    outs, (send_sem, recv_sem) = refs[:-2], refs[-2:]
    me = lax.axis_index("space")
    ahead, behind = lax.rem(me + 1, n), lax.rem(me + n - 1, n)
    barrier = greet([ahead, behind])
    pl.semaphore_wait(barrier, 2)
    odd = lax.rem(me, 2)
    copies = []
    for i, (direction, select) in enumerate(moves):
        copy = pltpu.make_async_remote_copy(
            src_ref=select(source, odd),
            dst_ref=outs[i],
            send_sem=send_sem.at[i],
            recv_sem=recv_sem.at[i],
            device_id={"space": ahead if direction > 0 else behind},
            device_id_type=MESH,
        )
        copy.start()
        copies.append(copy)
    for copy in copies:
        copy.wait()


def halos(source, n, moves, shapes, number):
    count = len(moves)
    return call(
        functools.partial(halo_kernel, n, moves),
        shapes,
        [pltpu.SemaphoreType.DMA((count,)), pltpu.SemaphoreType.DMA((count,))],
        source,
        params=pltpu.CompilerParams(collective_id=number, has_side_effects=True),
    )


def sum_kernel(n, scales, theta, deficit, out_theta, out_deficit, mine, held, send_sem, recv_sem):
    me = lax.axis_index("space")
    barrier = greet([lax.rem(me + i, n) for i in range(1, n)])
    slices = deficit.shape[0]
    lane = lane_ids(slices)
    t = jnp.sum(jnp.sum(theta[...], axis=1, keepdims=True), axis=0, keepdims=True)
    d = jnp.sum(deficit[...], axis=1, keepdims=True)
    own = lax.broadcasted_iota(jnp.int32, (slices, LANES), 0)
    mine[...] = jnp.where(lane == own, d, jnp.where(lane == slices, jnp.where(own == 0, t, 0.0), 0.0))
    pl.semaphore_wait(barrier, n - 1)
    copies = []
    for i in range(1, n):
        copy = pltpu.make_async_remote_copy(
            src_ref=mine,
            dst_ref=held.at[i],
            send_sem=send_sem.at[i],
            recv_sem=recv_sem.at[i],
            device_id={"space": lax.rem(me + i, n)},
            device_id_type=MESH,
        )
        copy.start()
        copies.append(copy)
    for copy in copies:
        copy.wait()
    total = mine[...]
    for i in range(1, n):
        total = total + held[i]
    row = jnp.sum(total, axis=0, keepdims=True)
    out_deficit[...] = row[:, :slices] * scales[1]
    out_theta[...] = row[:, slices : slices + 1] * scales[0]


def call(kernel, out_shape, scratch, *args, params=PARAMS):
    return pl.pallas_call(
        kernel,
        out_shape=out_shape,
        in_specs=[VM] * len(args),
        out_specs=jax.tree.map(lambda _: VM, out_shape),
        scratch_shapes=scratch,
        compiler_params=params,
    )(*args)


def wide(full):
    full = full.astype(np.float32)
    hi = full.astype(jnp.bfloat16)
    lo = (full - hi.astype(np.float32)).astype(jnp.bfloat16)
    return jnp.asarray(np.concatenate([hi, hi, lo], axis=1))


def hartley(n, offset=0):
    k = np.arange(n)
    angle = 2.0 * np.pi / n * ((k[:, None] * (k[None, :] - offset)) % n)
    return (np.cos(angle) + np.sin(angle)) / np.sqrt(n)


def decay_tables(n, planes):
    wave = 4.0 * np.sin(np.pi * np.arange(n) / n) ** 2
    p = (wave[:, None] + wave[None, :]).reshape(-1)
    p[0] = 1.0
    mu = 1.0 + 0.5 * p - np.sqrt(p + 0.25 * p * p)
    weight = top_momentum / (1.0 / mu - mu)
    close = 1.0 / (1.0 - mu ** (2 * planes))
    rows = np.stack([mu, weight, close, close * mu**planes])
    rows[:, 0] = 0.0
    rows = np.broadcast_to(rows[:, None, :], (4, 8, n * n)).astype(np.float32)
    return jnp.asarray(rows[0]), jnp.asarray(rows[1]), jnp.asarray(rows[2:])


def zero_tables(n, planes):
    d = np.arange(n)
    green = top_momentum * ((n * n - 1.0) / (12.0 * n) - d * (n - d) / (2.0 * n))
    y = np.arange(planes)
    outs = []
    for shift in (0, planes):
        small = green[(y[:, None] - y[None, :] + shift) % n]
        full = np.zeros((LANES, LANES), np.float32)
        full[: 4 * planes, : 4 * planes] = np.kron(small, np.eye(4))
        outs.append(jnp.asarray(full))
    return outs


def body(links):
    n = EXTENT
    slices, local = links.shape[0], links.shape[-1]
    devices = lax.axis_size("space")
    plane = n * n
    q = local // n
    me = lax.axis_index("space")
    shape = lambda *s: jax.ShapeDtypeStruct(s, f32)


    site = jnp.arange(local, dtype=jnp.int32)
    coords = jnp.stack([site % n, (me * q + site // n - 1) % n])
    coords = jnp.broadcast_to(coords[:, None, :], (2, slices, local))
    across = jnp.transpose(links, (1, 2, 3, 4, 0, 5))
    alg = call(algebra_kernel, shape(3, 8, slices, local), [], across)
    mid = (n // 2) * n
    side = lambda start: pl.ds(pl.multiple_of(start, LANES), LANES)
    y_rim, z_below, z_above = halos(
        alg,
        devices,
        [
            (1, lambda r, odd: r.at[1, :, :, local - plane :]),
            (1, lambda r, odd: r.at[2, :, :, local - LANES :]),
            (-1, lambda r, odd: r.at[2, :, :, side(odd * mid)]),
        ],
        (shape(8, slices, plane), shape(8, slices, LANES), shape(8, slices, LANES)),
        2,
    )
    group = devices // 2
    planes = n // 2
    nb = local // LANES
    assert group * 4 == 8 * slices and nb % UNITS == 0
    dma = lambda *s: pltpu.SemaphoreType.DMA(s)
    fields, theta = call(
        functools.partial(spread_kernel, n, group),
        (shape(group * nb + 1, 4, LANES), shape(slices, LANES)),
        [pltpu.VMEM((group, nb, 4, LANES), f32), dma(UNITS, group), dma(UNITS, group), dma(group), dma(1)],
        alg, y_rim, z_below, z_above, coords,
        params=pltpu.CompilerParams(collective_id=3, has_side_effects=True, vmem_limit_bytes=60 * 1024 * 1024),
    )
    vm = lambda *s: pltpu.VMEM(s, f32)
    smooth = call(
        functools.partial(solve_kernel, n, group),
        shape(8, slices, local),
        [
            vm(plane, LANES), vm(plane, LANES), vm(4 * planes, plane), vm(8, plane), vm(8, plane),
            vm(8, LANES), vm(8, LANES), vm(group * nb + 1, 4, LANES), vm(group, nb, 4, LANES), vm(group, 1, 4, LANES),
            dma(PIECES + 1), dma(PIECES + 1), dma(UNITS, group), dma(UNITS, group), dma(1), dma(group),
        ],
        fields, *decay_tables(n, planes), wide(hartley(n)), wide(hartley(n, 1)), wide(hartley(n, 1).T), *zero_tables(n, planes),
        params=pltpu.CompilerParams(collective_id=4, has_side_effects=True, vmem_limit_bytes=60 * 1024 * 1024),
    )
    above, below = halos(
        smooth,
        devices,
        [
            (-1, lambda r, odd: r.at[:, :, :plane]),
            (1, lambda r, odd: r.at[:, :, side(plane - odd * (plane - mid))]),
        ],
        (shape(8, slices, plane), shape(8, slices, LANES)),
        5,
    )
    turned, deficit = call(
        functools.partial(link_kernel, n),
        (shape(3, 2, 3, 2, slices, local), shape(slices, LANES)),
        [pltpu.VMEM((18, slices, local + plane + LANES), f32)],
        across, smooth, above, below, coords,
    )
    new_links = jnp.transpose(turned, (4, 0, 1, 2, 3, 5))
    times = lax.axis_size("tm")
    scales = (1.0 / (slices * times * n**3), 1.0 / n**3)
    total, shares = call(
        functools.partial(sum_kernel, devices, scales),
        (shape(1, 1), shape(1, slices)),
        [
            pltpu.VMEM((slices, LANES), f32),
            pltpu.VMEM((devices, slices, LANES), f32),
            pltpu.SemaphoreType.DMA((devices,)),
            pltpu.SemaphoreType.DMA((devices,)),
        ],
        theta, deficit,
        params=pltpu.CompilerParams(collective_id=1, has_side_effects=True),
    )
    total = total.reshape(())
    if times > 1:
        total = lax.psum(total, "tm")
    return (new_links, total, shares.reshape(slices))


def solution(mesh):
    placed = (P("tm", None, None, None, None, "space"),)
    return jax.shard_map(
        body,
        mesh=mesh,
        in_specs=placed,
        out_specs=(P("tm", None, None, None, None, "space"), P(), P("tm")),
        check_vma=False,
    )
```

```python
import functools
import math

import jax
import jax.numpy as jnp
import numpy as np
from jax import lax
from jax.experimental import pallas as pl
from jax.experimental.pallas import tpu as pltpu
from jax.sharding import PartitionSpec as P

EXTENT = 48
LANES = 128
UNITS = 3
PIECES = 6
LINK_MB = 24

root_three = math.sqrt(3.0)
step_size = 0.08
top_momentum = 12.0

f32 = jnp.float32
bf16 = jnp.bfloat16
MESH = pl.DeviceIdType.MESH
VM = pl.BlockSpec(memory_space=pltpu.VMEM)


def cmul(p, q):
    return (p[0] * q[0] - p[1] * q[1], p[0] * q[1] + p[1] * q[0])


def cadd(p, q):
    return (p[0] + q[0], p[1] + q[1])


def csub(p, q):
    return (p[0] - q[0], p[1] - q[1])


def conj(p):
    return (p[0], -p[1])


def conj_mul(p, q):
    return (p[0] * q[0] + p[1] * q[1], p[0] * q[1] - p[1] * q[0])


def mul_conj(p, q):
    return (p[0] * q[0] + p[1] * q[1], p[1] * q[0] - p[0] * q[1])


def dot_row(row, col, mul):
    out = mul(row[0], col[0])
    for k in (1, 2):
        out = cadd(out, mul(row[k], col[k]))
    return out


def cross_conj(a, b):
    return [
        conj(csub(cmul(a[(k + 1) % 3], b[(k + 2) % 3]), cmul(a[(k + 2) % 3], b[(k + 1) % 3])))
        for k in range(3)
    ]


def algebra_of(u):
    return [
        u[0][1][1] + u[1][0][1],
        u[0][1][0] - u[1][0][0],
        u[0][0][1] - u[1][1][1],
        u[0][2][1] + u[2][0][1],
        u[0][2][0] - u[2][0][0],
        u[1][2][1] + u[2][1][1],
        u[1][2][0] - u[2][1][0],
        (u[0][0][1] + u[1][1][1] - 2.0 * u[2][2][1]) * (1.0 / root_three),
    ]


def rotation_of(s):
    h = 0.5 * step_size
    s = [v * h for v in s]
    third = s[7] * (1.0 / root_three)
    d0, d1, d2 = s[2] + third, third - s[2], -2.0 * third
    herm = [
        [(d0, None), (s[0], -s[1]), (s[3], -s[4])],
        [(s[0], s[1]), (d1, None), (s[5], -s[6])],
        [(s[3], s[4]), (s[5], s[6]), (d2, None)],
    ]

    def mul(p, q):
        if p[1] is None and q[1] is None:
            return (p[0] * q[0], jnp.zeros_like(p[0]))
        if p[1] is None:
            return (p[0] * q[0], p[0] * q[1])
        if q[1] is None:
            return (p[0] * q[0], p[1] * q[0])
        return cmul(p, q)

    rows = []
    for i in range(2):
        row = []
        for j in range(3):
            sq = dot_row(herm[i], [herm[k][j] for k in range(3)], mul)
            re, im = -0.5 * sq[0], -0.5 * sq[1]
            if herm[i][j][1] is not None:
                re = re - herm[i][j][1]
            else:
                re = re + 1.0
            row.append((re, im + herm[i][j][0]))
        rows.append(row)

    def unit(row):
        inv = lax.rsqrt(sum(p[0] * p[0] + p[1] * p[1] for p in row))
        return [(p[0] * inv, p[1] * inv) for p in row]

    one = unit(rows[0])
    corr = dot_row(one, rows[1], conj_mul)
    two = unit([csub(rows[1][k], cmul(corr, one[k])) for k in range(3)])
    return [one, two, cross_conj(one, two)]


def block(k):
    return pl.ds(pl.multiple_of(k * LANES, LANES), LANES)


def lane_ids(rows=8):
    return lax.broadcasted_iota(jnp.int32, (rows, LANES), 1)


def rows_of(slices, d, r, c, p):
    return pl.ds((d * 2 + r) * 6 + c * 2 + p, slices, stride=36)


def flat_block(ref, k):
    return ref.at[k].reshape(ref.shape[1] * 36, LANES)


def load_link(ref, slices, d):
    rows = [[tuple(ref[rows_of(slices, d, r, c, p), :] for p in range(2)) for c in range(3)] for r in range(2)]
    return rows + [cross_conj(rows[0], rows[1])]


def site_of(k, extent):
    start = k * LANES
    shifted = lane_ids() + lax.rem(start, extent)
    wraps = sum((shifted >= extent * i).astype(jnp.int32) for i in range(1, (LANES + extent - 1) // extent + 1))
    return shifted - extent * wraps, lax.div(start, extent) + wraps


def at_z(row, z, me, rows, extent):
    first = lax.rem(extent + z + 1 - lax.rem(me * rows, extent), extent)
    hit = row == first
    for i in range(1, -(-rows // extent)):
        hit = hit | (row == first + i * extent)
    return hit


def fetch_block(links, held, sem, k, start=0):
    return pltpu.make_async_copy(links.at[:, :, :, :, :, pl.ds(k * LANES, LANES)], held.at[k - start], sem.at[k])


def split3(x):
    hi = x.astype(bf16)
    lo = (x - hi.astype(f32)).astype(bf16)
    return jnp.concatenate([hi, lo, hi], axis=0)


def transform(table, parts):
    both = jnp.dot(table, split3(jnp.concatenate(parts, axis=1)), preferred_element_type=f32)
    return [both[:, i * LANES : (i + 1) * LANES] for i in range(len(parts))]


def swap(v):
    return pltpu.roll(v, 4, 0)


def flip(place, i, group):
    other = place
    for b in range(group.bit_length() - 1):
        if i >> b & 1:
            other = other + (1 << b) * (1 - 2 * lax.rem(lax.div(place, 1 << b), 2))
    return other


def spread_kernel(
    extent, group, links, out, theta, *refs
):
    parts = refs[: UNITS + 1]
    (
        alg, y_rim, z_below, z_above, mine,
        load_sem, halo_send, halo_recv, send_sem, recv_sem, edge_send, edge_recv,
    ) = refs[UNITS + 1 :]
    n = 2 * group
    nb, slices = mine.shape[1], alg.shape[2]
    yb = extent * extent // LANES
    half = slices // 2
    unit = nb // UNITS
    q = nb * LANES // extent
    mid = (extent // 2) * extent
    lane = lane_ids()
    me = lax.axis_index("space")
    place = lax.rem(me, group)
    base = me - place
    beyond = group - base
    ahead, behind = lax.rem(me + 1, n), lax.rem(me + n - 1, n)
    spans = [(0, 1)] + [(i * unit, (i + 1) * unit) for i in range(1, UNITS)] + [(1, unit)]
    loads = [[fetch_block(links, held, load_sem, k, a) for k in range(a, b)] for (a, b), held in zip(spans, parts)]
    for copy in sum(loads, []):
        copy.start()
    barrier = greet([base + flip(place, i, group) for i in range(1, group)] + [beyond + i for i in range(group)])

    def algebra(i):
        start, stop = spans[i]

        def step(k, carry):
            flat = flat_block(parts[i], k - start)
            for d in range(3):
                for a, v in enumerate(algebra_of(load_link(flat, slices, d))):
                    alg[d, a, :, block(k)] = v
            return carry

        for copy in loads[i]:
            copy.wait()
        lax.fori_loop(start, stop, step, 0)

    def halo(i, source, dest, other):
        return pltpu.make_async_remote_copy(
            src_ref=source,
            dst_ref=dest,
            send_sem=halo_send.at[i],
            recv_sem=halo_recv.at[i],
            device_id={"space": other},
            device_id_type=MESH,
        )

    def span(start, size):
        return pl.ds(pl.multiple_of(start * LANES, LANES), size * LANES)

    first = nb - yb
    rims = [
        halo(i, alg.at[1, :, :, span(first + i * unit, unit)], y_rim.at[:, :, span(i * unit, unit)], ahead)
        for i in range(yb // unit)
    ]
    below_copy = halo(len(rims), alg.at[2, :, :, span(nb - 1, 1)], z_below, ahead)
    odd = lax.rem(me, 2)
    above_copy = halo(len(rims) + 1, alg.at[2, :, :, span(odd * (mid // LANES), 1)], z_above, behind)

    algebra(0)
    algebra(1)
    pl.semaphore_wait(barrier, n - 1)
    above_copy.start()
    rims[0].start()
    for i in range(1, len(rims)):
        algebra(1 + i)
        if i == len(rims) - 1:
            below_copy.start()
        rims[i].start()
    algebra(UNITS)

    def step(from_rim, k, total):
        sl = block(k)
        before = block(jnp.maximum(k - 1, 0))
        after = block(jnp.minimum(k + 1, nb - 1))
        x_at, row = site_of(k, extent)
        edge_x = x_at == 0
        edge_z = at_z(row, 0, me, q, extent)
        for a in range(8):
            x, y, z = alg[0, a, :, sl], alg[1, a, :, sl], alg[2, a, :, sl]
            near = pltpu.roll(jnp.where(lane == LANES - 1, alg[0, a, :, before], x), 1, 1)
            far = pltpu.roll(jnp.where(lane < extent - 1, alg[0, a, :, after], x), LANES - extent + 1, 1)
            bx = jnp.where(edge_x, far, near)
            by = y_rim[a, :, sl] if from_rim else alg[1, a, :, block(k - yb)]
            prev = jnp.where(k == 0, z_below[a], alg[2, a, :, before])
            near = pltpu.roll(jnp.where(lane >= LANES - extent, prev, z), extent, 1)
            far = pltpu.roll(jnp.where(k == 0, alg[2, a, :, block(yb)], z_above[a]), extent, 1)
            bz = jnp.where(edge_z, far, near)
            b = (bx - x) + (by - y) + (bz - z)
            total = total + b * b
            mine[2 * a, k] = b[:half]
            mine[2 * a + 1, k] = b[half:]
        return total

    def edge_copy(i):
        return pltpu.make_async_remote_copy(
            src_ref=mine.at[i, pl.ds(0, 1)],
            dst_ref=out.at[pl.ds(group * nb, 1)],
            send_sem=edge_send.at[i],
            recv_sem=edge_recv.at[0],
            device_id={"space": beyond + i},
            device_id_type=MESH,
        )

    total = jnp.zeros((8, LANES), f32)
    copies = []
    above_copy.wait_recv()
    below_copy.wait_recv()
    for c in [UNITS - 1] + list(range(UNITS - 1)):
        if c < len(rims):
            rims[c].wait_recv()
        total = lax.fori_loop(c * unit, (c + 1) * unit, functools.partial(step, c < len(rims)), total)
        if c == 0:

            @pl.when(place == 0)
            def _():
                for i in range(group):
                    edge_copy(i).start()

        for i in reversed(range(1, group)):
            other = flip(place, i, group)
            copy = pltpu.make_async_remote_copy(
                src_ref=mine.at[other, pl.ds(c * unit, unit)],
                dst_ref=out.at[pl.ds(place * nb + c * unit, unit)],
                send_sem=send_sem.at[c, i],
                recv_sem=recv_sem.at[c, i],
                device_id={"space": base + other},
                device_id_type=MESH,
            )
            copy.start()
            copies.append(copy)
    theta[...] = total

    def keep(k, carry):
        out[place * nb + k] = mine[place, k]
        return carry

    lax.fori_loop(0, nb, keep, 0)
    for copy in rims + [below_copy, above_copy]:
        copy.wait_send()
    for copy in copies:
        copy.wait()
    edge_copy(0).wait_recv()

    @pl.when(place == 0)
    def _():
        for i in range(group):
            edge_copy(i).wait_send()


def solve_kernel(
    extent, group, fields, decay, weight, close, x_table, z_table, z_back, own_zero, far_zero,
    smooth, one, two, modes, ends, far, mode, far_mode, outgo, held, edge_held,
    end_send, end_recv, send_sem, recv_sem, edge_send, edge_recv,
):
    n = extent
    nb = smooth.shape[-1] // LANES
    planes = group * nb * LANES // (n * n)
    columns = n * n // LANES
    pairs = planes // 2
    lanes = planes * 4
    per = columns // PIECES
    unit = nb // UNITS
    me = lax.axis_index("space")
    place = lax.rem(me, group)
    base = me - place
    beyond = group - base
    upper = lax.broadcasted_iota(jnp.int32, (8, LANES), 0) >= 4
    barrier = greet([base + flip(place, i, group) for i in range(1, group)] + [beyond + i for i in range(group)])

    def rows_at(i):
        return pl.ds(pl.multiple_of(i * n, 8), n)

    def turn_in(c, extra):
        tiles = [fields[y * columns + c] for y in range(planes)] + extra
        rest = LANES - 4 * len(tiles)
        full = jnp.concatenate(tiles + [jnp.zeros((rest, LANES), f32)], axis=0)
        one[block(c), :] = full.T

    turn_in(0, [fields[planes * columns]])

    def turn_rest(c, carry):
        turn_in(c, [])
        return carry

    lax.fori_loop(1, columns, turn_rest, 0)
    one[0:n, :] = pltpu.roll(one[0:n, :], LANES - 4, 1)

    def along_x(i, carry):
        parts = [one[rows_at(2 * i + e), :] for e in range(2)]
        for e, v in enumerate(transform(x_table[...], parts)):
            two[rows_at(2 * i + e), :] = v
        return carry

    lax.fori_loop(0, n // 2, along_x, 0, unroll=4)

    def along_z(i, carry):
        parts = [two[pl.ds(2 * i + e, n, stride=n), :] for e in range(2)]
        for e, v in enumerate(transform(z_table[...], parts)):
            one[rows_at(2 * i + e), :] = v
        return carry

    def end_copy(p):
        cols = pl.ds(p * per * LANES, per * LANES)
        return pltpu.make_async_remote_copy(
            src_ref=ends.at[:, cols],
            dst_ref=far.at[:, cols],
            send_sem=end_send.at[p],
            recv_sem=end_recv.at[p],
            device_id={"space": beyond + place},
            device_id_type=MESH,
        )

    mode_copy = pltpu.make_async_remote_copy(
        src_ref=mode,
        dst_ref=far_mode,
        send_sem=end_send.at[PIECES],
        recv_sem=end_recv.at[PIECES],
        device_id={"space": beyond + place},
        device_id_type=MESH,
    )

    def reduce_ends(c, carry):
        sl = block(c)
        modes[:, sl] = one[sl, :].T[:lanes]
        mu = decay[:, sl]
        mu2 = mu * mu
        low = jnp.where(upper, 1.0, mu)
        high = jnp.where(upper, mu, 1.0)
        fwd = modes[0:8, sl]
        bwd = modes[lanes - 8 : lanes, sl]
        for i in range(1, pairs):
            fwd = fwd * mu2 + modes[8 * i : 8 * i + 8, sl]
            bwd = bwd * mu2 + modes[lanes - 8 - 8 * i : lanes - 8 * i, sl]
        ends[:, sl] = jnp.where(upper, high * bwd + low * swap(bwd), low * fwd + high * swap(fwd))
        return carry

    step_z = n // 2 // PIECES
    for p in range(PIECES):
        lax.fori_loop(p * step_z, (p + 1) * step_z, along_z, 0, unroll=4)
        if p == 0:
            mode[...] = one[0:8, :]
        lax.fori_loop(p * per, (p + 1) * per, reduce_ends, 0)
        if p == 0:
            pl.semaphore_wait(barrier, 2 * group - 1)
            mode_copy.start()
        end_copy(p).start()

    def sweep(c, carry):
        sl = block(c)
        mu = decay[:, sl]
        mu2 = mu * mu
        low = jnp.where(upper, 1.0, mu)
        high = jnp.where(upper, mu, 1.0)
        total = close[0, :, sl] * far[:, sl] + close[1, :, sl] * ends[:, sl]
        turned = swap(total)
        e = jnp.where(upper, turned, total)
        f = jnp.where(upper, total, turned) * mu
        w = weight[:, sl]
        up = mu * high
        down = jnp.where(upper, 0.0, mu)
        rising = []
        for i in range(pairs):
            v = modes[8 * i : 8 * i + 8, sl]
            s = low * v + high * swap(v)
            rising.append(jnp.where(upper, s, v) + up * e)
            e = mu2 * e + s
        done = [None] * pairs
        for i in reversed(range(pairs)):
            v = modes[8 * i : 8 * i + 8, sl]
            t = swap(v)
            done[i] = w * (rising[i] + low * f + down * t)
            f = mu2 * f + mu * (high * v + low * t)
        full = jnp.concatenate(done + [jnp.zeros((LANES - lanes, LANES), f32)], axis=0)
        one[sl, :] = full.T
        return carry

    def back_z(i, carry):
        parts = [one[rows_at(2 * i + e), :] for e in range(2)]
        for e, v in enumerate(transform(z_back[...], parts)):
            two[pl.ds(2 * i + e, n, stride=n), :] = v
        return carry

    for p in range(PIECES):
        end_copy(p).wait_recv()
        if p == 0:
            mode_copy.wait_recv()
        lax.fori_loop(p * per, (p + 1) * per, sweep, 0)
        if p == 0:
            exact = functools.partial(jnp.dot, preferred_element_type=f32, precision=lax.Precision.HIGHEST)
            flat = exact(mode[...], own_zero[...]) + exact(far_mode[...], far_zero[...])
            first = lax.broadcasted_iota(jnp.int32, (8, LANES), 0) == 0
            one[0:8, :] = jnp.where(first, flat, one[0:8, :])
        lax.fori_loop(p * step_z, (p + 1) * step_z, back_z, 0, unroll=4)

    def back_x(i, carry):
        parts = [two[rows_at(2 * i + e), :] for e in range(2)]
        for e, v in enumerate(transform(x_table[...], parts)):
            one[rows_at(2 * i + e), :] = v
        return carry

    lax.fori_loop(0, n // 2, back_x, 0, unroll=4)
    one[0:n, :] = pltpu.roll(one[0:n, :], 4, 1)

    def turn_out(c):
        full = one[block(c), :].T
        for y in range(planes):
            outgo[y * columns + c] = full[4 * y : 4 * y + 4]
        return full

    def turn_out_rest(c, carry):
        turn_out(c)
        return carry

    def unit_copy(i, v):
        other = flip(place, i, group)
        return pltpu.make_async_remote_copy(
            src_ref=outgo.at[pl.ds(other * nb + v * unit, unit)],
            dst_ref=held.at[place, pl.ds(v * unit, unit)],
            send_sem=send_sem.at[v, i],
            recv_sem=recv_sem.at[v, i],
            device_id={"space": base + other},
            device_id_type=MESH,
        )

    edge_copy = pltpu.make_async_remote_copy(
        src_ref=outgo.at[pl.ds(planes * columns, 1)],
        dst_ref=edge_held.at[place],
        send_sem=edge_send.at[0],
        recv_sem=edge_recv.at[place],
        device_id={"space": beyond},
        device_id_type=MESH,
    )

    full = turn_out(0)
    outgo[planes * columns] = full[lanes : lanes + 4]
    for side in range(2):
        lax.fori_loop(max(1, side * unit), (side + 1) * unit, turn_out_rest, 0)
        if side == 0:
            edge_copy.start()
        for i in reversed(range(1, group)):
            odd = lax.rem(place + i + side, 2)
            unit_copy(i, odd).start()

            @pl.when(odd == 0)
            def _():
                unit_copy(i, 2).start()

    def keep(k, carry):
        held[place, k] = outgo[place * nb + k]
        return carry

    lax.fori_loop(0, nb, keep, 0)
    for p in range(PIECES):
        end_copy(p).wait_send()
    mode_copy.wait_send()
    for i in reversed(range(1, group)):
        for v in range(UNITS):
            unit_copy(i, v).wait()

    def gather(k, carry):
        for a in range(8):
            smooth[a, :, block(k)] = jnp.concatenate([held[2 * a, k], held[2 * a + 1, k]], axis=0)
        return carry

    lax.fori_loop(0, nb, gather, 0)
    edge_copy.wait_send()

    @pl.when(place == 0)
    def _():
        for i in range(group):
            pltpu.make_async_remote_copy(
                src_ref=outgo.at[pl.ds(planes * columns, 1)],
                dst_ref=edge_held.at[i],
                send_sem=edge_send.at[0],
                recv_sem=edge_recv.at[i],
                device_id={"space": beyond},
                device_id_type=MESH,
            ).wait_recv()
        for a in range(8):
            row = jnp.concatenate([edge_held[2 * a, 0], edge_held[2 * a + 1, 0]], axis=0)
            smooth[a, :, 0:LANES] = jnp.where(lane_ids() < n, row, smooth[a, :, 0:LANES])


def link_kernel(
    extent, scales, links, smooth, theta, done, out_theta, out_deficit,
    held, above, below, rot, mine, sums, load_sem, halo_send, halo_recv, send_sem, recv_sem,
):
    nb, slices = held.shape[0], held.shape[1]
    n = sums.shape[0]
    yb = extent * extent // LANES
    unit = nb // UNITS
    q = nb * LANES // extent
    mid = (extent // 2) * extent
    lane = lane_ids()
    me = lax.axis_index("space")
    ahead, behind = lax.rem(me + 1, n), lax.rem(me + n - 1, n)
    loads = [fetch_block(links, held, load_sem, k) for k in range(nb)]
    for copy in loads:
        copy.start()
    barrier = greet([lax.rem(me + i, n) for i in range(1, n)])

    def rotate(values, sl):
        g = rotation_of(values)
        for i in range(3):
            for j in range(3):
                for p in range(2):
                    rot[6 * i + 2 * j + p, :, sl] = g[i][j][p]

    def rotate_own(k, carry):
        rotate([smooth[a, :, block(k)] for a in range(8)], block(k))
        return carry

    def rotate_above(k, carry):
        rotate([above[a, :, block(k)] for a in range(8)], block(nb + k))
        return carry

    def halo(i, source, dest, other):
        return pltpu.make_async_remote_copy(
            src_ref=source,
            dst_ref=dest,
            send_sem=halo_send.at[i],
            recv_sem=halo_recv.at[i],
            device_id={"space": other},
            device_id_type=MESH,
        )

    def span(start, size):
        return pl.ds(pl.multiple_of(start * LANES, LANES), size * LANES)

    odd = lax.rem(me, 2)
    pick = yb - odd * (yb - mid // LANES)
    below_copy = halo(0, smooth.at[:, :, span(pick, 1)], below, ahead)
    rims = [
        halo(1 + i, smooth.at[:, :, span(i * unit, unit)], above.at[:, :, span(i * unit, unit)], behind)
        for i in range(yb // unit)
    ]

    lax.fori_loop(0, unit, rotate_own, 0)
    pl.semaphore_wait(barrier, n - 1)
    for copy in [below_copy] + rims:
        copy.start()
    lax.fori_loop(unit, nb, rotate_own, 0)

    def step(which, k, total):
        sl = block(k)
        before = block(jnp.maximum(k - 1, 0))
        after = block(k + 1)
        wrap = block(jnp.where(k == yb, 0, nb + yb))
        x_at, row = site_of(k, extent)
        edge_x = x_at == extent - 1
        edge_z = at_z(row, extent - 1, me, q, extent)

        def ahead_x(e):
            cur = rot[e, :, sl]
            near = pltpu.roll(jnp.where(lane == 0, rot[e, :, after], cur), LANES - 1, 1)
            far = pltpu.roll(jnp.where(lane >= LANES - extent + 1, rot[e, :, before], cur), extent - 1, 1)
            return jnp.where(edge_x, far, near)

        def ahead_y(e):
            return rot[e, :, block(k + yb)]

        def ahead_z(e):
            cur = rot[e, :, sl]
            near = pltpu.roll(jnp.where(lane < extent, rot[e, :, after], cur), LANES - extent, 1)
            far = pltpu.roll(rot[e, :, wrap], LANES - extent, 1)
            return jnp.where(edge_z, far, near)

        flat_out = flat_block(done, k)
        for d in which:
            forward = (ahead_x, ahead_y, ahead_z)[d]
            u = load_link(flat_block(held, k), slices, d)
            own = [[(rot[6 * i + 2 * j, :, sl], rot[6 * i + 2 * j + 1, :, sl]) for j in range(3)] for i in range(3)]
            left = [
                [dot_row(own[i], [u[k2][j] for k2 in range(3)], cmul) for j in range(3)]
                for i in range(3)
            ]
            for j in range(3):
                row3 = [(forward(6 * j + 2 * c), forward(6 * j + 2 * c + 1)) for c in range(3)]
                for i in range(2):
                    v = dot_row(left[i], row3, mul_conj)
                    flat_out[rows_of(slices, d, i, j, 0), :] = v[0]
                    flat_out[rows_of(slices, d, i, j, 1), :] = v[1]
                    if i == j:
                        total = total + (1.0 - v[0])
                if j == 2:
                    total = total + (1.0 - dot_row(left[2], row3, mul_conj)[0])
        return total

    for copy in loads:
        copy.wait()
    below_copy.wait_recv()
    rotate([below[a] for a in range(8)], block(nb + yb))
    total = jnp.zeros((8, LANES), f32)
    total = lax.fori_loop(0, nb - yb, functools.partial(step, (0, 1, 2)), total)
    total = lax.fori_loop(nb - yb, nb - 1, functools.partial(step, (0, 2)), total)
    for i, copy in enumerate(rims):
        copy.wait_recv()
        lax.fori_loop(i * unit, (i + 1) * unit, rotate_above, 0)
    total = lax.fori_loop(nb - yb, nb - 1, functools.partial(step, (1,)), total)
    total = lax.fori_loop(nb - 1, nb, functools.partial(step, (0, 1, 2)), total)

    wide_lane = lane_ids(slices)
    t = jnp.sum(jnp.sum(theta[...], axis=1, keepdims=True), axis=0, keepdims=True)
    d = jnp.sum(total, axis=1, keepdims=True)
    own_row = lax.broadcasted_iota(jnp.int32, (slices, LANES), 0)
    mine[...] = jnp.where(
        wide_lane == own_row, d, jnp.where(wide_lane == slices, jnp.where(own_row == 0, t, 0.0), 0.0)
    )
    copies = []
    for i in range(1, n):
        copy = pltpu.make_async_remote_copy(
            src_ref=mine,
            dst_ref=sums.at[i],
            send_sem=send_sem.at[i],
            recv_sem=recv_sem.at[i],
            device_id={"space": lax.rem(me + i, n)},
            device_id_type=MESH,
        )
        copy.start()
        copies.append(copy)
    for copy in [below_copy] + rims:
        copy.wait_send()
    for copy in copies:
        copy.wait()
    total = mine[...]
    for i in range(1, n):
        total = total + sums[i]
    row = jnp.sum(total, axis=0, keepdims=True)
    out_deficit[...] = row[:, :slices] * scales[1]
    out_theta[...] = row[:, slices : slices + 1] * scales[0]


def place_kernel(blocks, out, sem):
    copies = [
        pltpu.make_async_copy(blocks.at[k], out.at[:, :, :, :, :, pl.ds(k * LANES, LANES)], sem.at[k])
        for k in range(blocks.shape[0])
    ]
    for copy in copies:
        copy.start()
    for copy in copies:
        copy.wait()


def greet(others):
    barrier = pltpu.get_barrier_semaphore()
    for other in others:
        pl.semaphore_signal(barrier, inc=1, device_id={"space": other}, device_id_type=MESH)
    return barrier


ANY = pl.BlockSpec(memory_space=pl.ANY)


def call(kernel, number, out_shape, scratch, *args, in_specs=None, out_specs=None, limit=60):
    return pl.pallas_call(
        kernel,
        out_shape=out_shape,
        in_specs=in_specs or [VM] * len(args),
        out_specs=out_specs or jax.tree.map(lambda _: VM, out_shape),
        scratch_shapes=scratch,
        compiler_params=pltpu.CompilerParams(
            collective_id=number, has_side_effects=True, vmem_limit_bytes=limit * 1024 * 1024
        ),
    )(*args)


def wide(full):
    full = full.astype(np.float32)
    hi = full.astype(jnp.bfloat16)
    lo = (full - hi.astype(np.float32)).astype(jnp.bfloat16)
    return jnp.asarray(np.concatenate([hi, hi, lo], axis=1))


def hartley(n, offset=0):
    k = np.arange(n)
    angle = 2.0 * np.pi / n * ((k[:, None] * (k[None, :] - offset)) % n)
    return (np.cos(angle) + np.sin(angle)) / np.sqrt(n)


def decay_tables(n, planes):
    wave = 4.0 * np.sin(np.pi * np.arange(n) / n) ** 2
    p = (wave[:, None] + wave[None, :]).reshape(-1)
    p[0] = 1.0
    mu = 1.0 + 0.5 * p - np.sqrt(p + 0.25 * p * p)
    weight = top_momentum / (1.0 / mu - mu)
    close = 1.0 / (1.0 - mu ** (2 * planes))
    rows = np.stack([mu, weight, close, close * mu**planes])
    rows[:, 0] = 0.0
    rows = np.broadcast_to(rows[:, None, :], (4, 8, n * n)).astype(np.float32)
    return jnp.asarray(rows[0]), jnp.asarray(rows[1]), jnp.asarray(rows[2:])


def zero_tables(n, planes):
    d = np.arange(n)
    green = top_momentum * ((n * n - 1.0) / (12.0 * n) - d * (n - d) / (2.0 * n))
    y = np.arange(planes)
    outs = []
    for shift in (0, planes):
        small = green[(y[:, None] - y[None, :] + shift) % n]
        full = np.zeros((LANES, LANES), np.float32)
        full[: 4 * planes, : 4 * planes] = np.kron(small, np.eye(4))
        outs.append(jnp.asarray(full))
    return outs


def body(links):
    n = EXTENT
    slices, local = links.shape[0], links.shape[-1]
    devices = lax.axis_size("space")
    plane = n * n
    shape = lambda *s: jax.ShapeDtypeStruct(s, f32)
    vm = lambda *s: pltpu.VMEM(s, f32)
    dma = lambda *s: pltpu.SemaphoreType.DMA(s)
    group = devices // 2
    planes = n // 2
    nb = local // LANES
    assert group * 4 == 8 * slices and nb % UNITS == 0 and plane % (nb // UNITS * LANES) == 0
    rims = plane // (nb // UNITS * LANES)
    blocks = (nb, slices, 3, 2, 3, 2, LANES)
    fields, theta = call(
        functools.partial(spread_kernel, n, group),
        1,
        (shape(group * nb + 1, 4, LANES), shape(slices, LANES)),
        [
            *[vm(count, *blocks[1:]) for count in [1] + [nb // UNITS] * (UNITS - 1) + [nb // UNITS - 1]],
            vm(3, 8, slices, local), vm(8, slices, plane), vm(8, slices, LANES), vm(8, slices, LANES),
            vm(group, nb, 4, LANES), dma(nb), dma(rims + 2), dma(rims + 2),
            dma(UNITS, group), dma(UNITS, group), dma(group), dma(1),
        ],
        links,
        in_specs=[ANY],
    )
    smooth = call(
        functools.partial(solve_kernel, n, group),
        2,
        shape(8, slices, local),
        [
            vm(plane, LANES), vm(plane, LANES), vm(4 * planes, plane), vm(8, plane), vm(8, plane),
            vm(8, LANES), vm(8, LANES), vm(group * nb + 1, 4, LANES), vm(group, nb, 4, LANES), vm(group, 1, 4, LANES),
            dma(PIECES + 1), dma(PIECES + 1), dma(UNITS, group), dma(UNITS, group), dma(1), dma(group),
        ],
        fields, *decay_tables(n, planes), wide(hartley(n)), wide(hartley(n, 1)), wide(hartley(n, 1).T), *zero_tables(n, planes),
    )
    times = lax.axis_size("tm")
    scales = (1.0 / (slices * times * n**3), 1.0 / n**3)
    placed, total, shares = call(
        functools.partial(link_kernel, n, scales),
        3,
        (shape(*blocks), shape(1, 1), shape(1, slices)),
        [
            vm(*blocks), vm(8, slices, plane), vm(8, slices, LANES), vm(18, slices, local + plane + LANES),
            vm(slices, LANES), vm(devices, slices, LANES), dma(nb), dma(rims + 1), dma(rims + 1),
            dma(devices), dma(devices),
        ],
        links, smooth, theta,
        in_specs=[ANY, VM, VM],
        limit=LINK_MB,
    )
    new_links = pl.pallas_call(
        place_kernel,
        out_shape=shape(*links.shape),
        in_specs=[VM],
        out_specs=ANY,
        scratch_shapes=[dma(nb)],
        compiler_params=pltpu.CompilerParams(vmem_limit_bytes=8 * 1024 * 1024),
    )(placed)
    total = total.reshape(())
    if times > 1:
        total = lax.psum(total, "tm")
    return (new_links, total, shares.reshape(slices))


def solution(mesh):
    placed = (P("tm", None, None, None, None, "space"),)
    return jax.shard_map(
        body,
        mesh=mesh,
        in_specs=placed,
        out_specs=(P("tm", None, None, None, None, "space"), P(), P("tm")),
        check_vma=False,
    )
```

```python
import functools
import math

import jax
import jax.numpy as jnp
from jax import lax
from jax.experimental import pallas as pl
from jax.experimental.pallas import tpu as pltpu
from jax.sharding import PartitionSpec as P

EXTENT = 48
LANES = 128
UNITS = 3
PIECES = 6
COST = 10**9
GAUGE_KB = 50 * 1000

root_three = math.sqrt(3.0)
step_size = 0.08
top_momentum = 12.0

f32 = jnp.float32
bf16 = jnp.bfloat16
MESH = pl.DeviceIdType.MESH
VM = pl.BlockSpec(memory_space=pltpu.VMEM)


def cmul(p, q):
    return (p[0] * q[0] - p[1] * q[1], p[0] * q[1] + p[1] * q[0])


def cadd(p, q):
    return (p[0] + q[0], p[1] + q[1])


def csub(p, q):
    return (p[0] - q[0], p[1] - q[1])


def conj(p):
    return (p[0], -p[1])


def conj_mul(p, q):
    return (p[0] * q[0] + p[1] * q[1], p[0] * q[1] - p[1] * q[0])


def mul_conj(p, q):
    return (p[0] * q[0] + p[1] * q[1], p[1] * q[0] - p[0] * q[1])


def dot_row(row, col, mul):
    out = mul(row[0], col[0])
    for k in (1, 2):
        out = cadd(out, mul(row[k], col[k]))
    return out


def cross_conj(a, b):
    return [
        conj(csub(cmul(a[(k + 1) % 3], b[(k + 2) % 3]), cmul(a[(k + 2) % 3], b[(k + 1) % 3])))
        for k in range(3)
    ]


def algebra_of(u):
    return [
        u[0][1][1] + u[1][0][1],
        u[0][1][0] - u[1][0][0],
        u[0][0][1] - u[1][1][1],
        u[0][2][1] + u[2][0][1],
        u[0][2][0] - u[2][0][0],
        u[1][2][1] + u[2][1][1],
        u[1][2][0] - u[2][1][0],
        (u[0][0][1] + u[1][1][1] - 2.0 * u[2][2][1]) * (1.0 / root_three),
    ]


def rotation_of(s):
    h = 0.5 * step_size
    s = [v * h for v in s]
    third = s[7] * (1.0 / root_three)
    d0, d1, d2 = s[2] + third, third - s[2], -2.0 * third
    herm = [
        [(d0, None), (s[0], -s[1]), (s[3], -s[4])],
        [(s[0], s[1]), (d1, None), (s[5], -s[6])],
        [(s[3], s[4]), (s[5], s[6]), (d2, None)],
    ]

    def mul(p, q):
        if p[1] is None and q[1] is None:
            return (p[0] * q[0], jnp.zeros_like(p[0]))
        if p[1] is None:
            return (p[0] * q[0], p[0] * q[1])
        if q[1] is None:
            return (p[0] * q[0], p[1] * q[0])
        return cmul(p, q)

    rows = []
    for i in range(2):
        row = []
        for j in range(3):
            sq = dot_row(herm[i], [herm[k][j] for k in range(3)], mul)
            re, im = -0.5 * sq[0], -0.5 * sq[1]
            if herm[i][j][1] is not None:
                re = re - herm[i][j][1]
            else:
                re = re + 1.0
            row.append((re, im + herm[i][j][0]))
        rows.append(row)

    def unit(row):
        inv = lax.rsqrt(sum(p[0] * p[0] + p[1] * p[1] for p in row))
        return [(p[0] * inv, p[1] * inv) for p in row]

    one = unit(rows[0])
    corr = dot_row(one, rows[1], conj_mul)
    two = unit([csub(rows[1][k], cmul(corr, one[k])) for k in range(3)])
    return [one, two, cross_conj(one, two)]


def block(k):
    return pl.ds(pl.multiple_of(k * LANES, LANES), LANES)


def lane_ids(rows=8):
    return lax.broadcasted_iota(jnp.int32, (rows, LANES), 1)


def rows_of(slices, d, r, c, p):
    return pl.ds((d * 2 + r) * 6 + c * 2 + p, slices, stride=36)


def flat_block(ref, k):
    return ref.at[k].reshape(ref.shape[1] * 36, LANES)


def load_link(ref, slices, d):
    rows = [[tuple(ref[rows_of(slices, d, r, c, p), :] for p in range(2)) for c in range(3)] for r in range(2)]
    return rows + [cross_conj(rows[0], rows[1])]


def site_of(k, extent):
    start = k * LANES
    shifted = lane_ids() + lax.rem(start, extent)
    wraps = sum((shifted >= extent * i).astype(jnp.int32) for i in range(1, (LANES + extent - 1) // extent + 1))
    return shifted - extent * wraps, lax.div(start, extent) + wraps


def at_z(row, z, me, rows, extent):
    first = lax.rem(extent + z + 1 - lax.rem(me * rows, extent), extent)
    hit = row == first
    for i in range(1, -(-rows // extent)):
        hit = hit | (row == first + i * extent)
    return hit


def fetch_block(links, held, sem, k, start=0):
    return pltpu.make_async_copy(links.at[:, :, :, :, :, pl.ds(k * LANES, LANES)], held.at[k - start], sem.at[k])


def split3(x):
    hi = x.astype(bf16)
    lo = (x - hi.astype(f32)).astype(bf16)
    return jnp.concatenate([hi, lo, hi], axis=0)


def transform(table, parts):
    both = jnp.dot(table, split3(jnp.concatenate(parts, axis=1)), preferred_element_type=f32)
    return [both[:, i * LANES : (i + 1) * LANES] for i in range(len(parts))]


def swap(v):
    return pltpu.roll(v, 4, 0)


def flip(place, i, group):
    other = place
    for b in range(group.bit_length() - 1):
        if i >> b & 1:
            other = other + (1 << b) * (1 - 2 * lax.rem(lax.div(place, 1 << b), 2))
    return other


def iota(shape, axis):
    return lax.broadcasted_iota(jnp.int32, shape, axis).astype(f32)


def divide(v, n):
    whole = jnp.floor((v + 0.5) * (1.0 / n))
    return whole, v - n * whole


def make_tables(n, planes, wave, tables, zero):
    shape = (n, 3 * n)
    row = iota(shape, 0)
    third, col = divide(iota(shape, 1), n)
    for i, turn in enumerate([row * col, row * (col + (n - 1.0)), col * (row + (n - 1.0))]):
        angle = divide(turn, n)[1] * (2.0 * math.pi / n)
        full = (jnp.cos(angle) + jnp.sin(angle)) * (1.0 / math.sqrt(n))
        high = full.astype(bf16).astype(f32)
        tables[i] = jnp.where(third == 2.0, full - high, high).astype(bf16)
    mode = iota((8, n * n), 1)
    p = jnp.zeros((8, n * n), f32)
    for k in divide(mode, n):
        s = jnp.sin(k * (math.pi / n))
        p = p + 4.0 * s * s
    p = jnp.where(mode == 0.0, 1.0, p)
    root = jnp.sqrt(p + 0.25 * p * p)
    mu = 1.0 / (1.0 + 0.5 * p + root)
    power = lax.integer_pow(mu, planes)
    close = 1.0 / (1.0 - power * power)
    for i, v in enumerate([mu, (0.5 * top_momentum) / root, close, close * power]):
        wave[i] = jnp.where(mode == 0.0, 0.0, v)
    square = (LANES, LANES)
    source, sub = divide(iota(square, 0), 4)
    target, lane = divide(iota(square, 1), 4)
    used = (sub == lane) & (source < planes) & (target < planes)
    for i in range(2):
        d = divide(target - source + (n + i * planes * 1.0), n)[1]
        green = top_momentum * ((n * n - 1.0) / (12.0 * n) - d * (n - d) * (0.5 / n))
        zero[i] = jnp.where(used, green, 0.0)


def link_part(extent, held, smooth, arrive, done, above, below, rot, halo_send, halo_recv, n):
    nb, slices = held.shape[0], held.shape[1]
    yb = extent * extent // LANES
    unit = nb // UNITS
    q = nb * LANES // extent
    mid = (extent // 2) * extent
    lane = lane_ids()
    me = lax.axis_index("space")
    ahead, behind = lax.rem(me + 1, n), lax.rem(me + n - 1, n)
    def rotate(values, sl):
        g = rotation_of(values)
        for i in range(3):
            for j in range(3):
                for p in range(2):
                    rot[6 * i + 2 * j + p, :, sl] = g[i][j][p]

    def rotate_own(k, carry):
        rotate([smooth[a, :, block(k)] for a in range(8)], block(k))
        return carry

    def rotate_above(k, carry):
        rotate([above[a, :, block(k)] for a in range(8)], block(nb + k))
        return carry

    def halo(i, source, dest, other):
        return pltpu.make_async_remote_copy(
            src_ref=source,
            dst_ref=dest,
            send_sem=halo_send.at[i],
            recv_sem=halo_recv.at[i],
            device_id={"space": other},
            device_id_type=MESH,
        )

    def span(start, size):
        return pl.ds(pl.multiple_of(start * LANES, LANES), size * LANES)

    odd = lax.rem(me, 2)
    pick = yb - odd * (yb - mid // LANES)
    below_copy = halo(0, smooth.at[:, :, span(pick, 1)], below, ahead)
    rims = [
        halo(1 + i, smooth.at[:, :, span(i * unit, unit)], above.at[:, :, span(i * unit, unit)], behind)
        for i in range(yb // unit)
    ]

    for v in range(UNITS):
        arrive(v)
        lax.fori_loop(v * unit, (v + 1) * unit, rotate_own, 0)
        if v < len(rims):
            rims[v].start()
    below_copy.start()

    def step(which, k, total):
        sl = block(k)
        before = block(jnp.maximum(k - 1, 0))
        after = block(k + 1)
        wrap = block(jnp.where(k == yb, 0, nb + yb))
        x_at, row = site_of(k, extent)
        edge_x = x_at == extent - 1
        edge_z = at_z(row, extent - 1, me, q, extent)

        def ahead_x(e):
            cur = rot[e, :, sl]
            near = pltpu.roll(jnp.where(lane == 0, rot[e, :, after], cur), LANES - 1, 1)
            far = pltpu.roll(jnp.where(lane >= LANES - extent + 1, rot[e, :, before], cur), extent - 1, 1)
            return jnp.where(edge_x, far, near)

        def ahead_y(e):
            return rot[e, :, block(k + yb)]

        def ahead_z(e):
            cur = rot[e, :, sl]
            near = pltpu.roll(jnp.where(lane < extent, rot[e, :, after], cur), LANES - extent, 1)
            far = pltpu.roll(rot[e, :, wrap], LANES - extent, 1)
            return jnp.where(edge_z, far, near)

        flat_out = flat_block(done, k)
        for d in which:
            forward = (ahead_x, ahead_y, ahead_z)[d]
            u = load_link(flat_block(held, k), slices, d)
            own = [[(rot[6 * i + 2 * j, :, sl], rot[6 * i + 2 * j + 1, :, sl]) for j in range(3)] for i in range(2)]
            left = [
                [dot_row(own[i], [u[k2][j] for k2 in range(3)], cmul) for j in range(3)]
                for i in range(2)
            ]
            made = []
            for j in range(3):
                row3 = [(forward(6 * j + 2 * c), forward(6 * j + 2 * c + 1)) for c in range(3)]
                for i in range(2):
                    v = dot_row(left[i], row3, mul_conj)
                    flat_out[rows_of(slices, d, i, j, 0), :] = v[0]
                    flat_out[rows_of(slices, d, i, j, 1), :] = v[1]
                    if j < 2:
                        made.append(v)
            p00, p10, p01, p11 = made
            minor = csub(cmul(p00, p11), cmul(p01, p10))[0]
            total = total + ((1.0 - p00[0]) + (1.0 - p11[0]) + (1.0 - minor))
        return total

    total = jnp.zeros((8, LANES), f32)
    total = lax.fori_loop(1, nb - yb, functools.partial(step, (0, 1, 2)), total)
    below_copy.wait_recv()
    rotate([below[a] for a in range(8)], block(nb + yb))
    total = lax.fori_loop(0, 1, functools.partial(step, (0, 1, 2)), total)
    total = lax.fori_loop(nb - yb, nb - 1, functools.partial(step, (0, 2)), total)
    for i, copy in enumerate(rims):
        copy.wait_recv()
        lax.fori_loop(i * unit, (i + 1) * unit, rotate_above, 0)
        last = i == len(rims) - 1
        total = lax.fori_loop(nb - yb + i * unit, nb - yb + (i + 1) * unit - last, functools.partial(step, (1,)), total)
    total = lax.fori_loop(nb - 1, nb, functools.partial(step, (0, 1, 2)), total)
    for copy in [below_copy] + rims:
        copy.wait_send()
    return total


def gauge_kernel(
    extent, group, scales, links, done, out_theta, out_deficit, *refs
):
    (
        held_links, smooth, above, below, rot, sum_row, sums, late_send, late_recv, sum_send, sum_recv,
        alg, y_rim, z_below, z_above, mine, fields, load_sem, halo_send, halo_recv,
        in_send_sem, in_recv_sem, in_edge_send, in_edge_recv,
        wave, tables, zero, one, two, modes, ends, far, mode, far_mode, outgo, held, edge_held,
        end_send, end_recv, send_sem, recv_sem, edge_send, edge_recv,
    ) = refs
    devices = 2 * group
    nb, slices = mine.shape[1], alg.shape[2]
    yb = extent * extent // LANES
    half = slices // 2
    unit = nb // UNITS
    q = nb * LANES // extent
    mid = (extent // 2) * extent
    lane = lane_ids()
    me = lax.axis_index("space")
    place = lax.rem(me, group)
    base = me - place
    beyond = group - base
    ahead, behind = lax.rem(me + 1, devices), lax.rem(me + devices - 1, devices)
    in_spans = [(0, 1)] + [(i * unit, (i + 1) * unit) for i in range(1, UNITS)] + [(1, unit)]
    in_loads = [[fetch_block(links, held_links, load_sem, k) for k in range(a, b)] for a, b in in_spans]
    for copy in sum(in_loads, []):
        copy.start()
    barrier = greet([base + flip(place, i, group) for i in range(1, group)] + [beyond + i for i in range(group)])

    make_tables(extent, extent // 2, wave, tables, zero)

    def algebra(i):
        start, stop = in_spans[i]

        def step(k, carry):
            flat = flat_block(held_links, k)
            for d in range(3):
                for a, v in enumerate(algebra_of(load_link(flat, slices, d))):
                    alg[d, a, :, block(k)] = v
            return carry

        for copy in in_loads[i]:
            copy.wait()
        lax.fori_loop(start, stop, step, 0)

    def halo(i, source, dest, other):
        return pltpu.make_async_remote_copy(
            src_ref=source,
            dst_ref=dest,
            send_sem=halo_send.at[i],
            recv_sem=halo_recv.at[i],
            device_id={"space": other},
            device_id_type=MESH,
        )

    def span(start, size):
        return pl.ds(pl.multiple_of(start * LANES, LANES), size * LANES)

    first = nb - yb
    rims = [
        halo(i, alg.at[1, :, :, span(first + i * unit, unit)], y_rim.at[:, :, span(i * unit, unit)], ahead)
        for i in range(yb // unit)
    ]
    below_copy = halo(len(rims), alg.at[2, :, :, span(nb - 1, 1)], z_below, ahead)
    odd = lax.rem(me, 2)
    above_copy = halo(len(rims) + 1, alg.at[2, :, :, span(odd * (mid // LANES), 1)], z_above, behind)

    algebra(0)
    algebra(1)
    pl.semaphore_wait(barrier, devices - 1)
    above_copy.start()
    rims[0].start()
    for i in range(1, len(rims)):
        algebra(1 + i)
        if i == len(rims) - 1:
            below_copy.start()
        rims[i].start()
    algebra(UNITS)

    def step(from_rim, k, total):
        sl = block(k)
        before = block(jnp.maximum(k - 1, 0))
        after = block(jnp.minimum(k + 1, nb - 1))
        x_at, row = site_of(k, extent)
        edge_x = x_at == 0
        edge_z = at_z(row, 0, me, q, extent)
        for a in range(8):
            x, y, z = alg[0, a, :, sl], alg[1, a, :, sl], alg[2, a, :, sl]
            near = pltpu.roll(jnp.where(lane == LANES - 1, alg[0, a, :, before], x), 1, 1)
            far = pltpu.roll(jnp.where(lane < extent - 1, alg[0, a, :, after], x), LANES - extent + 1, 1)
            bx = jnp.where(edge_x, far, near)
            by = y_rim[a, :, sl] if from_rim else alg[1, a, :, block(k - yb)]
            prev = jnp.where(k == 0, z_below[a], alg[2, a, :, before])
            near = pltpu.roll(jnp.where(lane >= LANES - extent, prev, z), extent, 1)
            far = pltpu.roll(jnp.where(k == 0, alg[2, a, :, block(yb)], z_above[a]), extent, 1)
            bz = jnp.where(edge_z, far, near)
            b = (bx - x) + (by - y) + (bz - z)
            total = total + b * b
            mine[2 * a, k] = b[:half]
            mine[2 * a + 1, k] = b[half:]
        return total

    def in_edge_copy(i):
        return pltpu.make_async_remote_copy(
            src_ref=mine.at[i, pl.ds(0, 1)],
            dst_ref=fields.at[pl.ds(group * nb, 1)],
            send_sem=in_edge_send.at[i],
            recv_sem=in_edge_recv.at[0],
            device_id={"space": beyond + i},
            device_id_type=MESH,
        )

    total = jnp.zeros((8, LANES), f32)
    in_copies = []
    above_copy.wait_recv()
    below_copy.wait_recv()
    for c in [UNITS - 1] + list(range(UNITS - 1)):
        if c < len(rims):
            rims[c].wait_recv()
        total = lax.fori_loop(c * unit, (c + 1) * unit, functools.partial(step, c < len(rims)), total)
        if c == 0:

            @pl.when(place == 0)
            def _():
                for i in range(group):
                    in_edge_copy(i).start()

        for i in reversed(range(1, group)):
            other = flip(place, i, group)
            copy = pltpu.make_async_remote_copy(
                src_ref=mine.at[other, pl.ds(c * unit, unit)],
                dst_ref=fields.at[pl.ds(place * nb + c * unit, unit)],
                send_sem=in_send_sem.at[c, i],
                recv_sem=in_recv_sem.at[c, i],
                device_id={"space": base + other},
                device_id_type=MESH,
            )
            copy.start()
            in_copies.append(copy)
    theta = total

    def keep(k, carry):
        fields[place * nb + k] = mine[place, k]
        return carry

    lax.fori_loop(0, nb, keep, 0)
    for copy in rims + [below_copy, above_copy]:
        copy.wait_send()
    for copy in in_copies:
        copy.wait()
    in_edge_copy(0).wait_recv()

    @pl.when(place == 0)
    def _():
        for i in range(group):
            in_edge_copy(i).wait_send()

    n = extent
    planes = group * nb * LANES // (n * n)
    columns = n * n // LANES
    pairs = planes // 2
    lanes = planes * 4
    per = columns // PIECES
    upper = lax.broadcasted_iota(jnp.int32, (8, LANES), 0) >= 4
    x_table, z_table, z_back = (tables.at[i] for i in range(3))
    decay, weight = wave.at[0], wave.at[1]
    close = wave.at[pl.ds(2, 2)]
    own_zero, far_zero = zero.at[0], zero.at[1]
    def rows_at(i):
        return pl.ds(pl.multiple_of(i * n, 8), n)

    def turn_in(c, extra):
        tiles = [fields[y * columns + c] for y in range(planes)] + extra
        rest = LANES - 4 * len(tiles)
        full = jnp.concatenate(tiles + [jnp.zeros((rest, LANES), f32)], axis=0)
        one[block(c), :] = full.T

    def turn_rest(c, carry):
        turn_in(c, [])
        return carry

    lax.fori_loop(0, columns, turn_rest, 0, unroll=3)
    turn_in(0, [fields[planes * columns]])
    one[0:n, :] = pltpu.roll(one[0:n, :], LANES - 4, 1)
    def along_x(i, carry):
        parts = [one[rows_at(2 * i + e), :] for e in range(2)]
        for e, v in enumerate(transform(x_table[...], parts)):
            two[rows_at(2 * i + e), :] = v
        return carry

    lax.fori_loop(0, n // 2, along_x, 0, unroll=4)

    def along_z(i, carry):
        parts = [two[pl.ds(2 * i + e, n, stride=n), :] for e in range(2)]
        for e, v in enumerate(transform(z_table[...], parts)):
            one[rows_at(2 * i + e), :] = v
        return carry

    def end_copy(p):
        cols = pl.ds(p * per * LANES, per * LANES)
        return pltpu.make_async_remote_copy(
            src_ref=ends.at[:, cols],
            dst_ref=far.at[:, cols],
            send_sem=end_send.at[p],
            recv_sem=end_recv.at[p],
            device_id={"space": beyond + place},
            device_id_type=MESH,
        )

    mode_copy = pltpu.make_async_remote_copy(
        src_ref=mode,
        dst_ref=far_mode,
        send_sem=end_send.at[PIECES],
        recv_sem=end_recv.at[PIECES],
        device_id={"space": beyond + place},
        device_id_type=MESH,
    )

    def reduce_ends(c, carry):
        sl = block(c)
        modes[:, sl] = one[sl, :].T[:lanes]
        mu = decay[:, sl]
        mu2 = mu * mu
        low = jnp.where(upper, 1.0, mu)
        high = jnp.where(upper, mu, 1.0)
        fwd = modes[0:8, sl]
        bwd = modes[lanes - 8 : lanes, sl]
        for i in range(1, pairs):
            fwd = fwd * mu2 + modes[8 * i : 8 * i + 8, sl]
            bwd = bwd * mu2 + modes[lanes - 8 - 8 * i : lanes - 8 * i, sl]
        ends[:, sl] = jnp.where(upper, high * bwd + low * swap(bwd), low * fwd + high * swap(fwd))
        return carry

    step_z = n // 2 // PIECES
    for p in range(PIECES):
        lax.fori_loop(p * step_z, (p + 1) * step_z, along_z, 0, unroll=4)
        if p == 0:
            mode[...] = one[0:8, :]
        lax.fori_loop(p * per, (p + 1) * per, reduce_ends, 0, unroll=per)
        if p == 0:
            mode_copy.start()
        end_copy(p).start()

    def sweep(c, carry):
        sl = block(c)
        mu = decay[:, sl]
        mu2 = mu * mu
        low = jnp.where(upper, 1.0, mu)
        high = jnp.where(upper, mu, 1.0)
        total = close[0, :, sl] * far[:, sl] + close[1, :, sl] * ends[:, sl]
        turned = swap(total)
        e = jnp.where(upper, turned, total)
        f = jnp.where(upper, total, turned) * mu
        w = weight[:, sl]
        up = mu * high
        down = jnp.where(upper, 0.0, mu)
        rising = []
        for i in range(pairs):
            v = modes[8 * i : 8 * i + 8, sl]
            s = low * v + high * swap(v)
            rising.append(jnp.where(upper, s, v) + up * e)
            e = mu2 * e + s
        done = [None] * pairs
        for i in reversed(range(pairs)):
            v = modes[8 * i : 8 * i + 8, sl]
            t = swap(v)
            done[i] = w * (rising[i] + low * f + down * t)
            f = mu2 * f + mu * (high * v + low * t)
        full = jnp.concatenate(done + [jnp.zeros((LANES - lanes, LANES), f32)], axis=0)
        one[sl, :] = full.T
        return carry

    def back_z(i, carry):
        parts = [one[rows_at(2 * i + e), :] for e in range(2)]
        for e, v in enumerate(transform(z_back[...], parts)):
            two[pl.ds(2 * i + e, n, stride=n), :] = v
        return carry

    for p in range(PIECES):
        end_copy(p).wait_recv()
        if p == 0:
            mode_copy.wait_recv()
        lax.fori_loop(p * per, (p + 1) * per, sweep, 0, unroll=per)
        if p == 0:
            exact = functools.partial(jnp.dot, preferred_element_type=f32, precision=lax.Precision.HIGHEST)
            flat = exact(mode[...], own_zero[...]) + exact(far_mode[...], far_zero[...])
            first = lax.broadcasted_iota(jnp.int32, (8, LANES), 0) == 0
            one[0:8, :] = jnp.where(first, flat, one[0:8, :])
        lax.fori_loop(p * step_z, (p + 1) * step_z, back_z, 0, unroll=4)

    def back_x(i, carry):
        parts = [two[rows_at(2 * i + e), :] for e in range(2)]
        for e, v in enumerate(transform(x_table[...], parts)):
            one[rows_at(2 * i + e), :] = v
        return carry

    def turn_out(c):
        full = one[block(c), :].T
        for y in range(planes):
            outgo[y * columns + c] = full[4 * y : 4 * y + 4]
        return full

    def turn_out_rest(c, carry):
        turn_out(c)
        return carry

    def unit_copy(i, v):
        other = flip(place, i, group)
        return pltpu.make_async_remote_copy(
            src_ref=outgo.at[pl.ds(other * nb + v * unit, unit)],
            dst_ref=held.at[place, pl.ds(v * unit, unit)],
            send_sem=send_sem.at[v, i],
            recv_sem=recv_sem.at[v, i],
            device_id={"space": base + other},
            device_id_type=MESH,
        )

    edge_copy = pltpu.make_async_remote_copy(
        src_ref=outgo.at[pl.ds(planes * columns, 1)],
        dst_ref=edge_held.at[place],
        send_sem=edge_send.at[0],
        recv_sem=edge_recv.at[place],
        device_id={"space": beyond},
        device_id_type=MESH,
    )

    for side in range(2):
        lax.fori_loop(side * n // 4, (side + 1) * n // 4, back_x, 0, unroll=4)
        if side == 0:
            one[0:n, :] = pltpu.roll(one[0:n, :], 4, 1)
            outgo[planes * columns] = turn_out(0)[lanes : lanes + 4]
        lax.fori_loop(side * unit, (side + 1) * unit, turn_out_rest, 0, unroll=3)
        if side == 0:
            edge_copy.start()
        for i in reversed(range(1, group)):
            odd = lax.rem(place + i + side, 2)
            unit_copy(i, odd).start()

            @pl.when(odd == 0)
            def _():
                unit_copy(i, 2).start()

    def keep(k, carry):
        held[place, k] = outgo[place * nb + k]
        return carry

    lax.fori_loop(0, nb, keep, 0)
    for p in range(PIECES):
        end_copy(p).wait_send()
    mode_copy.wait_send()
    if True:
        edge_copy.wait_send()

    def edge_wait():
        @pl.when(place == 0)
        def _():
            for i in range(group):
                pltpu.make_async_remote_copy(
                    src_ref=outgo.at[pl.ds(planes * columns, 1)],
                    dst_ref=edge_held.at[i],
                    send_sem=edge_send.at[0],
                    recv_sem=edge_recv.at[i],
                    device_id={"space": beyond},
                    device_id_type=MESH,
                ).wait_recv()
            for a in range(8):
                row = jnp.concatenate([edge_held[2 * a, 0], edge_held[2 * a + 1, 0]], axis=0)
                smooth[a, :, 0:LANES] = jnp.where(lane_ids() < n, row, smooth[a, :, 0:LANES])

    def gather(k, carry):
        for a in range(8):
            smooth[a, :, block(k)] = jnp.concatenate([held[2 * a, k], held[2 * a + 1, k]], axis=0)
        return carry

    def arrive(v):
        for i in reversed(range(1, group)):
            unit_copy(i, v).wait()
        lax.fori_loop(v * unit, (v + 1) * unit, gather, 0)
        if v == 0:
            edge_wait()

    total = link_part(extent, held_links, smooth, arrive, done, above, below, rot, late_send, late_recv, devices)

    wide_lane = lane_ids(slices)
    t = jnp.sum(jnp.sum(theta, axis=1, keepdims=True), axis=0, keepdims=True)
    d = jnp.sum(total, axis=1, keepdims=True)
    own_row = lax.broadcasted_iota(jnp.int32, (slices, LANES), 0)
    spread = jnp.where(
        wide_lane == own_row, d, jnp.where(wide_lane == slices, jnp.where(own_row == 0, t, 0.0), 0.0)
    )
    sum_row[...] = jnp.sum(spread, axis=0, keepdims=True)
    copies = []
    for i in range(1, devices):
        copy = pltpu.make_async_remote_copy(
            src_ref=sum_row,
            dst_ref=sums.at[i],
            send_sem=sum_send.at[i],
            recv_sem=sum_recv.at[i],
            device_id={"space": lax.rem(me + i, devices)},
            device_id_type=MESH,
        )
        copy.start()
        copies.append(copy)
    for copy in copies:
        copy.wait()
    row = sum_row[...]
    for i in range(1, devices):
        row = row + sums[i]
    out_deficit[...] = row[:, :slices] * scales[1]
    out_theta[...] = row[:, slices : slices + 1] * scales[0]


def place_kernel(blocks, out, sem):
    copies = [
        pltpu.make_async_copy(blocks.at[k], out.at[:, :, :, :, :, pl.ds(k * LANES, LANES)], sem.at[k])
        for k in range(blocks.shape[0])
    ]
    for copy in copies:
        copy.start()
    for copy in copies:
        copy.wait()


def greet(others):
    barrier = pltpu.get_barrier_semaphore()
    for other in others:
        pl.semaphore_signal(barrier, inc=1, device_id={"space": other}, device_id_type=MESH)
    return barrier


ANY = pl.BlockSpec(memory_space=pl.ANY)
HBM = pl.BlockSpec(memory_space=pltpu.HBM)


def call(kernel, number, out_shape, scratch, *args, in_specs=None, out_specs=None, limit=0):
    return pl.pallas_call(
        kernel,
        out_shape=out_shape,
        in_specs=in_specs or [VM] * len(args),
        out_specs=out_specs or jax.tree.map(lambda _: VM, out_shape),
        scratch_shapes=scratch,
        cost_estimate=pl.CostEstimate(flops=COST, bytes_accessed=COST // 1000, transcendentals=0),
        compiler_params=pltpu.CompilerParams(
            collective_id=number, has_side_effects=True, vmem_limit_bytes=limit * 1024
        ),
    )(*args)


def body(links):
    n = EXTENT
    slices, local = links.shape[0], links.shape[-1]
    devices = lax.axis_size("space")
    plane = n * n
    shape = lambda *s: jax.ShapeDtypeStruct(s, f32)
    vm = lambda *s: pltpu.VMEM(s, f32)
    dma = lambda *s: pltpu.SemaphoreType.DMA(s)
    group = devices // 2
    planes = n // 2
    nb = local // LANES
    assert group * 4 == 8 * slices and nb % UNITS == 0 and plane % (nb // UNITS * LANES) == 0
    rims = plane // (nb // UNITS * LANES)
    blocks = (nb, slices, 3, 2, 3, 2, LANES)
    times = lax.axis_size("tm")
    scales = (1.0 / (slices * times * n**3), 1.0 / n**3)
    placed, total, shares = call(
        functools.partial(gauge_kernel, n, group, scales),
        1,
        (shape(*blocks), shape(1, 1), shape(1, slices)),
        [
            vm(*blocks), vm(8, slices, local), vm(8, slices, plane), vm(8, slices, LANES),
            vm(18, slices, local + plane + LANES), vm(1, LANES), vm(devices, 1, LANES),
            dma(rims + 1), dma(rims + 1), dma(devices), dma(devices),
            vm(3, 8, slices, local), vm(8, slices, plane), vm(8, slices, LANES), vm(8, slices, LANES),
            vm(group, nb, 4, LANES), vm(group * nb + 1, 4, LANES), dma(nb), dma(rims + 2), dma(rims + 2),
            dma(UNITS, group), dma(UNITS, group), dma(group), dma(1),
            vm(4, 8, plane), pltpu.VMEM((3, n, 3 * n), bf16), vm(2, LANES, LANES),
            vm(plane, LANES), vm(plane, LANES), vm(4 * planes, plane), vm(8, plane), vm(8, plane),
            vm(8, LANES), vm(8, LANES), vm(group * nb + 1, 4, LANES), vm(group, nb, 4, LANES), vm(group, 1, 4, LANES),
            dma(PIECES + 1), dma(PIECES + 1), dma(UNITS, group), dma(UNITS, group), dma(1), dma(group),
        ],
        links,
        in_specs=[HBM],
        limit=GAUGE_KB,
    )
    new_links = pl.pallas_call(
        place_kernel,
        out_shape=shape(*links.shape),
        in_specs=[VM],
        out_specs=ANY,
        scratch_shapes=[dma(nb)],
        compiler_params=pltpu.CompilerParams(vmem_limit_bytes=8 * 1024 * 1024),
    )(placed)
    total = total.reshape(())
    if times > 1:
        total = lax.psum(total, "tm")
    return (new_links, total, shares.reshape(slices))


def solution(mesh):
    placed = (P("tm", None, None, None, None, "space"),)
    return jax.shard_map(
        body,
        mesh=mesh,
        in_specs=placed,
        out_specs=(P("tm", None, None, None, None, "space"), P(), P("tm")),
        check_vma=False,
    )
```

```python
import functools
import math

import jax
import jax.numpy as jnp
from jax import lax
from jax.experimental import pallas as pl
from jax.experimental.pallas import tpu as pltpu
from jax.sharding import PartitionSpec as P

EXTENT = 48
LANES = 128
UNITS = 3
PIECES = 6
COST = 10**9
GAUGE_KB = 50 * 1000

root_three = math.sqrt(3.0)
step_size = 0.08
top_momentum = 12.0

f32 = jnp.float32
bf16 = jnp.bfloat16
MESH = pl.DeviceIdType.MESH
VM = pl.BlockSpec(memory_space=pltpu.VMEM)


def cmul(p, q):
    return (p[0] * q[0] - p[1] * q[1], p[0] * q[1] + p[1] * q[0])


def cadd(p, q):
    return (p[0] + q[0], p[1] + q[1])


def csub(p, q):
    return (p[0] - q[0], p[1] - q[1])


def conj(p):
    return (p[0], -p[1])


def conj_mul(p, q):
    return (p[0] * q[0] + p[1] * q[1], p[0] * q[1] - p[1] * q[0])


def mul_conj(p, q):
    return (p[0] * q[0] + p[1] * q[1], p[1] * q[0] - p[0] * q[1])


def dot_row(row, col, mul):
    out = mul(row[0], col[0])
    for k in (1, 2):
        out = cadd(out, mul(row[k], col[k]))
    return out


def cross_conj(a, b):
    return [
        conj(csub(cmul(a[(k + 1) % 3], b[(k + 2) % 3]), cmul(a[(k + 2) % 3], b[(k + 1) % 3])))
        for k in range(3)
    ]


def algebra_of(u):
    return [
        u[0][1][1] + u[1][0][1],
        u[0][1][0] - u[1][0][0],
        u[0][0][1] - u[1][1][1],
        u[0][2][1] + u[2][0][1],
        u[0][2][0] - u[2][0][0],
        u[1][2][1] + u[2][1][1],
        u[1][2][0] - u[2][1][0],
        (u[0][0][1] + u[1][1][1] - 2.0 * u[2][2][1]) * (1.0 / root_three),
    ]


def rotation_of(s):
    h = 0.5 * step_size
    s = [v * h for v in s]
    third = s[7] * (1.0 / root_three)
    d0, d1, d2 = s[2] + third, third - s[2], -2.0 * third
    herm = [
        [(d0, None), (s[0], -s[1]), (s[3], -s[4])],
        [(s[0], s[1]), (d1, None), (s[5], -s[6])],
        [(s[3], s[4]), (s[5], s[6]), (d2, None)],
    ]

    def mul(p, q):
        if p[1] is None and q[1] is None:
            return (p[0] * q[0], jnp.zeros_like(p[0]))
        if p[1] is None:
            return (p[0] * q[0], p[0] * q[1])
        if q[1] is None:
            return (p[0] * q[0], p[1] * q[0])
        return cmul(p, q)

    rows = []
    for i in range(2):
        row = []
        for j in range(3):
            sq = dot_row(herm[i], [herm[k][j] for k in range(3)], mul)
            re, im = -0.5 * sq[0], -0.5 * sq[1]
            if herm[i][j][1] is not None:
                re = re - herm[i][j][1]
            else:
                re = re + 1.0
            row.append((re, im + herm[i][j][0]))
        rows.append(row)

    def unit(row):
        inv = lax.rsqrt(sum(p[0] * p[0] + p[1] * p[1] for p in row))
        return [(p[0] * inv, p[1] * inv) for p in row]

    one = unit(rows[0])
    corr = dot_row(one, rows[1], conj_mul)
    two = unit([csub(rows[1][k], cmul(corr, one[k])) for k in range(3)])
    return [one, two, cross_conj(one, two)]


def block(k):
    return pl.ds(pl.multiple_of(k * LANES, LANES), LANES)


def lane_ids(rows=8):
    return lax.broadcasted_iota(jnp.int32, (rows, LANES), 1)


def rows_of(slices, d, r, c, p):
    return pl.ds((d * 2 + r) * 6 + c * 2 + p, slices, stride=36)


def flat_block(ref, k):
    return ref.at[k].reshape(ref.shape[1] * 36, LANES)


def load_link(ref, slices, d):
    rows = [[tuple(ref[rows_of(slices, d, r, c, p), :] for p in range(2)) for c in range(3)] for r in range(2)]
    return rows + [cross_conj(rows[0], rows[1])]


def site_of(k, extent):
    start = k * LANES
    shifted = lane_ids() + lax.rem(start, extent)
    wraps = sum((shifted >= extent * i).astype(jnp.int32) for i in range(1, (LANES + extent - 1) // extent + 1))
    return shifted - extent * wraps, lax.div(start, extent) + wraps


def at_z(row, z, me, rows, extent):
    first = lax.rem(extent + z + 1 - lax.rem(me * rows, extent), extent)
    hit = row == first
    for i in range(1, -(-rows // extent)):
        hit = hit | (row == first + i * extent)
    return hit


def fetch_block(links, held, sem, k, start=0):
    return pltpu.make_async_copy(links.at[:, :, :, :, :, pl.ds(k * LANES, LANES)], held.at[k - start], sem.at[k])


def split3(x):
    hi = x.astype(bf16)
    lo = (x - hi.astype(f32)).astype(bf16)
    return jnp.concatenate([hi, lo, hi], axis=0)


def transform(table, parts):
    both = jnp.dot(table, split3(jnp.concatenate(parts, axis=1)), preferred_element_type=f32)
    return [both[:, i * LANES : (i + 1) * LANES] for i in range(len(parts))]


def swap(v):
    return pltpu.roll(v, 4, 0)


def flip(place, i, group):
    other = place
    for b in range(group.bit_length() - 1):
        if i >> b & 1:
            other = other + (1 << b) * (1 - 2 * lax.rem(lax.div(place, 1 << b), 2))
    return other


def iota(shape, axis):
    return lax.broadcasted_iota(jnp.int32, shape, axis).astype(f32)


def divide(v, n):
    whole = jnp.floor((v + 0.5) * (1.0 / n))
    return whole, v - n * whole


def make_tables(n, planes, wave, tables, zero):
    shape = (n, 3 * n)
    row = iota(shape, 0)
    third, col = divide(iota(shape, 1), n)
    for i, turn in enumerate([row * col, row * (col + (n - 1.0)), col * (row + (n - 1.0))]):
        angle = divide(turn, n)[1] * (2.0 * math.pi / n)
        full = (jnp.cos(angle) + jnp.sin(angle)) * (1.0 / math.sqrt(n))
        high = full.astype(bf16).astype(f32)
        tables[i] = jnp.where(third == 2.0, full - high, high).astype(bf16)
    mode = iota((8, n * n), 1)
    p = jnp.zeros((8, n * n), f32)
    for k in divide(mode, n):
        s = jnp.sin(k * (math.pi / n))
        p = p + 4.0 * s * s
    p = jnp.where(mode == 0.0, 1.0, p)
    root = jnp.sqrt(p + 0.25 * p * p)
    mu = 1.0 / (1.0 + 0.5 * p + root)
    power = lax.integer_pow(mu, planes)
    close = 1.0 / (1.0 - power * power)
    for i, v in enumerate([mu, (0.5 * top_momentum) / root, close, close * power]):
        wave[i] = jnp.where(mode == 0.0, 0.0, v)
    square = (LANES, LANES)
    source, sub = divide(iota(square, 0), 4)
    target, lane = divide(iota(square, 1), 4)
    used = (sub == lane) & (source < planes) & (target < planes)
    for i in range(2):
        d = divide(target - source + (n + i * planes * 1.0), n)[1]
        green = top_momentum * ((n * n - 1.0) / (12.0 * n) - d * (n - d) * (0.5 / n))
        zero[i] = jnp.where(used, green, 0.0)


def link_part(extent, held, smooth, arrive, done, above, below, rot, halo_send, halo_recv, n):
    nb, slices = held.shape[0], held.shape[1]
    yb = extent * extent // LANES
    unit = nb // UNITS
    q = nb * LANES // extent
    mid = (extent // 2) * extent
    lane = lane_ids()
    me = lax.axis_index("space")
    ahead, behind = lax.rem(me + 1, n), lax.rem(me + n - 1, n)
    def rotate(values, sl):
        g = rotation_of(values)
        for i in range(3):
            for j in range(3):
                for p in range(2):
                    rot[6 * i + 2 * j + p, :, sl] = g[i][j][p]

    def rotate_own(k, carry):
        rotate([smooth[a, :, block(k)] for a in range(8)], block(k))
        return carry

    def rotate_above(k, carry):
        rotate([above[a, :, block(k)] for a in range(8)], block(nb + k))
        return carry

    def halo(i, source, dest, other):
        return pltpu.make_async_remote_copy(
            src_ref=source,
            dst_ref=dest,
            send_sem=halo_send.at[i],
            recv_sem=halo_recv.at[i],
            device_id={"space": other},
            device_id_type=MESH,
        )

    def span(start, size):
        return pl.ds(pl.multiple_of(start * LANES, LANES), size * LANES)

    odd = lax.rem(me, 2)
    pick = yb - odd * (yb - mid // LANES)
    below_copy = halo(0, smooth.at[:, :, span(pick, 1)], below, ahead)
    rims = [
        halo(1 + i, smooth.at[:, :, span(i * unit, unit)], above.at[:, :, span(i * unit, unit)], behind)
        for i in range(yb // unit)
    ]

    for v in range(UNITS):
        arrive(v)
        lax.fori_loop(v * unit, (v + 1) * unit, rotate_own, 0)
        if v < len(rims):
            rims[v].start()
    below_copy.start()

    def step(which, k, total):
        sl = block(k)
        before = block(jnp.maximum(k - 1, 0))
        after = block(k + 1)
        wrap = block(jnp.where(k == yb, 0, nb + yb))
        x_at, row = site_of(k, extent)
        edge_x = x_at == extent - 1
        edge_z = at_z(row, extent - 1, me, q, extent)

        def ahead_x(e):
            cur = rot[e, :, sl]
            near = pltpu.roll(jnp.where(lane == 0, rot[e, :, after], cur), LANES - 1, 1)
            far = pltpu.roll(jnp.where(lane >= LANES - extent + 1, rot[e, :, before], cur), extent - 1, 1)
            return jnp.where(edge_x, far, near)

        def ahead_y(e):
            return rot[e, :, block(k + yb)]

        def ahead_z(e):
            cur = rot[e, :, sl]
            near = pltpu.roll(jnp.where(lane < extent, rot[e, :, after], cur), LANES - extent, 1)
            far = pltpu.roll(rot[e, :, wrap], LANES - extent, 1)
            return jnp.where(edge_z, far, near)

        flat_out = flat_block(done, k)
        for d in which:
            forward = (ahead_x, ahead_y, ahead_z)[d]
            u = load_link(flat_block(held, k), slices, d)
            own = [[(rot[6 * i + 2 * j, :, sl], rot[6 * i + 2 * j + 1, :, sl]) for j in range(3)] for i in range(2)]
            left = [
                [dot_row(own[i], [u[k2][j] for k2 in range(3)], cmul) for j in range(3)]
                for i in range(2)
            ]
            made = []
            for j in range(3):
                row3 = [(forward(6 * j + 2 * c), forward(6 * j + 2 * c + 1)) for c in range(3)]
                for i in range(2):
                    v = dot_row(left[i], row3, mul_conj)
                    flat_out[rows_of(slices, d, i, j, 0), :] = v[0]
                    flat_out[rows_of(slices, d, i, j, 1), :] = v[1]
                    if j < 2:
                        made.append(v)
            p00, p10, p01, p11 = made
            minor = csub(cmul(p00, p11), cmul(p01, p10))[0]
            total = total + ((1.0 - p00[0]) + (1.0 - p11[0]) + (1.0 - minor))
        return total

    total = jnp.zeros((8, LANES), f32)
    total = lax.fori_loop(1, nb - yb, functools.partial(step, (0, 1, 2)), total)
    below_copy.wait_recv()
    rotate([below[a] for a in range(8)], block(nb + yb))
    total = lax.fori_loop(0, 1, functools.partial(step, (0, 1, 2)), total)
    total = lax.fori_loop(nb - yb, nb - 1, functools.partial(step, (0, 2)), total)
    for i, copy in enumerate(rims):
        copy.wait_recv()
        lax.fori_loop(i * unit, (i + 1) * unit, rotate_above, 0)
        last = i == len(rims) - 1
        total = lax.fori_loop(nb - yb + i * unit, nb - yb + (i + 1) * unit - last, functools.partial(step, (1,)), total)
    total = lax.fori_loop(nb - 1, nb, functools.partial(step, (0, 1, 2)), total)
    for copy in [below_copy] + rims:
        copy.wait_send()
    return total


def gauge_kernel(
    extent, group, scales, links, done, out_theta, out_deficit, *refs
):
    (
        held_links, smooth, above, below, rot, sum_row, sums, late_send, late_recv, sum_send, sum_recv,
        alg, y_rim, z_below, z_above, mine, fields, load_sem, halo_send, halo_recv,
        in_send_sem, in_recv_sem, in_edge_send, in_edge_recv,
        extra, extra_held, extra_send, extra_recv, tip_send, tip_recv, wave, tables, zero, one, two, modes, ends, far, mode, far_mode, outgo, held, edge_held,
        end_send, end_recv, send_sem, recv_sem, edge_send, edge_recv,
    ) = refs
    devices = 2 * group
    nb, slices = mine.shape[1], alg.shape[2]
    yb = extent * extent // LANES
    half = slices // 2
    unit = nb // UNITS
    q = nb * LANES // extent
    mid = (extent // 2) * extent
    lane = lane_ids()
    me = lax.axis_index("space")
    place = lax.rem(me, group)
    base = me - place
    beyond = group - base
    ahead, behind = lax.rem(me + 1, devices), lax.rem(me + devices - 1, devices)
    in_spans = [(0, 1)] + [(i * unit, (i + 1) * unit) for i in range(1, UNITS)] + [(1, unit)]
    in_loads = [[fetch_block(links, held_links, load_sem, k) for k in range(a, b)] for a, b in in_spans]
    for copy in sum(in_loads, []):
        copy.start()
    barrier = greet([base + flip(place, i, group) for i in range(1, group)] + [beyond + i for i in range(group)])

    make_tables(extent, extent // 2, wave, tables, zero)

    first = nb - yb

    def algebra(i):
        start, stop = in_spans[i]

        def step(k, carry):
            flat = flat_block(held_links, k)
            for d in range(3):
                for a, v in enumerate(algebra_of(load_link(flat, slices, d))):
                    alg[d, a, :, block(k)] = v
                    if d == 1 and start >= first:
                        extra[2 * a, k - first] = v[:half]
                        extra[2 * a + 1, k - first] = v[half:]
            return carry

        for copy in in_loads[i]:
            copy.wait()
        lax.fori_loop(start, stop, step, 0)

    def halo(i, source, dest, other):
        return pltpu.make_async_remote_copy(
            src_ref=source,
            dst_ref=dest,
            send_sem=halo_send.at[i],
            recv_sem=halo_recv.at[i],
            device_id={"space": other},
            device_id_type=MESH,
        )

    def span(start, size):
        return pl.ds(pl.multiple_of(start * LANES, LANES), size * LANES)

    rims = [
        halo(i, alg.at[1, :, :, span(first + i * unit, unit)], y_rim.at[:, :, span(i * unit, unit)], ahead)
        for i in range(yb // unit)
    ]
    below_copy = halo(len(rims), alg.at[2, :, :, span(nb - 1, 1)], z_below, ahead)
    odd = lax.rem(me, 2)
    above_copy = halo(len(rims) + 1, alg.at[2, :, :, span(odd * (mid // LANES), 1)], z_above, behind)

    last = lax.div(place + 1, group)
    next_base = base + last * (beyond - base)
    slot = lax.div(lax.rem(place + 1, group), 2)

    def extra_copy(u, i):
        other = flip(place, i, group)
        return pltpu.make_async_remote_copy(
            src_ref=extra.at[other, pl.ds(u * unit, unit)],
            dst_ref=extra_held.at[pl.ds(slot * yb + u * unit, unit)],
            send_sem=extra_send.at[u, i],
            recv_sem=extra_recv.at[u, slot],
            device_id={"space": next_base + other},
            device_id_type=MESH,
        )

    def tip_copy(i):
        other = flip(place, i, group)
        return pltpu.make_async_remote_copy(
            src_ref=extra.at[other, pl.ds(0, 1)],
            dst_ref=extra_held.at[pl.ds(group // 2 * yb, 1)],
            send_sem=tip_send.at[i],
            recv_sem=tip_recv.at[0],
            device_id={"space": base + other},
            device_id_type=MESH,
        )

    def send_rim(u):
        @pl.when(odd == 0)
        def _():
            rims[u].start()

        @pl.when(odd == 1)
        def _():
            for i in reversed(range(1, group)):
                extra_copy(u, i).start()

        @pl.when(last == 1)
        def _():
            extra_copy(u, 0).start()

    algebra(0)
    algebra(1)
    pl.semaphore_wait(barrier, devices - 1)
    above_copy.start()
    send_rim(0)
    for i in range(1, len(rims)):
        algebra(1 + i)
        if i == len(rims) - 1:
            below_copy.start()
        send_rim(i)

    @pl.when(last == 1)
    def _():
        for i in range(1, group):
            tip_copy(i).start()
        extra_held[group // 2 * yb] = extra[place, 0]

    @pl.when(odd == 0)
    def _():
        y_rim[...] = jnp.zeros_like(y_rim)

    algebra(UNITS)

    @pl.when((odd == 1) & (last == 0))
    def _():
        def keep_extra(k, carry):
            extra_held[slot * yb + k] = extra[place, k]
            return carry

        lax.fori_loop(0, yb, keep_extra, 0)

    def step(from_rim, k, carry):
        sl = block(k)
        before = block(jnp.maximum(k - 1, 0))
        after = block(jnp.minimum(k + 1, nb - 1))
        x_at, row = site_of(k, extent)
        edge_x = x_at == 0
        edge_z = at_z(row, 0, me, q, extent)
        for a in range(8):
            x, y, z = alg[0, a, :, sl], alg[1, a, :, sl], alg[2, a, :, sl]
            near = pltpu.roll(jnp.where(lane == LANES - 1, alg[0, a, :, before], x), 1, 1)
            far = pltpu.roll(jnp.where(lane < extent - 1, alg[0, a, :, after], x), LANES - extent + 1, 1)
            bx = jnp.where(edge_x, far, near)
            by = y_rim[a, :, sl] if from_rim else alg[1, a, :, block(k - yb)]
            prev = jnp.where(k == 0, z_below[a], alg[2, a, :, before])
            near = pltpu.roll(jnp.where(lane >= LANES - extent, prev, z), extent, 1)
            far = pltpu.roll(jnp.where(k == 0, alg[2, a, :, block(yb)], z_above[a]), extent, 1)
            bz = jnp.where(edge_z, far, near)
            b = (bx - x) + (by - y) + (bz - z)
            mine[2 * a, k] = b[:half]
            mine[2 * a + 1, k] = b[half:]
        return carry

    def in_edge_copy(i):
        return pltpu.make_async_remote_copy(
            src_ref=mine.at[i, pl.ds(0, 1)],
            dst_ref=fields.at[pl.ds(group * nb, 1)],
            send_sem=in_edge_send.at[i],
            recv_sem=in_edge_recv.at[0],
            device_id={"space": beyond + i},
            device_id_type=MESH,
        )

    in_copies = []
    above_copy.wait_recv()
    below_copy.wait_recv()
    for c in [UNITS - 1] + list(range(UNITS - 1)):
        if c < len(rims):

            @pl.when(odd == 1)
            def _():
                rims[c].wait_recv()

        lax.fori_loop(c * unit, (c + 1) * unit, functools.partial(step, c < len(rims)), 0)
        if c == 0:

            @pl.when(place == 0)
            def _():
                for i in range(group):
                    in_edge_copy(i).start()

        for i in reversed(range(1, group)):
            other = flip(place, i, group)
            copy = pltpu.make_async_remote_copy(
                src_ref=mine.at[other, pl.ds(c * unit, unit)],
                dst_ref=fields.at[pl.ds(place * nb + c * unit, unit)],
                send_sem=in_send_sem.at[c, i],
                recv_sem=in_recv_sem.at[c, i],
                device_id={"space": base + other},
                device_id_type=MESH,
            )
            copy.start()
            in_copies.append(copy)
    def keep(k, carry):
        fields[place * nb + k] = mine[place, k]
        return carry

    lax.fori_loop(0, nb, keep, 0)
    for copy in [below_copy, above_copy]:
        copy.wait_send()

    @pl.when(odd == 0)
    def _():
        for copy in rims:
            copy.wait_send()

    @pl.when(odd == 1)
    def _():
        for u in range(len(rims)):
            for i in range(1, group):
                extra_copy(u, i).wait_send()

    @pl.when(last == 1)
    def _():
        for u in range(len(rims)):
            extra_copy(u, 0).wait_send()
        for i in range(1, group):
            tip_copy(i).wait_send()

    for copy in in_copies:
        copy.wait()
    in_edge_copy(0).wait_recv()

    @pl.when(last == 0)
    def _():
        tip_copy(1).wait_recv()

    def wait_extra(m):
        @pl.when(place != 2 * m - 1)
        def _():
            for u in range(len(rims)):
                pltpu.make_async_remote_copy(
                    src_ref=extra.at[0, pl.ds(u * unit, unit)],
                    dst_ref=extra_held.at[pl.ds(m * yb + u * unit, unit)],
                    send_sem=extra_send.at[u, 0],
                    recv_sem=extra_recv.at[u, m],
                    device_id={"space": beyond},
                    device_id_type=MESH,
                ).wait_recv()

    for m in range(group // 2):
        wait_extra(m)

    @pl.when(place == 0)
    def _():
        for i in range(group):
            in_edge_copy(i).wait_send()

    n = extent
    planes = group * nb * LANES // (n * n)
    columns = n * n // LANES
    pairs = planes // 2
    lanes = planes * 4
    per = columns // PIECES
    upper = lax.broadcasted_iota(jnp.int32, (8, LANES), 0) >= 4
    x_table, z_table, z_back = (tables.at[i] for i in range(3))
    decay, weight = wave.at[0], wave.at[1]
    close = wave.at[pl.ds(2, 2)]
    own_zero, far_zero = zero.at[0], zero.at[1]
    def rows_at(i):
        return pl.ds(pl.multiple_of(i * n, 8), n)

    def turn_in(c, tip):
        tiles = [fields[y * columns + c] for y in range(planes)]
        for m in range(group // 2):
            y = m * (planes // (group // 2))
            tiles[y] = tiles[y] + extra_held[m * yb + c]
        tiles = tiles + tip
        rest = LANES - 4 * len(tiles)
        full = jnp.concatenate(tiles + [jnp.zeros((rest, LANES), f32)], axis=0)
        one[block(c), :] = full.T
        return full

    def turn_rest(c, total):
        full = turn_in(c, [])
        return total + sum(full[8 * i : 8 * i + 8] * full[8 * i : 8 * i + 8] for i in range(lanes // 8))

    theta = lax.fori_loop(0, columns, turn_rest, jnp.zeros((8, LANES), f32), unroll=3)
    turn_in(0, [fields[planes * columns] + extra_held[group // 2 * yb]])
    one[0:n, :] = pltpu.roll(one[0:n, :], LANES - 4, 1)
    def along_x(i, carry):
        parts = [one[rows_at(2 * i + e), :] for e in range(2)]
        for e, v in enumerate(transform(x_table[...], parts)):
            two[rows_at(2 * i + e), :] = v
        return carry

    lax.fori_loop(0, n // 2, along_x, 0, unroll=4)

    def along_z(i, carry):
        parts = [two[pl.ds(2 * i + e, n, stride=n), :] for e in range(2)]
        for e, v in enumerate(transform(z_table[...], parts)):
            one[rows_at(2 * i + e), :] = v
        return carry

    def end_copy(p):
        cols = pl.ds(p * per * LANES, per * LANES)
        return pltpu.make_async_remote_copy(
            src_ref=ends.at[:, cols],
            dst_ref=far.at[:, cols],
            send_sem=end_send.at[p],
            recv_sem=end_recv.at[p],
            device_id={"space": beyond + place},
            device_id_type=MESH,
        )

    mode_copy = pltpu.make_async_remote_copy(
        src_ref=mode,
        dst_ref=far_mode,
        send_sem=end_send.at[PIECES],
        recv_sem=end_recv.at[PIECES],
        device_id={"space": beyond + place},
        device_id_type=MESH,
    )

    def reduce_ends(c, carry):
        sl = block(c)
        modes[:, sl] = one[sl, :].T[:lanes]
        mu = decay[:, sl]
        mu2 = mu * mu
        low = jnp.where(upper, 1.0, mu)
        high = jnp.where(upper, mu, 1.0)
        fwd = modes[0:8, sl]
        bwd = modes[lanes - 8 : lanes, sl]
        for i in range(1, pairs):
            fwd = fwd * mu2 + modes[8 * i : 8 * i + 8, sl]
            bwd = bwd * mu2 + modes[lanes - 8 - 8 * i : lanes - 8 * i, sl]
        ends[:, sl] = jnp.where(upper, high * bwd + low * swap(bwd), low * fwd + high * swap(fwd))
        return carry

    step_z = n // 2 // PIECES
    for p in range(PIECES):
        lax.fori_loop(p * step_z, (p + 1) * step_z, along_z, 0, unroll=4)
        if p == 0:
            mode[...] = one[0:8, :]
        lax.fori_loop(p * per, (p + 1) * per, reduce_ends, 0, unroll=per)
        if p == 0:
            mode_copy.start()
        end_copy(p).start()

    def sweep(c, carry):
        sl = block(c)
        mu = decay[:, sl]
        mu2 = mu * mu
        low = jnp.where(upper, 1.0, mu)
        high = jnp.where(upper, mu, 1.0)
        total = close[0, :, sl] * far[:, sl] + close[1, :, sl] * ends[:, sl]
        turned = swap(total)
        e = jnp.where(upper, turned, total)
        f = jnp.where(upper, total, turned) * mu
        w = weight[:, sl]
        up = mu * high
        down = jnp.where(upper, 0.0, mu)
        rising = []
        for i in range(pairs):
            v = modes[8 * i : 8 * i + 8, sl]
            s = low * v + high * swap(v)
            rising.append(jnp.where(upper, s, v) + up * e)
            e = mu2 * e + s
        done = [None] * pairs
        for i in reversed(range(pairs)):
            v = modes[8 * i : 8 * i + 8, sl]
            t = swap(v)
            done[i] = w * (rising[i] + low * f + down * t)
            f = mu2 * f + mu * (high * v + low * t)
        full = jnp.concatenate(done + [jnp.zeros((LANES - lanes, LANES), f32)], axis=0)
        one[sl, :] = full.T
        return carry

    def back_z(i, carry):
        parts = [one[rows_at(2 * i + e), :] for e in range(2)]
        for e, v in enumerate(transform(z_back[...], parts)):
            two[pl.ds(2 * i + e, n, stride=n), :] = v
        return carry

    for p in range(PIECES):
        end_copy(p).wait_recv()
        if p == 0:
            mode_copy.wait_recv()
        lax.fori_loop(p * per, (p + 1) * per, sweep, 0, unroll=per)
        if p == 0:
            exact = functools.partial(jnp.dot, preferred_element_type=f32, precision=lax.Precision.HIGHEST)
            flat = exact(mode[...], own_zero[...]) + exact(far_mode[...], far_zero[...])
            first = lax.broadcasted_iota(jnp.int32, (8, LANES), 0) == 0
            one[0:8, :] = jnp.where(first, flat, one[0:8, :])
        lax.fori_loop(p * step_z, (p + 1) * step_z, back_z, 0, unroll=4)

    def back_x(i, carry):
        parts = [two[rows_at(2 * i + e), :] for e in range(2)]
        for e, v in enumerate(transform(x_table[...], parts)):
            one[rows_at(2 * i + e), :] = v
        return carry

    def turn_out(c):
        full = one[block(c), :].T
        for y in range(planes):
            outgo[y * columns + c] = full[4 * y : 4 * y + 4]
        return full

    def turn_out_rest(c, carry):
        turn_out(c)
        return carry

    def unit_copy(i, v):
        other = flip(place, i, group)
        return pltpu.make_async_remote_copy(
            src_ref=outgo.at[pl.ds(other * nb + v * unit, unit)],
            dst_ref=held.at[place, pl.ds(v * unit, unit)],
            send_sem=send_sem.at[v, i],
            recv_sem=recv_sem.at[v, i],
            device_id={"space": base + other},
            device_id_type=MESH,
        )

    edge_copy = pltpu.make_async_remote_copy(
        src_ref=outgo.at[pl.ds(planes * columns, 1)],
        dst_ref=edge_held.at[place],
        send_sem=edge_send.at[0],
        recv_sem=edge_recv.at[place],
        device_id={"space": beyond},
        device_id_type=MESH,
    )

    for side in range(2):
        lax.fori_loop(side * n // 4, (side + 1) * n // 4, back_x, 0, unroll=4)
        if side == 0:
            one[0:n, :] = pltpu.roll(one[0:n, :], 4, 1)
            outgo[planes * columns] = turn_out(0)[lanes : lanes + 4]
        lax.fori_loop(side * unit, (side + 1) * unit, turn_out_rest, 0, unroll=3)
        if side == 0:
            edge_copy.start()
        for i in reversed(range(1, group)):
            odd = lax.rem(place + i + side, 2)
            unit_copy(i, odd).start()

            @pl.when(odd == 0)
            def _():
                unit_copy(i, 2).start()

    def keep(k, carry):
        held[place, k] = outgo[place * nb + k]
        return carry

    lax.fori_loop(0, nb, keep, 0)
    for p in range(PIECES):
        end_copy(p).wait_send()
    mode_copy.wait_send()
    edge_copy.wait_send()

    def edge_wait():
        @pl.when(place == 0)
        def _():
            for i in range(group):
                pltpu.make_async_remote_copy(
                    src_ref=outgo.at[pl.ds(planes * columns, 1)],
                    dst_ref=edge_held.at[i],
                    send_sem=edge_send.at[0],
                    recv_sem=edge_recv.at[i],
                    device_id={"space": beyond},
                    device_id_type=MESH,
                ).wait_recv()
            for a in range(8):
                row = jnp.concatenate([edge_held[2 * a, 0], edge_held[2 * a + 1, 0]], axis=0)
                smooth[a, :, 0:LANES] = jnp.where(lane_ids() < n, row, smooth[a, :, 0:LANES])

    def gather(k, carry):
        for a in range(8):
            smooth[a, :, block(k)] = jnp.concatenate([held[2 * a, k], held[2 * a + 1, k]], axis=0)
        return carry

    def arrive(v):
        for i in reversed(range(1, group)):
            unit_copy(i, v).wait()
        lax.fori_loop(v * unit, (v + 1) * unit, gather, 0)
        if v == 0:
            edge_wait()

    total = link_part(extent, held_links, smooth, arrive, done, above, below, rot, late_send, late_recv, devices)

    wide_lane = lane_ids(slices)
    t = jnp.sum(jnp.sum(theta, axis=1, keepdims=True), axis=0, keepdims=True)
    d = jnp.sum(total, axis=1, keepdims=True)
    own_row = lax.broadcasted_iota(jnp.int32, (slices, LANES), 0)
    spread = jnp.where(
        wide_lane == own_row, d, jnp.where(wide_lane == slices, jnp.where(own_row == 0, t, 0.0), 0.0)
    )
    sum_row[...] = jnp.sum(spread, axis=0, keepdims=True)
    copies = []
    for i in range(1, devices):
        copy = pltpu.make_async_remote_copy(
            src_ref=sum_row,
            dst_ref=sums.at[i],
            send_sem=sum_send.at[i],
            recv_sem=sum_recv.at[i],
            device_id={"space": lax.rem(me + i, devices)},
            device_id_type=MESH,
        )
        copy.start()
        copies.append(copy)
    for copy in copies:
        copy.wait()
    row = sum_row[...]
    for i in range(1, devices):
        row = row + sums[i]
    out_deficit[...] = row[:, :slices] * scales[1]
    out_theta[...] = row[:, slices : slices + 1] * scales[0]


def place_kernel(blocks, out, sem):
    copies = [
        pltpu.make_async_copy(blocks.at[k], out.at[:, :, :, :, :, pl.ds(k * LANES, LANES)], sem.at[k])
        for k in range(blocks.shape[0])
    ]
    for copy in copies:
        copy.start()
    for copy in copies:
        copy.wait()


def greet(others):
    barrier = pltpu.get_barrier_semaphore()
    for other in others:
        pl.semaphore_signal(barrier, inc=1, device_id={"space": other}, device_id_type=MESH)
    return barrier


ANY = pl.BlockSpec(memory_space=pl.ANY)
HBM = pl.BlockSpec(memory_space=pltpu.HBM)


def call(kernel, number, out_shape, scratch, *args, in_specs=None, out_specs=None, limit=0):
    return pl.pallas_call(
        kernel,
        out_shape=out_shape,
        in_specs=in_specs or [VM] * len(args),
        out_specs=out_specs or jax.tree.map(lambda _: VM, out_shape),
        scratch_shapes=scratch,
        cost_estimate=pl.CostEstimate(flops=COST, bytes_accessed=COST // 1000, transcendentals=0),
        compiler_params=pltpu.CompilerParams(
            collective_id=number, has_side_effects=True, vmem_limit_bytes=limit * 1024
        ),
    )(*args)


def body(links):
    n = EXTENT
    slices, local = links.shape[0], links.shape[-1]
    devices = lax.axis_size("space")
    plane = n * n
    shape = lambda *s: jax.ShapeDtypeStruct(s, f32)
    vm = lambda *s: pltpu.VMEM(s, f32)
    dma = lambda *s: pltpu.SemaphoreType.DMA(s)
    group = devices // 2
    planes = n // 2
    nb = local // LANES
    assert group * 4 == 8 * slices and nb % UNITS == 0 and plane % (nb // UNITS * LANES) == 0
    rims = plane // (nb // UNITS * LANES)
    blocks = (nb, slices, 3, 2, 3, 2, LANES)
    times = lax.axis_size("tm")
    scales = (1.0 / (slices * times * n**3), 1.0 / n**3)
    placed, total, shares = call(
        functools.partial(gauge_kernel, n, group, scales),
        1,
        (shape(*blocks), shape(1, 1), shape(1, slices)),
        [
            vm(*blocks), vm(8, slices, local), vm(8, slices, plane), vm(8, slices, LANES),
            vm(18, slices, local + plane + LANES), vm(1, LANES), vm(devices, 1, LANES),
            dma(rims + 1), dma(rims + 1), dma(devices), dma(devices),
            vm(3, 8, slices, local), vm(8, slices, plane), vm(8, slices, LANES), vm(8, slices, LANES),
            vm(group, nb, 4, LANES), vm(group * nb + 1, 4, LANES), dma(nb), dma(rims + 2), dma(rims + 2),
            dma(UNITS, group), dma(UNITS, group), dma(group), dma(1),
            vm(group, plane // LANES, 4, LANES), vm(devices // 4 * (plane // LANES) + 1, 4, LANES),
            dma(rims, group), dma(rims, group // 2), dma(group), dma(1),
            vm(4, 8, plane), pltpu.VMEM((3, n, 3 * n), bf16), vm(2, LANES, LANES),
            vm(plane, LANES), vm(plane, LANES), vm(4 * planes, plane), vm(8, plane), vm(8, plane),
            vm(8, LANES), vm(8, LANES), vm(group * nb + 1, 4, LANES), vm(group, nb, 4, LANES), vm(group, 1, 4, LANES),
            dma(PIECES + 1), dma(PIECES + 1), dma(UNITS, group), dma(UNITS, group), dma(1), dma(group),
        ],
        links,
        in_specs=[HBM],
        limit=GAUGE_KB,
    )
    new_links = pl.pallas_call(
        place_kernel,
        out_shape=shape(*links.shape),
        in_specs=[VM],
        out_specs=ANY,
        scratch_shapes=[dma(nb)],
        compiler_params=pltpu.CompilerParams(vmem_limit_bytes=8 * 1024 * 1024),
    )(placed)
    total = total.reshape(())
    if times > 1:
        total = lax.psum(total, "tm")
    return (new_links, total, shares.reshape(slices))


def solution(mesh):
    placed = (P("tm", None, None, None, None, "space"),)
    return jax.shard_map(
        body,
        mesh=mesh,
        in_specs=placed,
        out_specs=(P("tm", None, None, None, None, "space"), P(), P("tm")),
        check_vma=False,
    )
```

```python
import functools
import math

import jax
import jax.numpy as jnp
from jax import lax
from jax.experimental import pallas as pl
from jax.experimental.pallas import tpu as pltpu
from jax.sharding import PartitionSpec as P

EXTENT = 48
LANES = 128
UNITS = 3
PIECES = 6
COST = 10**9
GAUGE_KB = 50 * 1000

root_three = math.sqrt(3.0)
step_size = 0.08
top_momentum = 12.0

f32 = jnp.float32
bf16 = jnp.bfloat16
MESH = pl.DeviceIdType.MESH
VM = pl.BlockSpec(memory_space=pltpu.VMEM)


def cmul(p, q):
    return (p[0] * q[0] - p[1] * q[1], p[0] * q[1] + p[1] * q[0])


def cadd(p, q):
    return (p[0] + q[0], p[1] + q[1])


def csub(p, q):
    return (p[0] - q[0], p[1] - q[1])


def conj(p):
    return (p[0], -p[1])


def conj_mul(p, q):
    return (p[0] * q[0] + p[1] * q[1], p[0] * q[1] - p[1] * q[0])


def mul_conj(p, q):
    return (p[0] * q[0] + p[1] * q[1], p[1] * q[0] - p[0] * q[1])


def dot_row(row, col, mul):
    out = mul(row[0], col[0])
    for k in (1, 2):
        out = cadd(out, mul(row[k], col[k]))
    return out


def cross_conj(a, b):
    return [
        conj(csub(cmul(a[(k + 1) % 3], b[(k + 2) % 3]), cmul(a[(k + 2) % 3], b[(k + 1) % 3])))
        for k in range(3)
    ]


def algebra_of(u):
    return [
        u[0][1][1] + u[1][0][1],
        u[0][1][0] - u[1][0][0],
        u[0][0][1] - u[1][1][1],
        u[0][2][1] + u[2][0][1],
        u[0][2][0] - u[2][0][0],
        u[1][2][1] + u[2][1][1],
        u[1][2][0] - u[2][1][0],
        (u[0][0][1] + u[1][1][1] - 2.0 * u[2][2][1]) * (1.0 / root_three),
    ]


def rotation_of(s):
    h = 0.5 * step_size
    s = [v * h for v in s]
    third = s[7] * (1.0 / root_three)
    d0, d1, d2 = s[2] + third, third - s[2], -2.0 * third
    herm = [
        [(d0, None), (s[0], -s[1]), (s[3], -s[4])],
        [(s[0], s[1]), (d1, None), (s[5], -s[6])],
        [(s[3], s[4]), (s[5], s[6]), (d2, None)],
    ]

    def mul(p, q):
        if p[1] is None and q[1] is None:
            return (p[0] * q[0], jnp.zeros_like(p[0]))
        if p[1] is None:
            return (p[0] * q[0], p[0] * q[1])
        if q[1] is None:
            return (p[0] * q[0], p[1] * q[0])
        return cmul(p, q)

    rows = []
    for i in range(2):
        row = []
        for j in range(3):
            sq = dot_row(herm[i], [herm[k][j] for k in range(3)], mul)
            re, im = -0.5 * sq[0], -0.5 * sq[1]
            if herm[i][j][1] is not None:
                re = re - herm[i][j][1]
            else:
                re = re + 1.0
            row.append((re, im + herm[i][j][0]))
        rows.append(row)

    def unit(row):
        inv = lax.rsqrt(sum(p[0] * p[0] + p[1] * p[1] for p in row))
        return [(p[0] * inv, p[1] * inv) for p in row]

    one = unit(rows[0])
    corr = dot_row(one, rows[1], conj_mul)
    two = unit([csub(rows[1][k], cmul(corr, one[k])) for k in range(3)])
    return [one, two, cross_conj(one, two)]


def block(k):
    return pl.ds(pl.multiple_of(k * LANES, LANES), LANES)


def lane_ids(rows=8):
    return lax.broadcasted_iota(jnp.int32, (rows, LANES), 1)


def rows_of(slices, d, r, c, p):
    return pl.ds((d * 2 + r) * 6 + c * 2 + p, slices, stride=36)


def flat_block(ref, k):
    return ref.at[k].reshape(ref.shape[1] * 36, LANES)


def load_link(ref, slices, d):
    rows = [[tuple(ref[rows_of(slices, d, r, c, p), :] for p in range(2)) for c in range(3)] for r in range(2)]
    return rows + [cross_conj(rows[0], rows[1])]


def site_of(k, extent):
    start = k * LANES
    shifted = lane_ids() + lax.rem(start, extent)
    wraps = sum((shifted >= extent * i).astype(jnp.int32) for i in range(1, (LANES + extent - 1) // extent + 1))
    return shifted - extent * wraps, lax.div(start, extent) + wraps


def at_z(row, z, me, rows, extent):
    first = lax.rem(extent + z + 1 - lax.rem(me * rows, extent), extent)
    hit = row == first
    for i in range(1, -(-rows // extent)):
        hit = hit | (row == first + i * extent)
    return hit


def fetch_block(links, held, sem, k, start=0):
    return pltpu.make_async_copy(links.at[:, :, :, :, :, pl.ds(k * LANES, LANES)], held.at[k - start], sem.at[k])


def split3(x):
    hi = x.astype(bf16)
    lo = (x - hi.astype(f32)).astype(bf16)
    return jnp.concatenate([hi, lo, hi], axis=0)


def transform(table, parts):
    both = jnp.dot(table, split3(jnp.concatenate(parts, axis=1)), preferred_element_type=f32)
    return [both[:, i * LANES : (i + 1) * LANES] for i in range(len(parts))]


def swap(v):
    return pltpu.roll(v, 4, 0)


def flip(place, i, group):
    other = place
    for b in range(group.bit_length() - 1):
        if i >> b & 1:
            other = other + (1 << b) * (1 - 2 * lax.rem(lax.div(place, 1 << b), 2))
    return other


def iota(shape, axis):
    return lax.broadcasted_iota(jnp.int32, shape, axis).astype(f32)


def divide(v, n):
    whole = jnp.floor((v + 0.5) * (1.0 / n))
    return whole, v - n * whole


def make_tables(n, planes, wave, tables, zero):
    shape = (n, 3 * n)
    row = iota(shape, 0)
    third, col = divide(iota(shape, 1), n)
    for i, turn in enumerate([row * col, row * (col + (n - 1.0)), col * (row + (n - 1.0))]):
        angle = divide(turn, n)[1] * (2.0 * math.pi / n)
        full = (jnp.cos(angle) + jnp.sin(angle)) * (1.0 / math.sqrt(n))
        high = full.astype(bf16).astype(f32)
        tables[i] = jnp.where(third == 2.0, full - high, high).astype(bf16)
    mode = iota((8, n * n), 1)
    p = jnp.zeros((8, n * n), f32)
    for k in divide(mode, n):
        s = jnp.sin(k * (math.pi / n))
        p = p + 4.0 * s * s
    p = jnp.where(mode == 0.0, 1.0, p)
    root = jnp.sqrt(p + 0.25 * p * p)
    mu = 1.0 / (1.0 + 0.5 * p + root)
    power = lax.integer_pow(mu, planes)
    close = 1.0 / (1.0 - power * power)
    for i, v in enumerate([mu, (0.5 * top_momentum) / root, close, close * power]):
        wave[i] = jnp.where(mode == 0.0, 0.0, v)
    square = (LANES, LANES)
    source, sub = divide(iota(square, 0), 4)
    target, lane = divide(iota(square, 1), 4)
    used = (sub == lane) & (source < planes) & (target < planes)
    for i in range(2):
        d = divide(target - source + (n + i * planes * 1.0), n)[1]
        green = top_momentum * ((n * n - 1.0) / (12.0 * n) - d * (n - d) * (0.5 / n))
        zero[i] = jnp.where(used, green, 0.0)


def link_part(extent, held, smooth, arrive, mend_edges, done, below, rot, halo_send, halo_recv, n):
    nb, slices = held.shape[0], held.shape[1]
    yb = extent * extent // LANES
    unit = nb // UNITS
    q = nb * LANES // extent
    mid = (extent // 2) * extent
    lane = lane_ids()
    me = lax.axis_index("space")
    ahead, behind = lax.rem(me + 1, n), lax.rem(me + n - 1, n)
    def rotate(values, sl):
        g = rotation_of(values)
        for i in range(3):
            for j in range(3):
                for p in range(2):
                    rot[6 * i + 2 * j + p, :, sl] = g[i][j][p]

    def rotate_own(k, carry):
        rotate([smooth[a, :, block(k)] for a in range(8)], block(k))
        return carry

    def halo(i, source, dest, other):
        return pltpu.make_async_remote_copy(
            src_ref=source,
            dst_ref=dest,
            send_sem=halo_send.at[i],
            recv_sem=halo_recv.at[i],
            device_id={"space": other},
            device_id_type=MESH,
        )

    def span(start, size):
        return pl.ds(pl.multiple_of(start * LANES, LANES), size * LANES)

    odd = lax.rem(me, 2)
    pick = yb - odd * (yb - mid // LANES)
    below_copy = halo(0, smooth.at[:, :, span(pick, 1)], below, ahead)
    rims = [
        halo(1 + i, smooth.at[:, :, span(i * unit, unit)], smooth.at[:, :, span(nb + i * unit, unit)], behind)
        for i in range(2)
    ]

    def turn(v):
        lax.fori_loop(v * unit, (v + 1) * unit, rotate_own, 0)

    def step(which, k, total):
        sl = block(k)
        before = block(jnp.maximum(k - 1, 0))
        after = block(k + 1)
        wrap = block(jnp.where(k == yb, 0, nb + yb))
        x_at, row = site_of(k, extent)
        edge_x = x_at == extent - 1
        edge_z = at_z(row, extent - 1, me, q, extent)

        def ahead_x(e):
            cur = rot[e, :, sl]
            near = pltpu.roll(jnp.where(lane == 0, rot[e, :, after], cur), LANES - 1, 1)
            far = pltpu.roll(jnp.where(lane >= LANES - extent + 1, rot[e, :, before], cur), extent - 1, 1)
            return jnp.where(edge_x, far, near)

        def ahead_y(e):
            return rot[e, :, block(k + yb)]

        def ahead_z(e):
            cur = rot[e, :, sl]
            near = pltpu.roll(jnp.where(lane < extent, rot[e, :, after], cur), LANES - extent, 1)
            far = pltpu.roll(rot[e, :, wrap], LANES - extent, 1)
            return jnp.where(edge_z, far, near)

        flat_out = flat_block(done, k)
        for d in which:
            forward = (ahead_x, ahead_y, ahead_z)[d]
            u = load_link(flat_block(held, k), slices, d)
            own = [[(rot[6 * i + 2 * j, :, sl], rot[6 * i + 2 * j + 1, :, sl]) for j in range(3)] for i in range(2)]
            left = [
                [dot_row(own[i], [u[k2][j] for k2 in range(3)], cmul) for j in range(3)]
                for i in range(2)
            ]
            made = []
            for j in range(3):
                row3 = [(forward(6 * j + 2 * c), forward(6 * j + 2 * c + 1)) for c in range(3)]
                for i in range(2):
                    v = dot_row(left[i], row3, mul_conj)
                    flat_out[rows_of(slices, d, i, j, 0), :] = v[0]
                    flat_out[rows_of(slices, d, i, j, 1), :] = v[1]
                    if j < 2:
                        made.append(v)
            p00, p10, p01, p11 = made
            minor = csub(cmul(p00, p11), cmul(p01, p10))[0]
            total = total + ((1.0 - p00[0]) + (1.0 - p11[0]) + (1.0 - minor))
        return total

    def links_of(start, stop, dirs, total):
        return lax.fori_loop(start, stop, functools.partial(step, dirs), total)

    arrive(odd)
    arrive(odd + 2)
    mend_edges()
    turn(odd)
    turn(odd + 2)

    @pl.when(odd == 1)
    def _():
        rims[1].start()

    below_copy.start()
    total = links_of(odd * unit, (odd + 1) * unit, (1,), jnp.zeros((8, LANES), f32))
    arrive(1 - odd)
    turn(1 - odd)

    @pl.when(odd == 1)
    def _():
        rims[0].start()
        for v in (2, 4):
            arrive(jnp.int32(v))
            turn(v)

    below_copy.wait_recv()
    rotate([below[a] for a in range(8)], block(nb + yb))
    total = links_of(0, nb - 1, (0, 2), total)

    @pl.when(odd == 0)
    def _():
        for v in (3, 4):
            rims[v - 3].wait_recv()
            turn(v)

    total = links_of((1 - odd) * unit, (2 - odd) * unit, (1,), total)
    total = links_of(2 * unit, nb - 1, (1,), total)
    total = links_of(nb - 1, nb, (0, 1, 2), total)
    below_copy.wait_send()

    @pl.when(odd == 1)
    def _():
        for copy in rims:
            copy.wait_send()

    return total


def gauge_kernel(
    extent, group, scales, links, done, out_theta, out_deficit, *refs
):
    (
        held_links, smooth, below, rot, sum_row, sums, late_send, late_recv, sum_send, sum_recv,
        alg, y_rim, z_below, z_above, mine, fields, load_sem, halo_send, halo_recv,
        in_send_sem, in_recv_sem, in_edge_send, in_edge_recv,
        extra, extra_held, extra_send, extra_recv, tip_send, tip_recv, wave, tables, zero, one, two, modes, ends, far, mode, far_mode, outgo, held, edge_held,
        end_send, end_recv, send_sem, recv_sem, edge_send, edge_recv,
    ) = refs
    devices = 2 * group
    nb, slices = mine.shape[1], alg.shape[2]
    yb = extent * extent // LANES
    half = slices // 2
    unit = nb // UNITS
    q = nb * LANES // extent
    mid = (extent // 2) * extent
    lane = lane_ids()
    me = lax.axis_index("space")
    place = lax.rem(me, group)
    base = me - place
    beyond = group - base
    ahead, behind = lax.rem(me + 1, devices), lax.rem(me + devices - 1, devices)
    in_spans = [(0, 1)] + [(i * unit, (i + 1) * unit) for i in range(1, UNITS)] + [(1, unit)]
    in_loads = [[fetch_block(links, held_links, load_sem, k) for k in range(a, b)] for a, b in in_spans]
    for copy in sum(in_loads, []):
        copy.start()
    barrier = greet([base + flip(place, i, group) for i in range(1, group)] + [beyond + i for i in range(group)])

    make_tables(extent, extent // 2, wave, tables, zero)

    first = nb - yb

    def algebra(i):
        start, stop = in_spans[i]

        def step(k, carry):
            flat = flat_block(held_links, k)
            for d in range(3):
                for a, v in enumerate(algebra_of(load_link(flat, slices, d))):
                    alg[d, a, :, block(k)] = v
                    if d == 1 and start >= first:
                        extra[2 * a, k - first] = v[:half]
                        extra[2 * a + 1, k - first] = v[half:]
            return carry

        for copy in in_loads[i]:
            copy.wait()
        lax.fori_loop(start, stop, step, 0)

    def halo(i, source, dest, other):
        return pltpu.make_async_remote_copy(
            src_ref=source,
            dst_ref=dest,
            send_sem=halo_send.at[i],
            recv_sem=halo_recv.at[i],
            device_id={"space": other},
            device_id_type=MESH,
        )

    def span(start, size):
        return pl.ds(pl.multiple_of(start * LANES, LANES), size * LANES)

    rims = [
        halo(i, alg.at[1, :, :, span(first + i * unit, unit)], y_rim.at[:, :, span(i * unit, unit)], ahead)
        for i in range(yb // unit)
    ]
    below_copy = halo(len(rims), alg.at[2, :, :, span(nb - 1, 1)], z_below, ahead)
    odd = lax.rem(me, 2)
    above_copy = halo(len(rims) + 1, alg.at[2, :, :, span(odd * (mid // LANES), 1)], z_above, behind)

    last = lax.div(place + 1, group)
    next_base = base + last * (beyond - base)
    slot = lax.div(lax.rem(place + 1, group), 2)

    def extra_copy(u, i):
        other = flip(place, i, group)
        return pltpu.make_async_remote_copy(
            src_ref=extra.at[other, pl.ds(u * unit, unit)],
            dst_ref=extra_held.at[pl.ds(slot * yb + u * unit, unit)],
            send_sem=extra_send.at[u, i],
            recv_sem=extra_recv.at[u, slot],
            device_id={"space": next_base + other},
            device_id_type=MESH,
        )

    def tip_copy(i):
        other = flip(place, i, group)
        return pltpu.make_async_remote_copy(
            src_ref=extra.at[other, pl.ds(0, 1)],
            dst_ref=extra_held.at[pl.ds(group // 2 * yb, 1)],
            send_sem=tip_send.at[i],
            recv_sem=tip_recv.at[0],
            device_id={"space": base + other},
            device_id_type=MESH,
        )

    def send_rim(u):
        @pl.when(odd == 0)
        def _():
            rims[u].start()

        @pl.when(odd == 1)
        def _():
            for i in reversed(range(1, group)):
                extra_copy(u, i).start()

        @pl.when(last == 1)
        def _():
            extra_copy(u, 0).start()

    algebra(0)
    algebra(1)
    pl.semaphore_wait(barrier, devices - 1)
    above_copy.start()
    send_rim(0)
    for i in range(1, len(rims)):
        algebra(1 + i)
        if i == len(rims) - 1:
            below_copy.start()
        send_rim(i)

    @pl.when(last == 1)
    def _():
        for i in range(1, group):
            tip_copy(i).start()
        extra_held[group // 2 * yb] = extra[place, 0]

    @pl.when(odd == 0)
    def _():
        y_rim[...] = jnp.zeros_like(y_rim)

    algebra(UNITS)

    @pl.when((odd == 1) & (last == 0))
    def _():
        def keep_extra(k, carry):
            extra_held[slot * yb + k] = extra[place, k]
            return carry

        lax.fori_loop(0, yb, keep_extra, 0)

    def step(from_rim, k, carry):
        sl = block(k)
        before = block(jnp.maximum(k - 1, 0))
        after = block(jnp.minimum(k + 1, nb - 1))
        x_at, row = site_of(k, extent)
        edge_x = x_at == 0
        edge_z = at_z(row, 0, me, q, extent)
        for a in range(8):
            x, y, z = alg[0, a, :, sl], alg[1, a, :, sl], alg[2, a, :, sl]
            near = pltpu.roll(jnp.where(lane == LANES - 1, alg[0, a, :, before], x), 1, 1)
            far = pltpu.roll(jnp.where(lane < extent - 1, alg[0, a, :, after], x), LANES - extent + 1, 1)
            bx = jnp.where(edge_x, far, near)
            by = y_rim[a, :, sl] if from_rim else alg[1, a, :, block(k - yb)]
            prev = jnp.where(k == 0, z_below[a], alg[2, a, :, before])
            near = pltpu.roll(jnp.where(lane >= LANES - extent, prev, z), extent, 1)
            far = pltpu.roll(jnp.where(k == 0, alg[2, a, :, block(yb)], z_above[a]), extent, 1)
            bz = jnp.where(edge_z, far, near)
            b = (bx - x) + (by - y) + (bz - z)
            mine[2 * a, k] = b[:half]
            mine[2 * a + 1, k] = b[half:]
        return carry

    def in_edge_copy(i):
        return pltpu.make_async_remote_copy(
            src_ref=mine.at[i, pl.ds(0, 1)],
            dst_ref=fields.at[pl.ds(group * nb, 1)],
            send_sem=in_edge_send.at[i],
            recv_sem=in_edge_recv.at[0],
            device_id={"space": beyond + i},
            device_id_type=MESH,
        )

    in_copies = []
    above_copy.wait_recv()
    below_copy.wait_recv()
    for c in [UNITS - 1] + list(range(UNITS - 1)):
        if c < len(rims):

            @pl.when(odd == 1)
            def _():
                rims[c].wait_recv()

        lax.fori_loop(c * unit, (c + 1) * unit, functools.partial(step, c < len(rims)), 0)
        if c == 0:

            @pl.when(place == 0)
            def _():
                for i in range(group):
                    in_edge_copy(i).start()

        for i in reversed(range(1, group)):
            other = flip(place, i, group)
            copy = pltpu.make_async_remote_copy(
                src_ref=mine.at[other, pl.ds(c * unit, unit)],
                dst_ref=fields.at[pl.ds(place * nb + c * unit, unit)],
                send_sem=in_send_sem.at[c, i],
                recv_sem=in_recv_sem.at[c, i],
                device_id={"space": base + other},
                device_id_type=MESH,
            )
            copy.start()
            in_copies.append(copy)
    def keep(k, carry):
        fields[place * nb + k] = mine[place, k]
        return carry

    lax.fori_loop(0, nb, keep, 0)
    for copy in [below_copy, above_copy]:
        copy.wait_send()

    @pl.when(odd == 0)
    def _():
        for copy in rims:
            copy.wait_send()

    @pl.when(odd == 1)
    def _():
        for u in range(len(rims)):
            for i in range(1, group):
                extra_copy(u, i).wait_send()

    @pl.when(last == 1)
    def _():
        for u in range(len(rims)):
            extra_copy(u, 0).wait_send()
        for i in range(1, group):
            tip_copy(i).wait_send()

    for copy in in_copies:
        copy.wait()
    in_edge_copy(0).wait_recv()

    @pl.when(last == 0)
    def _():
        tip_copy(1).wait_recv()

    def wait_extra(m):
        @pl.when(place != 2 * m - 1)
        def _():
            for u in range(len(rims)):
                pltpu.make_async_remote_copy(
                    src_ref=extra.at[0, pl.ds(u * unit, unit)],
                    dst_ref=extra_held.at[pl.ds(m * yb + u * unit, unit)],
                    send_sem=extra_send.at[u, 0],
                    recv_sem=extra_recv.at[u, m],
                    device_id={"space": beyond},
                    device_id_type=MESH,
                ).wait_recv()

    for m in range(group // 2):
        wait_extra(m)

    @pl.when(place == 0)
    def _():
        for i in range(group):
            in_edge_copy(i).wait_send()

    n = extent
    planes = group * nb * LANES // (n * n)
    columns = n * n // LANES
    pairs = planes // 2
    lanes = planes * 4
    per = columns // PIECES
    upper = lax.broadcasted_iota(jnp.int32, (8, LANES), 0) >= 4
    x_table, z_table, z_back = (tables.at[i] for i in range(3))
    decay, weight = wave.at[0], wave.at[1]
    close = wave.at[pl.ds(2, 2)]
    own_zero, far_zero = zero.at[0], zero.at[1]
    def rows_at(i):
        return pl.ds(pl.multiple_of(i * n, 8), n)

    def turn_in(c, tip):
        tiles = [fields[y * columns + c] for y in range(planes)]
        for m in range(group // 2):
            y = m * (planes // (group // 2))
            tiles[y] = tiles[y] + extra_held[m * yb + c]
        tiles = tiles + tip
        rest = LANES - 4 * len(tiles)
        full = jnp.concatenate(tiles + [jnp.zeros((rest, LANES), f32)], axis=0)
        one[block(c), :] = full.T
        return full

    def turn_rest(c, total):
        full = turn_in(c, [])
        return total + sum(full[8 * i : 8 * i + 8] * full[8 * i : 8 * i + 8] for i in range(lanes // 8))

    theta = lax.fori_loop(0, columns, turn_rest, jnp.zeros((8, LANES), f32), unroll=3)
    turn_in(0, [fields[planes * columns] + extra_held[group // 2 * yb]])
    one[0:n, :] = pltpu.roll(one[0:n, :], LANES - 4, 1)
    def along_x(i, carry):
        parts = [one[rows_at(2 * i + e), :] for e in range(2)]
        for e, v in enumerate(transform(x_table[...], parts)):
            two[rows_at(2 * i + e), :] = v
        return carry

    lax.fori_loop(0, n // 2, along_x, 0, unroll=4)

    def along_z(i, carry):
        parts = [two[pl.ds(2 * i + e, n, stride=n), :] for e in range(2)]
        for e, v in enumerate(transform(z_table[...], parts)):
            one[rows_at(2 * i + e), :] = v
        return carry

    def end_copy(p):
        cols = pl.ds(p * per * LANES, per * LANES)
        return pltpu.make_async_remote_copy(
            src_ref=ends.at[:, cols],
            dst_ref=far.at[:, cols],
            send_sem=end_send.at[p],
            recv_sem=end_recv.at[p],
            device_id={"space": beyond + place},
            device_id_type=MESH,
        )

    mode_copy = pltpu.make_async_remote_copy(
        src_ref=mode,
        dst_ref=far_mode,
        send_sem=end_send.at[PIECES],
        recv_sem=end_recv.at[PIECES],
        device_id={"space": beyond + place},
        device_id_type=MESH,
    )

    def reduce_ends(c, carry):
        sl = block(c)
        modes[:, sl] = one[sl, :].T[:lanes]
        mu = decay[:, sl]
        mu2 = mu * mu
        low = jnp.where(upper, 1.0, mu)
        high = jnp.where(upper, mu, 1.0)
        fwd = modes[0:8, sl]
        bwd = modes[lanes - 8 : lanes, sl]
        for i in range(1, pairs):
            fwd = fwd * mu2 + modes[8 * i : 8 * i + 8, sl]
            bwd = bwd * mu2 + modes[lanes - 8 - 8 * i : lanes - 8 * i, sl]
        ends[:, sl] = jnp.where(upper, high * bwd + low * swap(bwd), low * fwd + high * swap(fwd))
        return carry

    step_z = n // 2 // PIECES
    for p in range(PIECES):
        lax.fori_loop(p * step_z, (p + 1) * step_z, along_z, 0, unroll=4)
        if p == 0:
            mode[...] = one[0:8, :]
        lax.fori_loop(p * per, (p + 1) * per, reduce_ends, 0, unroll=per)
        if p == 0:
            mode_copy.start()
        end_copy(p).start()

    def sweep(c, carry):
        sl = block(c)
        mu = decay[:, sl]
        mu2 = mu * mu
        low = jnp.where(upper, 1.0, mu)
        high = jnp.where(upper, mu, 1.0)
        total = close[0, :, sl] * far[:, sl] + close[1, :, sl] * ends[:, sl]
        turned = swap(total)
        e = jnp.where(upper, turned, total)
        f = jnp.where(upper, total, turned) * mu
        w = weight[:, sl]
        up = mu * high
        down = jnp.where(upper, 0.0, mu)
        rising = []
        for i in range(pairs):
            v = modes[8 * i : 8 * i + 8, sl]
            s = low * v + high * swap(v)
            rising.append(jnp.where(upper, s, v) + up * e)
            e = mu2 * e + s
        done = [None] * pairs
        for i in reversed(range(pairs)):
            v = modes[8 * i : 8 * i + 8, sl]
            t = swap(v)
            done[i] = w * (rising[i] + low * f + down * t)
            f = mu2 * f + mu * (high * v + low * t)
        full = jnp.concatenate(done + [jnp.zeros((LANES - lanes, LANES), f32)], axis=0)
        one[sl, :] = full.T
        return carry

    def back_z(i, carry):
        parts = [one[rows_at(2 * i + e), :] for e in range(2)]
        for e, v in enumerate(transform(z_back[...], parts)):
            two[pl.ds(2 * i + e, n, stride=n), :] = v
        return carry

    for p in range(PIECES):
        end_copy(p).wait_recv()
        if p == 0:
            mode_copy.wait_recv()
        lax.fori_loop(p * per, (p + 1) * per, sweep, 0, unroll=per)
        if p == 0:
            exact = functools.partial(jnp.dot, preferred_element_type=f32, precision=lax.Precision.HIGHEST)
            flat = exact(mode[...], own_zero[...]) + exact(far_mode[...], far_zero[...])
            first = lax.broadcasted_iota(jnp.int32, (8, LANES), 0) == 0
            one[0:8, :] = jnp.where(first, flat, one[0:8, :])
        lax.fori_loop(p * step_z, (p + 1) * step_z, back_z, 0, unroll=4)

    def back_x(i, carry):
        parts = [two[rows_at(2 * i + e), :] for e in range(2)]
        for e, v in enumerate(transform(x_table[...], parts)):
            one[rows_at(2 * i + e), :] = v
        return carry

    def turn_out(c):
        full = one[block(c), :].T
        for y in range(planes):
            outgo[y * columns + c] = full[4 * y : 4 * y + 4]
        return full

    def turn_out_rest(c, carry):
        turn_out(c)
        return carry

    def unit_copy(i, v):
        other = flip(place, i, group)
        wrap = lax.div(v, UNITS) * lax.div(other + 1, group)
        return pltpu.make_async_remote_copy(
            src_ref=outgo.at[pl.ds(other * nb + v * unit - wrap * (planes * columns), unit)],
            dst_ref=held.at[place, pl.ds(v * unit, unit)],
            send_sem=send_sem.at[v, i],
            recv_sem=recv_sem.at[v, i],
            device_id={"space": base + other + wrap * (beyond - base)},
            device_id_type=MESH,
        )

    def edge_copy(i, other):
        return pltpu.make_async_remote_copy(
            src_ref=outgo.at[pl.ds(planes * columns, 1)],
            dst_ref=edge_held.at[place],
            send_sem=edge_send.at[i],
            recv_sem=edge_recv.at[place],
            device_id={"space": other},
            device_id_type=MESH,
        )

    edges = [edge_copy(0, beyond), edge_copy(1, base + group - 1)]

    def each_unit(side, act):
        for i in reversed(range(1, group)):
            parity = lax.rem(place + i, 2)
            if side == 0:
                act(unit_copy(i, parity))
                act(unit_copy(i, parity + 2))
            else:
                act(unit_copy(i, 1 - parity))

                @pl.when(parity == 1)
                def _():
                    act(unit_copy(i, jnp.int32(2)))
                    act(unit_copy(i, jnp.int32(4)))

        @pl.when(last == 1)
        def _():
            act(unit_copy(0, jnp.int32(3 + side)))

    for side in range(2):
        lax.fori_loop(side * n // 4, (side + 1) * n // 4, back_x, 0, unroll=4)
        if side == 0:
            one[0:n, :] = pltpu.roll(one[0:n, :], 4, 1)
            outgo[planes * columns] = turn_out(0)[lanes : lanes + 4]
        lax.fori_loop(side * unit, (side + 1) * unit, turn_out_rest, 0, unroll=3)
        if side == 0:
            edges[0].start()

            @pl.when(last == 0)
            def _():
                edges[1].start()

        each_unit(side, lambda copy: copy.start())

    def keep(k, carry):
        held[place, k] = outgo[place * nb + k]
        return carry

    lax.fori_loop(0, nb, keep, 0)

    @pl.when((odd == 1) & (last == 0))
    def _():
        lax.fori_loop(nb, nb + yb, keep, 0)

    @pl.when(last == 1)
    def _():
        edge_held[place] = outgo[planes * columns : planes * columns + 1]

    def edge_wait(i):
        pltpu.make_async_remote_copy(
            src_ref=outgo.at[pl.ds(planes * columns, 1)],
            dst_ref=edge_held.at[i],
            send_sem=edge_send.at[0],
            recv_sem=edge_recv.at[i],
            device_id={"space": beyond},
            device_id_type=MESH,
        ).wait_recv()

    def mend(start):
        for a in range(8):
            row = jnp.concatenate([edge_held[2 * a, 0], edge_held[2 * a + 1, 0]], axis=0)
            smooth[a, :, start : start + LANES] = jnp.where(
                lane_ids() < n, row, smooth[a, :, start : start + LANES]
            )

    def gather(k, carry):
        for a in range(8):
            smooth[a, :, block(k)] = jnp.concatenate([held[2 * a, k], held[2 * a + 1, k]], axis=0)
        return carry

    def arrive(v):
        for i in reversed(range(1, group)):
            unit_copy(i, v).wait_recv()

        @pl.when(last * lax.div(v, UNITS) == 1)
        def _():
            unit_copy(0, v).wait_recv()

        lax.fori_loop(v * unit, (v + 1) * unit, gather, 0)

    def mend_edges():
        @pl.when(place == 0)
        def _():
            for i in range(group):
                edge_wait(i)
            mend(0)

        @pl.when(last == 1)
        def _():
            for i in range(group - 1):
                edge_wait(i)
            mend(nb * LANES)

    total = link_part(extent, held_links, smooth, arrive, mend_edges, done, below, rot, late_send, late_recv, devices)
    for p in range(PIECES):
        end_copy(p).wait_send()
    mode_copy.wait_send()
    edges[0].wait_send()

    @pl.when(last == 0)
    def _():
        edges[1].wait_send()

    for side in range(2):
        each_unit(side, lambda copy: copy.wait_send())


    wide_lane = lane_ids(slices)
    t = jnp.sum(jnp.sum(theta, axis=1, keepdims=True), axis=0, keepdims=True)
    d = jnp.sum(total, axis=1, keepdims=True)
    own_row = lax.broadcasted_iota(jnp.int32, (slices, LANES), 0)
    spread = jnp.where(
        wide_lane == own_row, d, jnp.where(wide_lane == slices, jnp.where(own_row == 0, t, 0.0), 0.0)
    )
    sum_row[...] = jnp.sum(spread, axis=0, keepdims=True)
    copies = []
    for i in range(1, devices):
        copy = pltpu.make_async_remote_copy(
            src_ref=sum_row,
            dst_ref=sums.at[i],
            send_sem=sum_send.at[i],
            recv_sem=sum_recv.at[i],
            device_id={"space": lax.rem(me + i, devices)},
            device_id_type=MESH,
        )
        copy.start()
        copies.append(copy)
    for copy in copies:
        copy.wait()
    row = sum_row[...]
    for i in range(1, devices):
        row = row + sums[i]
    out_deficit[...] = row[:, :slices] * scales[1]
    out_theta[...] = row[:, slices : slices + 1] * scales[0]


def place_kernel(blocks, theta, deficit, out, out_theta, out_deficit, held_theta, held_deficit, small, sem):
    copies = [
        pltpu.make_async_copy(blocks.at[k], out.at[:, :, :, :, :, pl.ds(k * LANES, LANES)], sem.at[k])
        for k in range(blocks.shape[0])
    ]
    for copy in copies:
        copy.start()
    moves = [[(theta, held_theta), (held_theta, out_theta)], [(deficit, held_deficit), (held_deficit, out_deficit)]]
    for leg in range(2):
        short = [pltpu.make_async_copy(*move[leg], small.at[i]) for i, move in enumerate(moves)]
        for copy in short:
            copy.start()
        for copy in short:
            copy.wait()
    for copy in copies:
        copy.wait()


def greet(others):
    barrier = pltpu.get_barrier_semaphore()
    for other in others:
        pl.semaphore_signal(barrier, inc=1, device_id={"space": other}, device_id_type=MESH)
    return barrier


ANY = pl.BlockSpec(memory_space=pl.ANY)
HBM = pl.BlockSpec(memory_space=pltpu.HBM)


def call(kernel, number, out_shape, scratch, *args, in_specs=None, out_specs=None, limit=0):
    return pl.pallas_call(
        kernel,
        out_shape=out_shape,
        in_specs=in_specs or [VM] * len(args),
        out_specs=out_specs or jax.tree.map(lambda _: VM, out_shape),
        scratch_shapes=scratch,
        cost_estimate=pl.CostEstimate(flops=COST, bytes_accessed=COST // 1000, transcendentals=0),
        compiler_params=pltpu.CompilerParams(
            collective_id=number, has_side_effects=True, vmem_limit_bytes=limit * 1024
        ),
    )(*args)


def body(links):
    n = EXTENT
    slices, local = links.shape[0], links.shape[-1]
    devices = lax.axis_size("space")
    plane = n * n
    shape = lambda *s: jax.ShapeDtypeStruct(s, f32)
    vm = lambda *s: pltpu.VMEM(s, f32)
    dma = lambda *s: pltpu.SemaphoreType.DMA(s)
    group = devices // 2
    planes = n // 2
    nb = local // LANES
    assert group * 4 == 8 * slices and nb % UNITS == 0 and plane % (nb // UNITS * LANES) == 0
    rims = plane // (nb // UNITS * LANES)
    blocks = (nb, slices, 3, 2, 3, 2, LANES)
    times = lax.axis_size("tm")
    scales = (1.0 / (slices * times * n**3), 1.0 / n**3)
    placed, total, shares = call(
        functools.partial(gauge_kernel, n, group, scales),
        1,
        (shape(*blocks), shape(1, 1), shape(1, slices)),
        [
            vm(*blocks), vm(8, slices, local + plane), vm(8, slices, LANES),
            vm(18, slices, local + plane + LANES), vm(1, LANES), vm(devices, 1, LANES),
            dma(3), dma(3), dma(devices), dma(devices),
            vm(3, 8, slices, local), vm(8, slices, plane), vm(8, slices, LANES), vm(8, slices, LANES),
            vm(group, nb, 4, LANES), vm(group * nb + 1, 4, LANES), dma(nb), dma(rims + 2), dma(rims + 2),
            dma(UNITS, group), dma(UNITS, group), dma(group), dma(1),
            vm(group, plane // LANES, 4, LANES), vm(devices // 4 * (plane // LANES) + 1, 4, LANES),
            dma(rims, group), dma(rims, group // 2), dma(group), dma(1),
            vm(4, 8, plane), pltpu.VMEM((3, n, 3 * n), bf16), vm(2, LANES, LANES),
            vm(plane, LANES), vm(plane, LANES), vm(4 * planes, plane), vm(8, plane), vm(8, plane),
            vm(8, LANES), vm(8, LANES), vm(group * nb + 1, 4, LANES), vm(group, nb + plane // LANES, 4, LANES), vm(group, 1, 4, LANES),
            dma(PIECES + 1), dma(PIECES + 1), dma(UNITS + rims, group), dma(UNITS + rims, group), dma(2), dma(group),
        ],
        links,
        in_specs=[HBM],
        limit=GAUGE_KB,
    )
    new_links, total, shares = pl.pallas_call(
        place_kernel,
        out_shape=(shape(*links.shape), shape(1, 1), shape(1, slices)),
        in_specs=[VM, ANY, ANY],
        out_specs=(ANY, ANY, ANY),
        scratch_shapes=[vm(1, 1), vm(1, slices), dma(2), dma(nb)],
        compiler_params=pltpu.CompilerParams(vmem_limit_bytes=8 * 1024 * 1024),
    )(placed, total, shares)
    total = total.reshape(())
    if times > 1:
        total = lax.psum(total, "tm")
    return (new_links, total, shares.reshape(slices))


def solution(mesh):
    placed = (P("tm", None, None, None, None, "space"),)
    return jax.shard_map(
        body,
        mesh=mesh,
        in_specs=placed,
        out_specs=(P("tm", None, None, None, None, "space"), P(), P("tm")),
        check_vma=False,
    )
```

```python
import functools
import math

import jax
import jax.numpy as jnp
from jax import lax
from jax.experimental import pallas as pl
from jax.experimental.pallas import tpu as pltpu
from jax.sharding import PartitionSpec as P

EXTENT = 48
LANES = 128
UNITS = 3
PIECES = 6
COST = 10**9
GAUGE_KB = 50 * 1000

root_three = math.sqrt(3.0)
step_size = 0.08
top_momentum = 12.0

f32 = jnp.float32
bf16 = jnp.bfloat16
MESH = pl.DeviceIdType.MESH
VM = pl.BlockSpec(memory_space=pltpu.VMEM)


def cmul(p, q):
    return (p[0] * q[0] - p[1] * q[1], p[0] * q[1] + p[1] * q[0])


def cadd(p, q):
    return (p[0] + q[0], p[1] + q[1])


def csub(p, q):
    return (p[0] - q[0], p[1] - q[1])


def conj(p):
    return (p[0], -p[1])


def conj_mul(p, q):
    return (p[0] * q[0] + p[1] * q[1], p[0] * q[1] - p[1] * q[0])


def mul_conj(p, q):
    return (p[0] * q[0] + p[1] * q[1], p[1] * q[0] - p[0] * q[1])


def dot_row(row, col, mul):
    out = mul(row[0], col[0])
    for k in (1, 2):
        out = cadd(out, mul(row[k], col[k]))
    return out


def cross_conj(a, b):
    return [
        conj(csub(cmul(a[(k + 1) % 3], b[(k + 2) % 3]), cmul(a[(k + 2) % 3], b[(k + 1) % 3])))
        for k in range(3)
    ]


def algebra_of(u):
    return [
        u[0][1][1] + u[1][0][1],
        u[0][1][0] - u[1][0][0],
        u[0][0][1] - u[1][1][1],
        u[0][2][1] + u[2][0][1],
        u[0][2][0] - u[2][0][0],
        u[1][2][1] + u[2][1][1],
        u[1][2][0] - u[2][1][0],
        (u[0][0][1] + u[1][1][1] - 2.0 * u[2][2][1]) * (1.0 / root_three),
    ]


def rotation_of(s):
    h = 0.5 * step_size
    s = [v * h for v in s]
    third = s[7] * (1.0 / root_three)
    d0, d1, d2 = s[2] + third, third - s[2], -2.0 * third
    herm = [
        [(d0, None), (s[0], -s[1]), (s[3], -s[4])],
        [(s[0], s[1]), (d1, None), (s[5], -s[6])],
        [(s[3], s[4]), (s[5], s[6]), (d2, None)],
    ]

    def mul(p, q):
        if p[1] is None and q[1] is None:
            return (p[0] * q[0], jnp.zeros_like(p[0]))
        if p[1] is None:
            return (p[0] * q[0], p[0] * q[1])
        if q[1] is None:
            return (p[0] * q[0], p[1] * q[0])
        return cmul(p, q)

    rows = []
    for i in range(2):
        row = []
        for j in range(3):
            sq = dot_row(herm[i], [herm[k][j] for k in range(3)], mul)
            re, im = -0.5 * sq[0], -0.5 * sq[1]
            if herm[i][j][1] is not None:
                re = re - herm[i][j][1]
            else:
                re = re + 1.0
            row.append((re, im + herm[i][j][0]))
        rows.append(row)

    def unit(row):
        inv = lax.rsqrt(sum(p[0] * p[0] + p[1] * p[1] for p in row))
        return [(p[0] * inv, p[1] * inv) for p in row]

    one = unit(rows[0])
    corr = dot_row(one, rows[1], conj_mul)
    two = unit([csub(rows[1][k], cmul(corr, one[k])) for k in range(3)])
    return [one, two, cross_conj(one, two)]


def block(k):
    return pl.ds(pl.multiple_of(k * LANES, LANES), LANES)


def lane_ids(rows=8):
    return lax.broadcasted_iota(jnp.int32, (rows, LANES), 1)


def rows_of(slices, d, r, c, p):
    return pl.ds((d * 2 + r) * 6 + c * 2 + p, slices, stride=36)


def flat_block(ref, k):
    return ref.at[k].reshape(ref.shape[1] * 36, LANES)


def load_link(ref, slices, d):
    rows = [[tuple(ref[rows_of(slices, d, r, c, p), :] for p in range(2)) for c in range(3)] for r in range(2)]
    return rows + [cross_conj(rows[0], rows[1])]


def site_of(k, extent):
    start = k * LANES
    shifted = lane_ids() + lax.rem(start, extent)
    wraps = sum((shifted >= extent * i).astype(jnp.int32) for i in range(1, (LANES + extent - 1) // extent + 1))
    return shifted - extent * wraps, lax.div(start, extent) + wraps


def at_z(row, z, me, rows, extent):
    first = lax.rem(extent + z + 1 - lax.rem(me * rows, extent), extent)
    hit = row == first
    for i in range(1, -(-rows // extent)):
        hit = hit | (row == first + i * extent)
    return hit


def fetch_block(links, held, sem, k, start=0):
    return pltpu.make_async_copy(links.at[:, :, :, :, :, pl.ds(k * LANES, LANES)], held.at[k - start], sem.at[k])


def split3(x):
    hi = x.astype(bf16)
    lo = (x - hi.astype(f32)).astype(bf16)
    return jnp.concatenate([hi, lo, hi], axis=0)


def transform(table, parts):
    both = jnp.dot(table, split3(jnp.concatenate(parts, axis=1)), preferred_element_type=f32)
    return [both[:, i * LANES : (i + 1) * LANES] for i in range(len(parts))]


def swap(v):
    return pltpu.roll(v, 4, 0)


def flip(place, i, group):
    other = place
    for b in range(group.bit_length() - 1):
        if i >> b & 1:
            other = other + (1 << b) * (1 - 2 * lax.rem(lax.div(place, 1 << b), 2))
    return other


def iota(shape, axis):
    return lax.broadcasted_iota(jnp.int32, shape, axis).astype(f32)


def divide(v, n):
    whole = jnp.floor((v + 0.5) * (1.0 / n))
    return whole, v - n * whole


def send_order(group):
    axes = group.bit_length() - 2
    hops = lambda i: bin(i >> 1).count("1")
    near = sorted((i for i in range(2, group) if hops(i) == 1), key=lambda i: (i & 1, -i))
    far = sorted((i for i in range(2, group) if hops(i) > 1), key=lambda i: (-hops(i), -i))
    order = []
    while near:
        order += far[:1] + near[:axes]
        far, near = far[1:], near[axes:]
    return order + far + [1]


def make_tables(n, planes, wave, tables, zero):
    shape = (n, 3 * n)
    row = iota(shape, 0)
    third, col = divide(iota(shape, 1), n)
    for i, turn in enumerate([row * col, row * (col + (n - 1.0)), col * (row + (n - 1.0))]):
        angle = divide(turn, n)[1] * (2.0 * math.pi / n)
        full = (jnp.cos(angle) + jnp.sin(angle)) * (1.0 / math.sqrt(n))
        high = full.astype(bf16).astype(f32)
        tables[i] = jnp.where(third == 2.0, full - high, high).astype(bf16)
    mode = iota((8, n * n), 1)
    p = jnp.zeros((8, n * n), f32)
    for k in divide(mode, n):
        s = jnp.sin(k * (math.pi / n))
        p = p + 4.0 * s * s
    p = jnp.where(mode == 0.0, 1.0, p)
    root = jnp.sqrt(p + 0.25 * p * p)
    mu = 1.0 / (1.0 + 0.5 * p + root)
    power = lax.integer_pow(mu, planes)
    close = 1.0 / (1.0 - power * power)
    for i, v in enumerate([mu, (0.5 * top_momentum) / root, close, close * power]):
        wave[i] = jnp.where(mode == 0.0, 0.0, v)
    square = (LANES, LANES)
    source, sub = divide(iota(square, 0), 4)
    target, lane = divide(iota(square, 1), 4)
    used = (sub == lane) & (source < planes) & (target < planes)
    for i in range(2):
        d = divide(target - source + (n + i * planes * 1.0), n)[1]
        green = top_momentum * ((n * n - 1.0) / (12.0 * n) - d * (n - d) * (0.5 / n))
        zero[i] = jnp.where(used, green, 0.0)


def link_part(extent, held, smooth, arrive, mend_edges, done, below, rot, halo_send, halo_recv, n):
    nb, slices = held.shape[0], held.shape[1]
    yb = extent * extent // LANES
    unit = nb // UNITS
    q = nb * LANES // extent
    mid = (extent // 2) * extent
    lane = lane_ids()
    me = lax.axis_index("space")
    ahead, behind = lax.rem(me + 1, n), lax.rem(me + n - 1, n)
    def rotate(values, sl):
        g = rotation_of(values)
        for i in range(3):
            for j in range(3):
                for p in range(2):
                    rot[6 * i + 2 * j + p, :, sl] = g[i][j][p]

    def rotate_own(k, carry):
        rotate([smooth[a, :, block(k)] for a in range(8)], block(k))
        return carry

    def halo(i, source, dest, other):
        return pltpu.make_async_remote_copy(
            src_ref=source,
            dst_ref=dest,
            send_sem=halo_send.at[i],
            recv_sem=halo_recv.at[i],
            device_id={"space": other},
            device_id_type=MESH,
        )

    def span(start, size):
        return pl.ds(pl.multiple_of(start * LANES, LANES), size * LANES)

    odd = lax.rem(me, 2)
    pick = yb - odd * (yb - mid // LANES)
    below_copy = halo(0, smooth.at[:, :, span(pick, 1)], below, ahead)
    rims = [
        halo(1 + i, smooth.at[:, :, span(i * unit, unit)], smooth.at[:, :, span(nb + i * unit, unit)], behind)
        for i in range(2)
    ]

    def turn(v):
        lax.fori_loop(v * unit, (v + 1) * unit, rotate_own, 0)

    def step(which, k, total):
        sl = block(k)
        before = block(jnp.maximum(k - 1, 0))
        after = block(k + 1)
        wrap = block(jnp.where(k == yb, 0, nb + yb))
        x_at, row = site_of(k, extent)
        edge_x = x_at == extent - 1
        edge_z = at_z(row, extent - 1, me, q, extent)

        def ahead_x(e):
            cur = rot[e, :, sl]
            near = pltpu.roll(jnp.where(lane == 0, rot[e, :, after], cur), LANES - 1, 1)
            far = pltpu.roll(jnp.where(lane >= LANES - extent + 1, rot[e, :, before], cur), extent - 1, 1)
            return jnp.where(edge_x, far, near)

        def ahead_y(e):
            return rot[e, :, block(k + yb)]

        def ahead_z(e):
            cur = rot[e, :, sl]
            near = pltpu.roll(jnp.where(lane < extent, rot[e, :, after], cur), LANES - extent, 1)
            far = pltpu.roll(rot[e, :, wrap], LANES - extent, 1)
            return jnp.where(edge_z, far, near)

        flat_out = flat_block(done, k)
        for d in which:
            forward = (ahead_x, ahead_y, ahead_z)[d]
            u = load_link(flat_block(held, k), slices, d)
            own = [[(rot[6 * i + 2 * j, :, sl], rot[6 * i + 2 * j + 1, :, sl]) for j in range(3)] for i in range(2)]
            left = [
                [dot_row(own[i], [u[k2][j] for k2 in range(3)], cmul) for j in range(3)]
                for i in range(2)
            ]
            made = []
            for j in range(3):
                row3 = [(forward(6 * j + 2 * c), forward(6 * j + 2 * c + 1)) for c in range(3)]
                for i in range(2):
                    v = dot_row(left[i], row3, mul_conj)
                    flat_out[rows_of(slices, d, i, j, 0), :] = v[0]
                    flat_out[rows_of(slices, d, i, j, 1), :] = v[1]
                    if j < 2:
                        made.append(v)
            p00, p10, p01, p11 = made
            minor = csub(cmul(p00, p11), cmul(p01, p10))[0]
            total = total + ((1.0 - p00[0]) + (1.0 - p11[0]) + (1.0 - minor))
        return total

    def links_of(start, stop, dirs, total):
        return lax.fori_loop(start, stop, functools.partial(step, dirs), total)

    arrive(odd)
    arrive(odd + 2)
    mend_edges()
    turn(odd)
    turn(odd + 2)

    @pl.when(odd == 1)
    def _():
        rims[1].start()

    below_copy.start()
    start = odd * unit
    total = links_of(start, start + 1, (1,), jnp.zeros((8, LANES), f32))
    total = links_of(start + 1, start + unit - 1, (0, 1, 2), total)
    total = links_of(start + unit - 1, start + unit, (1,), total)
    total = links_of(2 * unit + 1, 2 * unit + 1 + (1 - odd) * (unit - 2), (0, 2), total)
    arrive(1 - odd)
    turn(1 - odd)

    @pl.when(odd == 1)
    def _():
        rims[0].start()
        for v in (2, 4):
            arrive(jnp.int32(v))
            turn(v)

    below_copy.wait_recv()
    rotate([below[a] for a in range(8)], block(nb + yb))
    total = links_of(0, start + 1, (0, 2), total)
    total = links_of(start + unit - 1, 2 * unit + 1 + odd * (unit - 2), (0, 2), total)

    @pl.when(odd == 0)
    def _():
        for v in (3, 4):
            rims[v - 3].wait_recv()
            turn(v)

    total = links_of((1 - odd) * unit, (2 - odd) * unit, (1,), total)
    total = links_of(2 * unit, nb - 1, (1,), total)
    total = links_of(nb - 1, nb, (0, 1, 2), total)
    below_copy.wait_send()

    @pl.when(odd == 1)
    def _():
        for copy in rims:
            copy.wait_send()

    return total


def gauge_kernel(
    extent, group, scales, links, done, out_theta, out_deficit, *refs
):
    (
        held_links, smooth, below, rot, sum_row, sums, late_send, late_recv, sum_send, sum_recv,
        alg, y_rim, z_below, z_above, mine, fields, load_sem, halo_send, halo_recv,
        in_send_sem, in_recv_sem, in_edge_send, in_edge_recv,
        extra, extra_held, extra_send, extra_recv, tip_send, tip_recv, wave, tables, zero, one, two, modes, ends, far, mode, far_mode, outgo, held, edge_held,
        end_send, end_recv, send_sem, recv_sem, edge_send, edge_recv,
    ) = refs
    devices = 2 * group
    nb, slices = mine.shape[1], alg.shape[2]
    yb = extent * extent // LANES
    half = slices // 2
    unit = nb // UNITS
    q = nb * LANES // extent
    mid = (extent // 2) * extent
    lane = lane_ids()
    me = lax.axis_index("space")
    place = lax.rem(me, group)
    base = me - place
    beyond = group - base
    ahead, behind = lax.rem(me + 1, devices), lax.rem(me + devices - 1, devices)
    in_spans = [(0, 1)] + [(i * unit, (i + 1) * unit) for i in range(1, UNITS)] + [(1, unit)]
    in_loads = [[fetch_block(links, held_links, load_sem, k) for k in range(a, b)] for a, b in in_spans]
    for copy in sum(in_loads, []):
        copy.start()
    barrier = greet([base + flip(place, i, group) for i in range(1, group)] + [beyond + i for i in range(group)])

    first = nb - yb

    def algebra(i):
        start, stop = in_spans[i]

        def step(k, carry):
            flat = flat_block(held_links, k)
            for d in range(3):
                for a, v in enumerate(algebra_of(load_link(flat, slices, d))):
                    alg[d, a, :, block(k)] = v
                    if d == 1 and start >= first:
                        extra[2 * a, k - first] = v[:half]
                        extra[2 * a + 1, k - first] = v[half:]
            return carry

        for copy in in_loads[i]:
            copy.wait()
        lax.fori_loop(start, stop, step, 0)

    def halo(i, source, dest, other):
        return pltpu.make_async_remote_copy(
            src_ref=source,
            dst_ref=dest,
            send_sem=halo_send.at[i],
            recv_sem=halo_recv.at[i],
            device_id={"space": other},
            device_id_type=MESH,
        )

    def span(start, size):
        return pl.ds(pl.multiple_of(start * LANES, LANES), size * LANES)

    rims = [
        halo(i, alg.at[1, :, :, span(first + i * unit, unit)], y_rim.at[:, :, span(i * unit, unit)], ahead)
        for i in range(yb // unit)
    ]
    below_copy = halo(len(rims), alg.at[2, :, :, span(nb - 1, 1)], z_below, ahead)
    odd = lax.rem(me, 2)
    above_copy = halo(len(rims) + 1, alg.at[2, :, :, span(odd * (mid // LANES), 1)], z_above, behind)

    last = lax.div(place + 1, group)
    next_base = base + last * (beyond - base)
    slot = lax.div(lax.rem(place + 1, group), 2)

    def extra_copy(u, i):
        other = flip(place, i, group)
        return pltpu.make_async_remote_copy(
            src_ref=extra.at[other, pl.ds(u * unit, unit)],
            dst_ref=extra_held.at[pl.ds(slot * yb + u * unit, unit)],
            send_sem=extra_send.at[u, i],
            recv_sem=extra_recv.at[u, slot],
            device_id={"space": next_base + other},
            device_id_type=MESH,
        )

    def tip_copy(i):
        other = flip(place, i, group)
        return pltpu.make_async_remote_copy(
            src_ref=extra.at[other, pl.ds(0, 1)],
            dst_ref=extra_held.at[pl.ds(group // 2 * yb, 1)],
            send_sem=tip_send.at[i],
            recv_sem=tip_recv.at[0],
            device_id={"space": base + other},
            device_id_type=MESH,
        )

    def send_rim(u):
        @pl.when(odd == 0)
        def _():
            rims[u].start()

        @pl.when(odd == 1)
        def _():
            for i in send_order(group):
                extra_copy(u, i).start()

        @pl.when(last == 1)
        def _():
            extra_copy(u, 0).start()

    algebra(0)
    algebra(1)
    pl.semaphore_wait(barrier, devices - 1)
    above_copy.start()
    send_rim(0)
    for i in range(1, len(rims)):
        algebra(1 + i)
        if i == len(rims) - 1:
            below_copy.start()
        send_rim(i)

    @pl.when(last == 1)
    def _():
        for i in range(1, group):
            tip_copy(i).start()
        extra_held[group // 2 * yb] = extra[place, 0]

    @pl.when(odd == 0)
    def _():
        y_rim[...] = jnp.zeros_like(y_rim)

    algebra(UNITS)

    @pl.when((odd == 1) & (last == 0))
    def _():
        def keep_extra(k, carry):
            extra_held[slot * yb + k] = extra[place, k]
            return carry

        lax.fori_loop(0, yb, keep_extra, 0)

    def step(k, carry):
        sl = block(k)
        before = block(jnp.maximum(k - 1, 0))
        after = block(jnp.minimum(k + 1, nb - 1))
        x_at, row = site_of(k, extent)
        edge_x = x_at == 0
        edge_z = at_z(row, 0, me, q, extent)
        for a in range(8):
            x, y, z = alg[0, a, :, sl], alg[1, a, :, sl], alg[2, a, :, sl]
            near = pltpu.roll(jnp.where(lane == LANES - 1, alg[0, a, :, before], x), 1, 1)
            far = pltpu.roll(jnp.where(lane < extent - 1, alg[0, a, :, after], x), LANES - extent + 1, 1)
            bx = jnp.where(edge_x, far, near)
            by = jnp.where(
                k < yb,
                y_rim[a, :, block(jnp.minimum(k, yb - 1))],
                alg[1, a, :, block(jnp.maximum(k - yb, 0))],
            )
            prev = jnp.where(k == 0, z_below[a], alg[2, a, :, before])
            near = pltpu.roll(jnp.where(lane >= LANES - extent, prev, z), extent, 1)
            far = pltpu.roll(jnp.where(k == 0, alg[2, a, :, block(yb)], z_above[a]), extent, 1)
            bz = jnp.where(edge_z, far, near)
            b = (bx - x) + (by - y) + (bz - z)
            mine[2 * a, k] = b[:half]
            mine[2 * a + 1, k] = b[half:]
        return carry

    def in_edge_copy(i):
        return pltpu.make_async_remote_copy(
            src_ref=mine.at[i, pl.ds(0, 1)],
            dst_ref=fields.at[pl.ds(group * nb, 1)],
            send_sem=in_edge_send.at[i],
            recv_sem=in_edge_recv.at[0],
            device_id={"space": beyond + i},
            device_id_type=MESH,
        )

    above_copy.wait_recv()
    below_copy.wait_recv()

    @pl.when(odd == 1)
    def _():
        for copy in rims:
            copy.wait_recv()

    def in_copy(u, i):
        other = flip(place, i, group)
        return pltpu.make_async_remote_copy(
            src_ref=mine.at[other, pl.ds(u * unit, unit)],
            dst_ref=fields.at[pl.ds(place * nb + u * unit, unit)],
            send_sem=in_send_sem.at[u, i],
            recv_sem=in_recv_sem.at[u, i],
            device_id={"space": base + other},
            device_id_type=MESH,
        )

    for c, u in enumerate([2 - odd, 2 * odd, 1 - odd]):
        lax.fori_loop(u * unit, (u + 1) * unit, step, 0)
        for i in send_order(group):
            in_copy(u, i).start()
        if c == 1:

            @pl.when(place == 0)
            def _():
                for i in range(group):
                    in_edge_copy(i).start()

    make_tables(extent, extent // 2, wave, tables, zero)

    def keep(k, carry):
        fields[place * nb + k] = mine[place, k]
        return carry

    lax.fori_loop(0, nb, keep, 0)
    for copy in [below_copy, above_copy]:
        copy.wait_send()

    @pl.when(odd == 0)
    def _():
        for copy in rims:
            copy.wait_send()

    @pl.when(odd == 1)
    def _():
        for u in range(len(rims)):
            for i in range(1, group):
                extra_copy(u, i).wait_send()

    @pl.when(last == 1)
    def _():
        for u in range(len(rims)):
            extra_copy(u, 0).wait_send()
        for i in range(1, group):
            tip_copy(i).wait_send()

    in_edge_copy(0).wait_recv()

    @pl.when(last == 0)
    def _():
        tip_copy(1).wait_recv()

    def wait_extra(u, m):
        @pl.when(place != 2 * m - 1)
        def _():
            pltpu.make_async_remote_copy(
                src_ref=extra.at[0, pl.ds(u * unit, unit)],
                dst_ref=extra_held.at[pl.ds(m * yb + u * unit, unit)],
                send_sem=extra_send.at[u, 0],
                recv_sem=extra_recv.at[u, m],
                device_id={"space": beyond},
                device_id_type=MESH,
            ).wait_recv()

    def wait_side(side):
        for i in send_order(group):
            parity = lax.rem(place + i + side, 2)
            in_copy(parity, i).wait_recv()

            @pl.when(parity == 0)
            def _():
                in_copy(jnp.int32(2), i).wait_recv()

        for m in range(group // 2):
            wait_extra(side, m)

    @pl.when(place == 0)
    def _():
        for i in range(group):
            in_edge_copy(i).wait_send()

    n = extent
    planes = group * nb * LANES // (n * n)
    columns = n * n // LANES
    pairs = planes // 2
    lanes = planes * 4
    per = columns // PIECES
    upper = lax.broadcasted_iota(jnp.int32, (8, LANES), 0) >= 4
    x_table, z_table, z_back = (tables.at[i] for i in range(3))
    decay, weight = wave.at[0], wave.at[1]
    close = wave.at[pl.ds(2, 2)]
    own_zero, far_zero = zero.at[0], zero.at[1]
    def rows_at(i):
        return pl.ds(pl.multiple_of(i * n, 8), n)

    def turn_in(c, tip):
        tiles = [fields[y * columns + c] for y in range(planes)]
        for m in range(group // 2):
            y = m * (planes // (group // 2))
            tiles[y] = tiles[y] + extra_held[m * yb + c]
        tiles = tiles + tip
        rest = LANES - 4 * len(tiles)
        full = jnp.concatenate(tiles + [jnp.zeros((rest, LANES), f32)], axis=0)
        one[block(c), :] = full.T
        return full

    def turn_rest(c, total):
        full = turn_in(c, [])
        return total + sum(full[8 * i : 8 * i + 8] * full[8 * i : 8 * i + 8] for i in range(lanes // 8))

    def along_x(i, carry):
        parts = [one[rows_at(2 * i + e), :] for e in range(2)]
        for e, v in enumerate(transform(x_table[...], parts)):
            two[rows_at(2 * i + e), :] = v
        return carry

    theta = jnp.zeros((8, LANES), f32)
    for side in range(2):
        wait_side(side)
        theta = lax.fori_loop(side * unit, (side + 1) * unit, turn_rest, theta, unroll=3)
        if side == 0:
            turn_in(0, [fields[planes * columns] + extra_held[group // 2 * yb]])
            one[0:n, :] = pltpu.roll(one[0:n, :], LANES - 4, 1)
        lax.fori_loop(side * n // 4, (side + 1) * n // 4, along_x, 0, unroll=4)
    for u in range(UNITS):
        for i in range(1, group):
            in_copy(u, i).wait_send()

    def along_z(i, carry):
        parts = [two[pl.ds(2 * i + e, n, stride=n), :] for e in range(2)]
        for e, v in enumerate(transform(z_table[...], parts)):
            one[rows_at(2 * i + e), :] = v
        return carry

    def end_copy(p):
        cols = pl.ds(p * per * LANES, per * LANES)
        return pltpu.make_async_remote_copy(
            src_ref=ends.at[:, cols],
            dst_ref=far.at[:, cols],
            send_sem=end_send.at[p],
            recv_sem=end_recv.at[p],
            device_id={"space": beyond + place},
            device_id_type=MESH,
        )

    mode_copy = pltpu.make_async_remote_copy(
        src_ref=mode,
        dst_ref=far_mode,
        send_sem=end_send.at[PIECES],
        recv_sem=end_recv.at[PIECES],
        device_id={"space": beyond + place},
        device_id_type=MESH,
    )

    def reduce_ends(c, carry):
        sl = block(c)
        modes[:, sl] = one[sl, :].T[:lanes]
        mu = decay[:, sl]
        mu2 = mu * mu
        low = jnp.where(upper, 1.0, mu)
        high = jnp.where(upper, mu, 1.0)
        fwd = modes[0:8, sl]
        bwd = modes[lanes - 8 : lanes, sl]
        for i in range(1, pairs):
            fwd = fwd * mu2 + modes[8 * i : 8 * i + 8, sl]
            bwd = bwd * mu2 + modes[lanes - 8 - 8 * i : lanes - 8 * i, sl]
        ends[:, sl] = jnp.where(upper, high * bwd + low * swap(bwd), low * fwd + high * swap(fwd))
        return carry

    step_z = n // 2 // PIECES
    for p in range(PIECES):
        lax.fori_loop(p * step_z, (p + 1) * step_z, along_z, 0, unroll=4)
        if p == 0:
            mode[...] = one[0:8, :]
        lax.fori_loop(p * per, (p + 1) * per, reduce_ends, 0, unroll=per)
        if p == 0:
            mode_copy.start()
        end_copy(p).start()

    def sweep(c, carry):
        sl = block(c)
        mu = decay[:, sl]
        mu2 = mu * mu
        low = jnp.where(upper, 1.0, mu)
        high = jnp.where(upper, mu, 1.0)
        total = close[0, :, sl] * far[:, sl] + close[1, :, sl] * ends[:, sl]
        turned = swap(total)
        e = jnp.where(upper, turned, total)
        f = jnp.where(upper, total, turned) * mu
        w = weight[:, sl]
        up = mu * high
        down = jnp.where(upper, 0.0, mu)
        rising = []
        for i in range(pairs):
            v = modes[8 * i : 8 * i + 8, sl]
            s = low * v + high * swap(v)
            rising.append(jnp.where(upper, s, v) + up * e)
            e = mu2 * e + s
        done = [None] * pairs
        for i in reversed(range(pairs)):
            v = modes[8 * i : 8 * i + 8, sl]
            t = swap(v)
            done[i] = w * (rising[i] + low * f + down * t)
            f = mu2 * f + mu * (high * v + low * t)
        full = jnp.concatenate(done + [jnp.zeros((LANES - lanes, LANES), f32)], axis=0)
        one[sl, :] = full.T
        return carry

    def back_z(i, carry):
        parts = [one[rows_at(2 * i + e), :] for e in range(2)]
        for e, v in enumerate(transform(z_back[...], parts)):
            two[pl.ds(2 * i + e, n, stride=n), :] = v
        return carry

    for p in range(PIECES):
        end_copy(p).wait_recv()
        if p == 0:
            mode_copy.wait_recv()
        lax.fori_loop(p * per, (p + 1) * per, sweep, 0, unroll=per)
        if p == 0:
            exact = functools.partial(jnp.dot, preferred_element_type=f32, precision=lax.Precision.HIGHEST)
            flat = exact(mode[...], own_zero[...]) + exact(far_mode[...], far_zero[...])
            first = lax.broadcasted_iota(jnp.int32, (8, LANES), 0) == 0
            one[0:8, :] = jnp.where(first, flat, one[0:8, :])
        lax.fori_loop(p * step_z, (p + 1) * step_z, back_z, 0, unroll=4)

    def back_x(i, carry):
        parts = [two[rows_at(2 * i + e), :] for e in range(2)]
        for e, v in enumerate(transform(x_table[...], parts)):
            one[rows_at(2 * i + e), :] = v
        return carry

    def turn_out(c):
        full = one[block(c), :].T
        for y in range(planes):
            outgo[y * columns + c] = full[4 * y : 4 * y + 4]
        return full

    def turn_out_rest(c, carry):
        turn_out(c)
        return carry

    def unit_copy(i, v):
        other = flip(place, i, group)
        wrap = lax.div(v, UNITS) * lax.div(other + 1, group)
        return pltpu.make_async_remote_copy(
            src_ref=outgo.at[pl.ds(other * nb + v * unit - wrap * (planes * columns), unit)],
            dst_ref=held.at[place, pl.ds(v * unit, unit)],
            send_sem=send_sem.at[v, i],
            recv_sem=recv_sem.at[v, i],
            device_id={"space": base + other + wrap * (beyond - base)},
            device_id_type=MESH,
        )

    def edge_copy(i, other):
        return pltpu.make_async_remote_copy(
            src_ref=outgo.at[pl.ds(planes * columns, 1)],
            dst_ref=edge_held.at[place],
            send_sem=edge_send.at[i],
            recv_sem=edge_recv.at[place],
            device_id={"space": other},
            device_id_type=MESH,
        )

    edges = [edge_copy(0, beyond), edge_copy(1, base + group - 1)]

    def each_unit(side, act):
        for i in send_order(group):
            parity = lax.rem(place + i, 2)
            if side == 0:
                act(unit_copy(i, parity))
                act(unit_copy(i, parity + 2))
            else:
                act(unit_copy(i, 1 - parity))

                @pl.when(parity == 1)
                def _():
                    act(unit_copy(i, jnp.int32(2)))
                    act(unit_copy(i, jnp.int32(4)))

        @pl.when(last == 1)
        def _():
            act(unit_copy(0, jnp.int32(3 + side)))

    for side in range(2):
        lax.fori_loop(side * n // 4, (side + 1) * n // 4, back_x, 0, unroll=4)
        if side == 0:
            one[0:n, :] = pltpu.roll(one[0:n, :], 4, 1)
            outgo[planes * columns] = turn_out(0)[lanes : lanes + 4]
        lax.fori_loop(side * unit, (side + 1) * unit, turn_out_rest, 0, unroll=3)
        if side == 0:
            edges[0].start()

            @pl.when(last == 0)
            def _():
                edges[1].start()

        each_unit(side, lambda copy: copy.start())

    def keep(k, carry):
        held[place, k] = outgo[place * nb + k]
        return carry

    lax.fori_loop(0, nb, keep, 0)

    @pl.when((odd == 1) & (last == 0))
    def _():
        lax.fori_loop(nb, nb + yb, keep, 0)

    @pl.when(last == 1)
    def _():
        edge_held[place] = outgo[planes * columns : planes * columns + 1]

    def edge_wait(i):
        pltpu.make_async_remote_copy(
            src_ref=outgo.at[pl.ds(planes * columns, 1)],
            dst_ref=edge_held.at[i],
            send_sem=edge_send.at[0],
            recv_sem=edge_recv.at[i],
            device_id={"space": beyond},
            device_id_type=MESH,
        ).wait_recv()

    def mend(start):
        for a in range(8):
            row = jnp.concatenate([edge_held[2 * a, 0], edge_held[2 * a + 1, 0]], axis=0)
            smooth[a, :, start : start + LANES] = jnp.where(
                lane_ids() < n, row, smooth[a, :, start : start + LANES]
            )

    def gather(k, carry):
        for a in range(8):
            smooth[a, :, block(k)] = jnp.concatenate([held[2 * a, k], held[2 * a + 1, k]], axis=0)
        return carry

    def arrive(v):
        for i in send_order(group):
            unit_copy(i, v).wait_recv()

        @pl.when(last * lax.div(v, UNITS) == 1)
        def _():
            unit_copy(0, v).wait_recv()

        lax.fori_loop(v * unit, (v + 1) * unit, gather, 0)

    def mend_edges():
        @pl.when(place == 0)
        def _():
            for i in range(group):
                edge_wait(i)
            mend(0)

        @pl.when(last == 1)
        def _():
            for i in range(group - 1):
                edge_wait(i)
            mend(nb * LANES)

    total = link_part(extent, held_links, smooth, arrive, mend_edges, done, below, rot, late_send, late_recv, devices)
    for p in range(PIECES):
        end_copy(p).wait_send()
    mode_copy.wait_send()
    edges[0].wait_send()

    @pl.when(last == 0)
    def _():
        edges[1].wait_send()

    for side in range(2):
        each_unit(side, lambda copy: copy.wait_send())


    wide_lane = lane_ids(slices)
    t = jnp.sum(jnp.sum(theta, axis=1, keepdims=True), axis=0, keepdims=True)
    d = jnp.sum(total, axis=1, keepdims=True)
    own_row = lax.broadcasted_iota(jnp.int32, (slices, LANES), 0)
    spread = jnp.where(
        wide_lane == own_row, d, jnp.where(wide_lane == slices, jnp.where(own_row == 0, t, 0.0), 0.0)
    )
    sum_row[...] = jnp.sum(spread, axis=0, keepdims=True)
    copies = []
    for i in range(1, devices):
        copy = pltpu.make_async_remote_copy(
            src_ref=sum_row,
            dst_ref=sums.at[i],
            send_sem=sum_send.at[i],
            recv_sem=sum_recv.at[i],
            device_id={"space": lax.rem(me + i, devices)},
            device_id_type=MESH,
        )
        copy.start()
        copies.append(copy)
    for copy in copies:
        copy.wait()
    row = sum_row[...]
    for i in range(1, devices):
        row = row + sums[i]
    out_deficit[...] = row[:, :slices] * scales[1]
    out_theta[...] = row[:, slices : slices + 1] * scales[0]


def place_kernel(blocks, theta, deficit, out, out_theta, out_deficit, small, sem):
    copies = [
        pltpu.make_async_copy(blocks.at[k], out.at[:, :, :, :, :, pl.ds(k * LANES, LANES)], sem.at[k])
        for k in range(blocks.shape[0])
    ]
    copies = [
        pltpu.make_async_copy(theta, out_theta, small.at[0]),
        pltpu.make_async_copy(deficit, out_deficit, small.at[1]),
    ] + copies
    for copy in copies:
        copy.start()
    for copy in copies:
        copy.wait()


def greet(others):
    barrier = pltpu.get_barrier_semaphore()
    for other in others:
        pl.semaphore_signal(barrier, inc=1, device_id={"space": other}, device_id_type=MESH)
    return barrier


ANY = pl.BlockSpec(memory_space=pl.ANY)
HBM = pl.BlockSpec(memory_space=pltpu.HBM)


def call(kernel, number, out_shape, scratch, *args, in_specs=None, out_specs=None, limit=0):
    return pl.pallas_call(
        kernel,
        out_shape=out_shape,
        in_specs=in_specs or [VM] * len(args),
        out_specs=out_specs or jax.tree.map(lambda _: VM, out_shape),
        scratch_shapes=scratch,
        cost_estimate=pl.CostEstimate(flops=COST, bytes_accessed=COST // 1000, transcendentals=0),
        compiler_params=pltpu.CompilerParams(
            collective_id=number, has_side_effects=True, vmem_limit_bytes=limit * 1024
        ),
    )(*args)


def body(links):
    n = EXTENT
    slices, local = links.shape[0], links.shape[-1]
    devices = lax.axis_size("space")
    plane = n * n
    shape = lambda *s: jax.ShapeDtypeStruct(s, f32)
    vm = lambda *s: pltpu.VMEM(s, f32)
    dma = lambda *s: pltpu.SemaphoreType.DMA(s)
    group = devices // 2
    planes = n // 2
    nb = local // LANES
    assert group * 4 == 8 * slices and nb % UNITS == 0 and plane % (nb // UNITS * LANES) == 0
    rims = plane // (nb // UNITS * LANES)
    blocks = (nb, slices, 3, 2, 3, 2, LANES)
    times = lax.axis_size("tm")
    scales = (1.0 / (slices * times * n**3), 1.0 / n**3)
    placed, total, shares = call(
        functools.partial(gauge_kernel, n, group, scales),
        1,
        (shape(*blocks), shape(1, 1), shape(1, slices)),
        [
            vm(*blocks), vm(8, slices, local + plane), vm(8, slices, LANES),
            vm(18, slices, local + plane + LANES), vm(1, LANES), vm(devices, 1, LANES),
            dma(3), dma(3), dma(devices), dma(devices),
            vm(3, 8, slices, local), vm(8, slices, plane), vm(8, slices, LANES), vm(8, slices, LANES),
            vm(group, nb, 4, LANES), vm(group * nb + 1, 4, LANES), dma(nb), dma(rims + 2), dma(rims + 2),
            dma(UNITS, group), dma(UNITS, group), dma(group), dma(1),
            vm(group, plane // LANES, 4, LANES), vm(devices // 4 * (plane // LANES) + 1, 4, LANES),
            dma(rims, group), dma(rims, group // 2), dma(group), dma(1),
            vm(4, 8, plane), pltpu.VMEM((3, n, 3 * n), bf16), vm(2, LANES, LANES),
            vm(plane, LANES), vm(plane, LANES), vm(4 * planes, plane), vm(8, plane), vm(8, plane),
            vm(8, LANES), vm(8, LANES), vm(group * nb + 1, 4, LANES), vm(group, nb + plane // LANES, 4, LANES), vm(group, 1, 4, LANES),
            dma(PIECES + 1), dma(PIECES + 1), dma(UNITS + rims, group), dma(UNITS + rims, group), dma(2), dma(group),
        ],
        links,
        in_specs=[HBM],
        limit=GAUGE_KB,
    )
    new_links, total, shares = pl.pallas_call(
        place_kernel,
        out_shape=(shape(*links.shape), shape(1, 1), shape(1, slices)),
        in_specs=[VM, VM, VM],
        out_specs=(ANY, ANY, ANY),
        scratch_shapes=[dma(2), dma(nb)],
        compiler_params=pltpu.CompilerParams(vmem_limit_bytes=8 * 1024 * 1024),
    )(placed, total, shares)
    total = total.reshape(())
    if times > 1:
        total = lax.psum(total, "tm")
    return (new_links, total, shares.reshape(slices))


def solution(mesh):
    placed = (P("tm", None, None, None, None, "space"),)
    return jax.shard_map(
        body,
        mesh=mesh,
        in_specs=placed,
        out_specs=(P("tm", None, None, None, None, "space"), P(), P("tm")),
        check_vma=False,
    )
```

```python
import functools
import math

import jax
import jax.numpy as jnp
from jax import lax
from jax.experimental import pallas as pl
from jax.experimental.pallas import tpu as pltpu
from jax.sharding import PartitionSpec as P

EXTENT = 48
LANES = 128
UNITS = 3
PIECES = 6
COST = 10**9
GAUGE_KB = 50 * 1000

root_three = math.sqrt(3.0)
step_size = 0.08
top_momentum = 12.0

f32 = jnp.float32
bf16 = jnp.bfloat16
MESH = pl.DeviceIdType.MESH
VM = pl.BlockSpec(memory_space=pltpu.VMEM)


def cmul(p, q):
    return (p[0] * q[0] - p[1] * q[1], p[0] * q[1] + p[1] * q[0])


def cadd(p, q):
    return (p[0] + q[0], p[1] + q[1])


def csub(p, q):
    return (p[0] - q[0], p[1] - q[1])


def conj(p):
    return (p[0], -p[1])


def conj_mul(p, q):
    return (p[0] * q[0] + p[1] * q[1], p[0] * q[1] - p[1] * q[0])


def mul_conj(p, q):
    return (p[0] * q[0] + p[1] * q[1], p[1] * q[0] - p[0] * q[1])


def dot_row(row, col, mul):
    out = mul(row[0], col[0])
    for k in (1, 2):
        out = cadd(out, mul(row[k], col[k]))
    return out


def cross_conj(a, b):
    return [
        conj(csub(cmul(a[(k + 1) % 3], b[(k + 2) % 3]), cmul(a[(k + 2) % 3], b[(k + 1) % 3])))
        for k in range(3)
    ]


def algebra_of(u):
    return [
        u[0][1][1] + u[1][0][1],
        u[0][1][0] - u[1][0][0],
        u[0][0][1] - u[1][1][1],
        u[0][2][1] + u[2][0][1],
        u[0][2][0] - u[2][0][0],
        u[1][2][1] + u[2][1][1],
        u[1][2][0] - u[2][1][0],
        (u[0][0][1] + u[1][1][1] - 2.0 * u[2][2][1]) * (1.0 / root_three),
    ]


def rotation_of(s):
    h = 0.5 * step_size
    s = [v * h for v in s]
    third = s[7] * (1.0 / root_three)
    d0, d1, d2 = s[2] + third, third - s[2], -2.0 * third
    herm = [
        [(d0, None), (s[0], -s[1]), (s[3], -s[4])],
        [(s[0], s[1]), (d1, None), (s[5], -s[6])],
        [(s[3], s[4]), (s[5], s[6]), (d2, None)],
    ]

    def mul(p, q):
        if p[1] is None and q[1] is None:
            return (p[0] * q[0], jnp.zeros_like(p[0]))
        if p[1] is None:
            return (p[0] * q[0], p[0] * q[1])
        if q[1] is None:
            return (p[0] * q[0], p[1] * q[0])
        return cmul(p, q)

    rows = []
    for i in range(2):
        row = []
        for j in range(3):
            sq = dot_row(herm[i], [herm[k][j] for k in range(3)], mul)
            re, im = -0.5 * sq[0], -0.5 * sq[1]
            if herm[i][j][1] is not None:
                re = re - herm[i][j][1]
            else:
                re = re + 1.0
            row.append((re, im + herm[i][j][0]))
        rows.append(row)

    def unit(row):
        inv = lax.rsqrt(sum(p[0] * p[0] + p[1] * p[1] for p in row))
        return [(p[0] * inv, p[1] * inv) for p in row]

    one = unit(rows[0])
    corr = dot_row(one, rows[1], conj_mul)
    two = unit([csub(rows[1][k], cmul(corr, one[k])) for k in range(3)])
    return [one, two, cross_conj(one, two)]


def block(k):
    return pl.ds(pl.multiple_of(k * LANES, LANES), LANES)


def lane_ids(rows=8):
    return lax.broadcasted_iota(jnp.int32, (rows, LANES), 1)


def rows_of(slices, d, r, c, p):
    return pl.ds((d * 2 + r) * 6 + c * 2 + p, slices, stride=36)


def flat_block(ref, k):
    return ref.at[k].reshape(ref.shape[1] * 36, LANES)


def load_link(ref, slices, d):
    rows = [[tuple(ref[rows_of(slices, d, r, c, p), :] for p in range(2)) for c in range(3)] for r in range(2)]
    return rows + [cross_conj(rows[0], rows[1])]


def site_of(k, extent):
    start = k * LANES
    shifted = lane_ids() + lax.rem(start, extent)
    wraps = sum((shifted >= extent * i).astype(jnp.int32) for i in range(1, (LANES + extent - 1) // extent + 1))
    return shifted - extent * wraps, lax.div(start, extent) + wraps


def at_z(row, z, me, rows, extent):
    first = lax.rem(extent + z + 1 - lax.rem(me * rows, extent), extent)
    hit = row == first
    for i in range(1, -(-rows // extent)):
        hit = hit | (row == first + i * extent)
    return hit


def fetch_block(links, held, sem, k, start=0):
    return pltpu.make_async_copy(links.at[:, :, :, :, :, pl.ds(k * LANES, LANES)], held.at[k - start], sem.at[k])


def split3(x):
    hi = x.astype(bf16)
    lo = (x - hi.astype(f32)).astype(bf16)
    return jnp.concatenate([hi, lo, hi], axis=0)


def transform(table, parts):
    both = jnp.dot(table, split3(jnp.concatenate(parts, axis=1)), preferred_element_type=f32)
    return [both[:, i * LANES : (i + 1) * LANES] for i in range(len(parts))]


def swap(v):
    return pltpu.roll(v, 4, 0)


def flip(place, i, group):
    other = place
    for b in range(group.bit_length() - 1):
        if i >> b & 1:
            other = other + (1 << b) * (1 - 2 * lax.rem(lax.div(place, 1 << b), 2))
    return other


def iota(shape, axis):
    return lax.broadcasted_iota(jnp.int32, shape, axis).astype(f32)


def divide(v, n):
    whole = jnp.floor((v + 0.5) * (1.0 / n))
    return whole, v - n * whole


def send_order(group):
    axes = group.bit_length() - 2
    hops = lambda i: bin(i >> 1).count("1")
    near = sorted((i for i in range(2, group) if hops(i) == 1), key=lambda i: (i & 1, -i))
    far = sorted((i for i in range(2, group) if hops(i) > 1), key=lambda i: (-hops(i), -i))
    order = []
    while near:
        order += far[:1] + near[:axes]
        far, near = far[1:], near[axes:]
    return order + far + [1]


def make_tables(n, planes, wave, tables, zero):
    shape = (n, 3 * n)
    row = iota(shape, 0)
    third, col = divide(iota(shape, 1), n)
    for i, turn in enumerate([row * col, row * (col + (n - 1.0)), col * (row + (n - 1.0))]):
        angle = divide(turn, n)[1] * (2.0 * math.pi / n)
        full = (jnp.cos(angle) + jnp.sin(angle)) * (1.0 / math.sqrt(n))
        high = full.astype(bf16).astype(f32)
        tables[i] = jnp.where(third == 2.0, full - high, high).astype(bf16)
    mode = iota((8, n * n), 1)
    p = jnp.zeros((8, n * n), f32)
    for k in divide(mode, n):
        s = jnp.sin(k * (math.pi / n))
        p = p + 4.0 * s * s
    p = jnp.where(mode == 0.0, 1.0, p)
    root = jnp.sqrt(p + 0.25 * p * p)
    mu = 1.0 / (1.0 + 0.5 * p + root)
    power = lax.integer_pow(mu, planes)
    close = 1.0 / (1.0 - power * power)
    for i, v in enumerate([mu, (0.5 * top_momentum) / root, close, close * power]):
        wave[i] = jnp.where(mode == 0.0, 0.0, v)
    square = (LANES, LANES)
    source, sub = divide(iota(square, 0), 4)
    target, lane = divide(iota(square, 1), 4)
    used = (sub == lane) & (source < planes) & (target < planes)
    for i in range(2):
        d = divide(target - source + (n + i * planes * 1.0), n)[1]
        green = top_momentum * ((n * n - 1.0) / (12.0 * n) - d * (n - d) * (0.5 / n))
        zero[i] = jnp.where(used, green, 0.0)


def link_part(extent, held, smooth, arrive, mend_edges, done, below, rot, halo_send, halo_recv, n):
    nb, slices = held.shape[0], held.shape[1]
    yb = extent * extent // LANES
    unit = nb // UNITS
    q = nb * LANES // extent
    mid = (extent // 2) * extent
    lane = lane_ids()
    me = lax.axis_index("space")
    ahead, behind = lax.rem(me + 1, n), lax.rem(me + n - 1, n)
    def rotate(values, sl):
        g = rotation_of(values)
        for i in range(3):
            for j in range(3):
                for p in range(2):
                    rot[6 * i + 2 * j + p, :, sl] = g[i][j][p]

    def rotate_own(k, carry):
        rotate([smooth[a, :, block(k)] for a in range(8)], block(k))
        return carry

    def halo(i, source, dest, other):
        return pltpu.make_async_remote_copy(
            src_ref=source,
            dst_ref=dest,
            send_sem=halo_send.at[i],
            recv_sem=halo_recv.at[i],
            device_id={"space": other},
            device_id_type=MESH,
        )

    def span(start, size):
        return pl.ds(pl.multiple_of(start * LANES, LANES), size * LANES)

    odd = lax.rem(me, 2)
    pick = yb - odd * (yb - mid // LANES)
    below_copy = halo(0, smooth.at[:, :, span(pick, 1)], below, ahead)
    rims = [
        halo(1 + i, smooth.at[:, :, span(i * unit, unit)], smooth.at[:, :, span(nb + i * unit, unit)], behind)
        for i in range(2)
    ]

    def turn(v):
        lax.fori_loop(0, unit, lambda i, carry: rotate_own(v * unit + i, carry), 0, unroll=3)

    def step(which, k, total):
        sl = block(k)
        before = block(jnp.maximum(k - 1, 0))
        after = block(k + 1)
        wrap = block(jnp.where(k == yb, 0, nb + yb))
        x_at, row = site_of(k, extent)
        edge_x = x_at == extent - 1
        edge_z = at_z(row, extent - 1, me, q, extent)

        def ahead_x(e):
            cur = rot[e, :, sl]
            near = pltpu.roll(jnp.where(lane == 0, rot[e, :, after], cur), LANES - 1, 1)
            far = pltpu.roll(jnp.where(lane >= LANES - extent + 1, rot[e, :, before], cur), extent - 1, 1)
            return jnp.where(edge_x, far, near)

        def ahead_y(e):
            return rot[e, :, block(k + yb)]

        def ahead_z(e):
            cur = rot[e, :, sl]
            near = pltpu.roll(jnp.where(lane < extent, rot[e, :, after], cur), LANES - extent, 1)
            far = pltpu.roll(rot[e, :, wrap], LANES - extent, 1)
            return jnp.where(edge_z, far, near)

        flat_out = flat_block(done, k)
        for d in which:
            forward = (ahead_x, ahead_y, ahead_z)[d]
            u = load_link(flat_block(held, k), slices, d)
            own = [[(rot[6 * i + 2 * j, :, sl], rot[6 * i + 2 * j + 1, :, sl]) for j in range(3)] for i in range(2)]
            left = [
                [dot_row(own[i], [u[k2][j] for k2 in range(3)], cmul) for j in range(3)]
                for i in range(2)
            ]
            made = []
            for j in range(3):
                row3 = [(forward(6 * j + 2 * c), forward(6 * j + 2 * c + 1)) for c in range(3)]
                for i in range(2):
                    v = dot_row(left[i], row3, mul_conj)
                    flat_out[rows_of(slices, d, i, j, 0), :] = v[0]
                    flat_out[rows_of(slices, d, i, j, 1), :] = v[1]
                    if j < 2:
                        made.append(v)
            p00, p10, p01, p11 = made
            minor = csub(cmul(p00, p11), cmul(p01, p10))[0]
            total = total + ((1.0 - p00[0]) + (1.0 - p11[0]) + (1.0 - minor))
        return total

    def links_of(start, stop, dirs, total):
        return lax.fori_loop(start, stop, functools.partial(step, dirs), total)

    arrive(odd)
    arrive(odd + 2)
    mend_edges()
    turn(odd)
    turn(odd + 2)

    @pl.when(odd == 1)
    def _():
        rims[1].start()

    below_copy.start()
    start = odd * unit
    total = links_of(start, start + 1, (1,), jnp.zeros((8, LANES), f32))
    total = links_of(start + 1, start + unit - 1, (0, 1, 2), total)
    total = links_of(start + unit - 1, start + unit, (1,), total)
    total = links_of(2 * unit + 1, 2 * unit + 1 + (1 - odd) * (unit - 2), (0, 2), total)
    arrive(1 - odd)
    turn(1 - odd)

    @pl.when(odd == 1)
    def _():
        rims[0].start()
        for v in (2, 4):
            arrive(jnp.int32(v))
            turn(v)

    below_copy.wait_recv()
    rotate([below[a] for a in range(8)], block(nb + yb))
    total = links_of(0, start + 1, (0, 2), total)
    total = links_of(start + unit - 1, 2 * unit + 1 + odd * (unit - 2), (0, 2), total)

    @pl.when(odd == 0)
    def _():
        for v in (3, 4):
            rims[v - 3].wait_recv()
            turn(v)

    total = links_of((1 - odd) * unit, (2 - odd) * unit, (1,), total)
    total = links_of(2 * unit, nb - 1, (1,), total)
    total = links_of(nb - 1, nb, (0, 1, 2), total)
    below_copy.wait_send()

    @pl.when(odd == 1)
    def _():
        for copy in rims:
            copy.wait_send()

    return total


def gauge_kernel(
    extent, group, scales, links, done, out_theta, out_deficit, *refs
):
    (
        held_links, smooth, below, rot, sum_row, sums, late_send, late_recv, sum_send, sum_recv,
        alg, y_rim, z_below, z_above, mine, fields, load_sem, halo_send, halo_recv,
        in_send_sem, in_recv_sem, in_edge_send, in_edge_recv,
        extra, extra_held, extra_send, extra_recv, tip_send, tip_recv, wave, tables, zero, one, two, modes, ends, far, mode, far_mode, outgo, held, edge_held,
        end_send, end_recv, send_sem, recv_sem, edge_send, edge_recv,
    ) = refs
    devices = 2 * group
    nb, slices = mine.shape[1], alg.shape[2]
    yb = extent * extent // LANES
    half = slices // 2
    unit = nb // UNITS
    q = nb * LANES // extent
    mid = (extent // 2) * extent
    lane = lane_ids()
    me = lax.axis_index("space")
    place = lax.rem(me, group)
    base = me - place
    beyond = group - base
    ahead, behind = lax.rem(me + 1, devices), lax.rem(me + devices - 1, devices)
    in_spans = [(0, 1)] + [(i * unit, (i + 1) * unit) for i in range(1, UNITS)] + [(1, unit)]
    in_loads = [[fetch_block(links, held_links, load_sem, k) for k in range(a, b)] for a, b in in_spans]
    for copy in sum(in_loads, []):
        copy.start()
    barrier = greet([base + flip(place, i, group) for i in range(1, group)] + [beyond + i for i in range(group)])

    first = nb - yb

    def algebra(i):
        start, stop = in_spans[i]

        def step(k, carry):
            flat = flat_block(held_links, k)
            for d in range(3):
                for a, v in enumerate(algebra_of(load_link(flat, slices, d))):
                    alg[d, a, :, block(k)] = v
                    if d == 1 and start >= first:
                        extra[2 * a, k - first] = v[:half]
                        extra[2 * a + 1, k - first] = v[half:]
            return carry

        for copy in in_loads[i]:
            copy.wait()
        lax.fori_loop(start, stop, step, 0)

    def halo(i, source, dest, other):
        return pltpu.make_async_remote_copy(
            src_ref=source,
            dst_ref=dest,
            send_sem=halo_send.at[i],
            recv_sem=halo_recv.at[i],
            device_id={"space": other},
            device_id_type=MESH,
        )

    def span(start, size):
        return pl.ds(pl.multiple_of(start * LANES, LANES), size * LANES)

    rims = [
        halo(i, alg.at[1, :, :, span(first + i * unit, unit)], y_rim.at[:, :, span(i * unit, unit)], ahead)
        for i in range(yb // unit)
    ]
    below_copy = halo(len(rims), alg.at[2, :, :, span(nb - 1, 1)], z_below, ahead)
    odd = lax.rem(me, 2)
    above_copy = halo(len(rims) + 1, alg.at[2, :, :, span(odd * (mid // LANES), 1)], z_above, behind)

    last = lax.div(place + 1, group)
    next_base = base + last * (beyond - base)
    slot = lax.div(lax.rem(place + 1, group), 2)

    def extra_copy(u, i):
        other = flip(place, i, group)
        return pltpu.make_async_remote_copy(
            src_ref=extra.at[other, pl.ds(u * unit, unit)],
            dst_ref=extra_held.at[pl.ds(slot * yb + u * unit, unit)],
            send_sem=extra_send.at[u, i],
            recv_sem=extra_recv.at[u, slot],
            device_id={"space": next_base + other},
            device_id_type=MESH,
        )

    def tip_copy(i):
        other = flip(place, i, group)
        return pltpu.make_async_remote_copy(
            src_ref=extra.at[other, pl.ds(0, 1)],
            dst_ref=extra_held.at[pl.ds(group // 2 * yb, 1)],
            send_sem=tip_send.at[i],
            recv_sem=tip_recv.at[0],
            device_id={"space": base + other},
            device_id_type=MESH,
        )

    def send_rim(u):
        @pl.when(odd == 0)
        def _():
            rims[u].start()

        @pl.when(odd == 1)
        def _():
            for i in send_order(group):
                extra_copy(u, i).start()

        @pl.when(last == 1)
        def _():
            extra_copy(u, 0).start()

    algebra(0)
    algebra(1)
    pl.semaphore_wait(barrier, devices - 1)
    above_copy.start()
    send_rim(0)
    for i in range(1, len(rims)):
        algebra(1 + i)
        if i == len(rims) - 1:
            below_copy.start()
        send_rim(i)

    @pl.when(last == 1)
    def _():
        for i in range(1, group):
            tip_copy(i).start()
        extra_held[group // 2 * yb] = extra[place, 0]

    @pl.when(odd == 0)
    def _():
        y_rim[...] = jnp.zeros_like(y_rim)

    algebra(UNITS)

    @pl.when((odd == 1) & (last == 0))
    def _():
        def keep_extra(k, carry):
            extra_held[slot * yb + k] = extra[place, k]
            return carry

        lax.fori_loop(0, yb, keep_extra, 0)

    def step(k, carry):
        sl = block(k)
        before = block(jnp.maximum(k - 1, 0))
        after = block(jnp.minimum(k + 1, nb - 1))
        x_at, row = site_of(k, extent)
        edge_x = x_at == 0
        edge_z = at_z(row, 0, me, q, extent)
        for a in range(8):
            x, y, z = alg[0, a, :, sl], alg[1, a, :, sl], alg[2, a, :, sl]
            near = pltpu.roll(jnp.where(lane == LANES - 1, alg[0, a, :, before], x), 1, 1)
            far = pltpu.roll(jnp.where(lane < extent - 1, alg[0, a, :, after], x), LANES - extent + 1, 1)
            bx = jnp.where(edge_x, far, near)
            by = jnp.where(
                k < yb,
                y_rim[a, :, block(jnp.minimum(k, yb - 1))],
                alg[1, a, :, block(jnp.maximum(k - yb, 0))],
            )
            prev = jnp.where(k == 0, z_below[a], alg[2, a, :, before])
            near = pltpu.roll(jnp.where(lane >= LANES - extent, prev, z), extent, 1)
            far = pltpu.roll(jnp.where(k == 0, alg[2, a, :, block(yb)], z_above[a]), extent, 1)
            bz = jnp.where(edge_z, far, near)
            b = (bx - x) + (by - y) + (bz - z)
            mine[2 * a, k] = b[:half]
            mine[2 * a + 1, k] = b[half:]
        return carry

    def in_edge_copy(i):
        return pltpu.make_async_remote_copy(
            src_ref=mine.at[i, pl.ds(0, 1)],
            dst_ref=fields.at[pl.ds(group * nb, 1)],
            send_sem=in_edge_send.at[i],
            recv_sem=in_edge_recv.at[0],
            device_id={"space": beyond + i},
            device_id_type=MESH,
        )

    above_copy.wait_recv()
    below_copy.wait_recv()

    @pl.when(odd == 1)
    def _():
        for copy in rims:
            copy.wait_recv()

    def in_copy(u, i):
        other = flip(place, i, group)
        return pltpu.make_async_remote_copy(
            src_ref=mine.at[other, pl.ds(u * unit, unit)],
            dst_ref=fields.at[pl.ds(place * nb + u * unit, unit)],
            send_sem=in_send_sem.at[u, i],
            recv_sem=in_recv_sem.at[u, i],
            device_id={"space": base + other},
            device_id_type=MESH,
        )

    for c, u in enumerate([2 - odd, 2 * odd, 1 - odd]):
        lax.fori_loop(u * unit, (u + 1) * unit, step, 0)
        for i in send_order(group):
            in_copy(u, i).start()
        if c == 1:

            @pl.when(place == 0)
            def _():
                for i in range(group):
                    in_edge_copy(i).start()

    make_tables(extent, extent // 2, wave, tables, zero)

    def keep(k, carry):
        fields[place * nb + k] = mine[place, k]
        return carry

    lax.fori_loop(0, nb, keep, 0)
    for copy in [below_copy, above_copy]:
        copy.wait_send()

    @pl.when(odd == 0)
    def _():
        for copy in rims:
            copy.wait_send()

    @pl.when(odd == 1)
    def _():
        for u in range(len(rims)):
            for i in range(1, group):
                extra_copy(u, i).wait_send()

    @pl.when(last == 1)
    def _():
        for u in range(len(rims)):
            extra_copy(u, 0).wait_send()
        for i in range(1, group):
            tip_copy(i).wait_send()

    in_edge_copy(0).wait_recv()

    @pl.when(last == 0)
    def _():
        tip_copy(1).wait_recv()

    def wait_extra(u, m):
        @pl.when(place != 2 * m - 1)
        def _():
            pltpu.make_async_remote_copy(
                src_ref=extra.at[0, pl.ds(u * unit, unit)],
                dst_ref=extra_held.at[pl.ds(m * yb + u * unit, unit)],
                send_sem=extra_send.at[u, 0],
                recv_sem=extra_recv.at[u, m],
                device_id={"space": beyond},
                device_id_type=MESH,
            ).wait_recv()

    def wait_side(side):
        for i in send_order(group):
            parity = lax.rem(place + i + side, 2)
            in_copy(parity, i).wait_recv()

            @pl.when(parity == 0)
            def _():
                in_copy(jnp.int32(2), i).wait_recv()

        for m in range(group // 2):
            wait_extra(side, m)

    @pl.when(place == 0)
    def _():
        for i in range(group):
            in_edge_copy(i).wait_send()

    n = extent
    planes = group * nb * LANES // (n * n)
    columns = n * n // LANES
    pairs = planes // 2
    lanes = planes * 4
    per = columns // PIECES
    upper = lax.broadcasted_iota(jnp.int32, (8, LANES), 0) >= 4
    x_table, z_table, z_back = (tables.at[i] for i in range(3))
    decay, weight = wave.at[0], wave.at[1]
    close = wave.at[pl.ds(2, 2)]
    own_zero, far_zero = zero.at[0], zero.at[1]
    def rows_at(i):
        return pl.ds(pl.multiple_of(i * n, 8), n)

    def turn_in(c, tip):
        tiles = [fields[y * columns + c] for y in range(planes)]
        for m in range(group // 2):
            y = m * (planes // (group // 2))
            tiles[y] = tiles[y] + extra_held[m * yb + c]
        tiles = tiles + tip
        rest = LANES - 4 * len(tiles)
        full = jnp.concatenate(tiles + [jnp.zeros((rest, LANES), f32)], axis=0)
        one[block(c), :] = full.T
        return full

    def turn_rest(c, total):
        full = turn_in(c, [])
        return total + sum(full[8 * i : 8 * i + 8] * full[8 * i : 8 * i + 8] for i in range(lanes // 8))

    def along_x(i, carry):
        parts = [one[rows_at(2 * i + e), :] for e in range(2)]
        for e, v in enumerate(transform(x_table[...], parts)):
            two[rows_at(2 * i + e), :] = v
        return carry

    theta = jnp.zeros((8, LANES), f32)
    for side in range(2):
        wait_side(side)
        theta = lax.fori_loop(side * unit, (side + 1) * unit, turn_rest, theta, unroll=3)
        if side == 0:
            turn_in(0, [fields[planes * columns] + extra_held[group // 2 * yb]])
            one[0:n, :] = pltpu.roll(one[0:n, :], LANES - 4, 1)
        lax.fori_loop(side * n // 4, (side + 1) * n // 4, along_x, 0, unroll=4)
    for u in range(UNITS):
        for i in range(1, group):
            in_copy(u, i).wait_send()

    def along_z(i, carry):
        parts = [two[pl.ds(2 * i + e, n, stride=n), :] for e in range(2)]
        for e, v in enumerate(transform(z_table[...], parts)):
            one[rows_at(2 * i + e), :] = v
        return carry

    def end_copy(p):
        cols = pl.ds(p * per * LANES, per * LANES)
        return pltpu.make_async_remote_copy(
            src_ref=ends.at[:, cols],
            dst_ref=far.at[:, cols],
            send_sem=end_send.at[p],
            recv_sem=end_recv.at[p],
            device_id={"space": beyond + place},
            device_id_type=MESH,
        )

    mode_copy = pltpu.make_async_remote_copy(
        src_ref=mode,
        dst_ref=far_mode,
        send_sem=end_send.at[PIECES],
        recv_sem=end_recv.at[PIECES],
        device_id={"space": beyond + place},
        device_id_type=MESH,
    )

    def reduce_ends(c, carry):
        sl = block(c)
        modes[:, sl] = one[sl, :].T[:lanes]
        mu = decay[:, sl]
        mu2 = mu * mu
        low = jnp.where(upper, 1.0, mu)
        high = jnp.where(upper, mu, 1.0)
        fwd = modes[0:8, sl]
        bwd = modes[lanes - 8 : lanes, sl]
        for i in range(1, pairs):
            fwd = fwd * mu2 + modes[8 * i : 8 * i + 8, sl]
            bwd = bwd * mu2 + modes[lanes - 8 - 8 * i : lanes - 8 * i, sl]
        ends[:, sl] = jnp.where(upper, high * bwd + low * swap(bwd), low * fwd + high * swap(fwd))
        return carry

    step_z = n // 2 // PIECES
    for p in range(PIECES):
        lax.fori_loop(p * step_z, (p + 1) * step_z, along_z, 0, unroll=4)
        if p == 0:
            mode[...] = one[0:8, :]
        lax.fori_loop(p * per, (p + 1) * per, reduce_ends, 0, unroll=per)
        if p == 0:
            mode_copy.start()
        end_copy(p).start()

    def sweep(c, carry):
        sl = block(c)
        mu = decay[:, sl]
        mu2 = mu * mu
        low = jnp.where(upper, 1.0, mu)
        high = jnp.where(upper, mu, 1.0)
        total = close[0, :, sl] * far[:, sl] + close[1, :, sl] * ends[:, sl]
        turned = swap(total)
        e = jnp.where(upper, turned, total)
        f = jnp.where(upper, total, turned) * mu
        w = weight[:, sl]
        up = mu * high
        down = jnp.where(upper, 0.0, mu)
        rising = []
        for i in range(pairs):
            v = modes[8 * i : 8 * i + 8, sl]
            s = low * v + high * swap(v)
            rising.append(jnp.where(upper, s, v) + up * e)
            e = mu2 * e + s
        done = [None] * pairs
        for i in reversed(range(pairs)):
            v = modes[8 * i : 8 * i + 8, sl]
            t = swap(v)
            done[i] = w * (rising[i] + low * f + down * t)
            f = mu2 * f + mu * (high * v + low * t)
        full = jnp.concatenate(done + [jnp.zeros((LANES - lanes, LANES), f32)], axis=0)
        one[sl, :] = full.T
        return carry

    def back_z(i, carry):
        parts = [one[rows_at(2 * i + e), :] for e in range(2)]
        for e, v in enumerate(transform(z_back[...], parts)):
            two[pl.ds(2 * i + e, n, stride=n), :] = v
        return carry

    for p in range(PIECES):
        end_copy(p).wait_recv()
        if p == 0:
            mode_copy.wait_recv()
        lax.fori_loop(p * per, (p + 1) * per, sweep, 0, unroll=per)
        if p == 0:
            exact = functools.partial(jnp.dot, preferred_element_type=f32, precision=lax.Precision.HIGHEST)
            flat = exact(mode[...], own_zero[...]) + exact(far_mode[...], far_zero[...])
            first = lax.broadcasted_iota(jnp.int32, (8, LANES), 0) == 0
            one[0:8, :] = jnp.where(first, flat, one[0:8, :])
        lax.fori_loop(p * step_z, (p + 1) * step_z, back_z, 0, unroll=4)

    def back_x(i, carry):
        parts = [two[rows_at(2 * i + e), :] for e in range(2)]
        for e, v in enumerate(transform(x_table[...], parts)):
            one[rows_at(2 * i + e), :] = v
        return carry

    def turn_out(c):
        full = one[block(c), :].T
        for y in range(planes):
            outgo[y * columns + c] = full[4 * y : 4 * y + 4]
        return full

    def turn_out_rest(c, carry):
        turn_out(c)
        return carry

    def unit_copy(i, v):
        other = flip(place, i, group)
        wrap = lax.div(v, UNITS) * lax.div(other + 1, group)
        return pltpu.make_async_remote_copy(
            src_ref=outgo.at[pl.ds(other * nb + v * unit - wrap * (planes * columns), unit)],
            dst_ref=held.at[place, pl.ds(v * unit, unit)],
            send_sem=send_sem.at[v, i],
            recv_sem=recv_sem.at[v, i],
            device_id={"space": base + other + wrap * (beyond - base)},
            device_id_type=MESH,
        )

    def edge_copy(i, other):
        return pltpu.make_async_remote_copy(
            src_ref=outgo.at[pl.ds(planes * columns, 1)],
            dst_ref=edge_held.at[place],
            send_sem=edge_send.at[i],
            recv_sem=edge_recv.at[place],
            device_id={"space": other},
            device_id_type=MESH,
        )

    edges = [edge_copy(0, beyond), edge_copy(1, base + group - 1)]

    def each_unit(side, act):
        for i in send_order(group):
            parity = lax.rem(place + i, 2)
            if side == 0:
                act(unit_copy(i, parity))
                act(unit_copy(i, parity + 2))
            else:
                act(unit_copy(i, 1 - parity))

                @pl.when(parity == 1)
                def _():
                    act(unit_copy(i, jnp.int32(2)))
                    act(unit_copy(i, jnp.int32(4)))

        @pl.when(last == 1)
        def _():
            act(unit_copy(0, jnp.int32(3 + side)))

    for side in range(2):
        lax.fori_loop(side * n // 4, (side + 1) * n // 4, back_x, 0, unroll=4)
        if side == 0:
            one[0:n, :] = pltpu.roll(one[0:n, :], 4, 1)
            outgo[planes * columns] = turn_out(0)[lanes : lanes + 4]
        lax.fori_loop(side * unit, (side + 1) * unit, turn_out_rest, 0, unroll=3)
        if side == 0:
            edges[0].start()

            @pl.when(last == 0)
            def _():
                edges[1].start()

        each_unit(side, lambda copy: copy.start())

    def keep(k, carry):
        held[place, k] = outgo[place * nb + k]
        return carry

    lax.fori_loop(0, nb, keep, 0)

    @pl.when((odd == 1) & (last == 0))
    def _():
        lax.fori_loop(nb, nb + yb, keep, 0)

    @pl.when(last == 1)
    def _():
        edge_held[place] = outgo[planes * columns : planes * columns + 1]

    def edge_wait(i):
        pltpu.make_async_remote_copy(
            src_ref=outgo.at[pl.ds(planes * columns, 1)],
            dst_ref=edge_held.at[i],
            send_sem=edge_send.at[0],
            recv_sem=edge_recv.at[i],
            device_id={"space": beyond},
            device_id_type=MESH,
        ).wait_recv()

    def mend(start):
        for a in range(8):
            row = jnp.concatenate([edge_held[2 * a, 0], edge_held[2 * a + 1, 0]], axis=0)
            smooth[a, :, start : start + LANES] = jnp.where(
                lane_ids() < n, row, smooth[a, :, start : start + LANES]
            )

    def gather(k, carry):
        for a in range(8):
            smooth[a, :, block(k)] = jnp.concatenate([held[2 * a, k], held[2 * a + 1, k]], axis=0)
        return carry

    def arrive(v):
        for i in send_order(group):
            unit_copy(i, v).wait_recv()

        @pl.when(last * lax.div(v, UNITS) == 1)
        def _():
            unit_copy(0, v).wait_recv()

        lax.fori_loop(0, unit, lambda i, carry: gather(v * unit + i, carry), 0, unroll=3)

    def mend_edges():
        @pl.when(place == 0)
        def _():
            for i in range(group):
                edge_wait(i)
            mend(0)

        @pl.when(last == 1)
        def _():
            for i in range(group - 1):
                edge_wait(i)
            mend(nb * LANES)

    total = link_part(extent, held_links, smooth, arrive, mend_edges, done, below, rot, late_send, late_recv, devices)
    for p in range(PIECES):
        end_copy(p).wait_send()
    mode_copy.wait_send()
    edges[0].wait_send()

    @pl.when(last == 0)
    def _():
        edges[1].wait_send()

    for side in range(2):
        each_unit(side, lambda copy: copy.wait_send())


    wide_lane = lane_ids(slices)
    t = jnp.sum(jnp.sum(theta, axis=1, keepdims=True), axis=0, keepdims=True)
    d = jnp.sum(total, axis=1, keepdims=True)
    own_row = lax.broadcasted_iota(jnp.int32, (slices, LANES), 0)
    spread = jnp.where(
        wide_lane == own_row, d, jnp.where(wide_lane == slices, jnp.where(own_row == 0, t, 0.0), 0.0)
    )
    sum_row[...] = jnp.sum(spread, axis=0, keepdims=True)
    copies = []
    for i in range(1, devices):
        copy = pltpu.make_async_remote_copy(
            src_ref=sum_row,
            dst_ref=sums.at[i],
            send_sem=sum_send.at[i],
            recv_sem=sum_recv.at[i],
            device_id={"space": lax.rem(me + i, devices)},
            device_id_type=MESH,
        )
        copy.start()
        copies.append(copy)
    for copy in copies:
        copy.wait()
    row = sum_row[...]
    for i in range(1, devices):
        row = row + sums[i]
    out_deficit[...] = row[:, :slices] * scales[1]
    out_theta[...] = row[:, slices : slices + 1] * scales[0]


def place_kernel(blocks, theta, deficit, out, out_theta, out_deficit, small, sem):
    copies = [
        pltpu.make_async_copy(blocks.at[k], out.at[:, :, :, :, :, pl.ds(k * LANES, LANES)], sem.at[k])
        for k in range(blocks.shape[0])
    ]
    copies = [
        pltpu.make_async_copy(theta, out_theta, small.at[0]),
        pltpu.make_async_copy(deficit, out_deficit, small.at[1]),
    ] + copies
    for copy in copies:
        copy.start()
    for copy in copies:
        copy.wait()


def greet(others):
    barrier = pltpu.get_barrier_semaphore()
    for other in others:
        pl.semaphore_signal(barrier, inc=1, device_id={"space": other}, device_id_type=MESH)
    return barrier


ANY = pl.BlockSpec(memory_space=pl.ANY)
HBM = pl.BlockSpec(memory_space=pltpu.HBM)


def call(kernel, number, out_shape, scratch, *args, in_specs=None, out_specs=None, limit=0):
    return pl.pallas_call(
        kernel,
        out_shape=out_shape,
        in_specs=in_specs or [VM] * len(args),
        out_specs=out_specs or jax.tree.map(lambda _: VM, out_shape),
        scratch_shapes=scratch,
        cost_estimate=pl.CostEstimate(flops=COST, bytes_accessed=COST // 1000, transcendentals=0),
        compiler_params=pltpu.CompilerParams(
            collective_id=number, has_side_effects=True, vmem_limit_bytes=limit * 1024
        ),
    )(*args)


def body(links):
    n = EXTENT
    slices, local = links.shape[0], links.shape[-1]
    devices = lax.axis_size("space")
    plane = n * n
    shape = lambda *s: jax.ShapeDtypeStruct(s, f32)
    vm = lambda *s: pltpu.VMEM(s, f32)
    dma = lambda *s: pltpu.SemaphoreType.DMA(s)
    group = devices // 2
    planes = n // 2
    nb = local // LANES
    assert group * 4 == 8 * slices and nb % UNITS == 0 and plane % (nb // UNITS * LANES) == 0
    rims = plane // (nb // UNITS * LANES)
    blocks = (nb, slices, 3, 2, 3, 2, LANES)
    times = lax.axis_size("tm")
    scales = (1.0 / (slices * times * n**3), 1.0 / n**3)
    placed, total, shares = call(
        functools.partial(gauge_kernel, n, group, scales),
        1,
        (shape(*blocks), shape(1, 1), shape(1, slices)),
        [
            vm(*blocks), vm(8, slices, local + plane), vm(8, slices, LANES),
            vm(18, slices, local + plane + LANES), vm(1, LANES), vm(devices, 1, LANES),
            dma(3), dma(3), dma(devices), dma(devices),
            vm(3, 8, slices, local), vm(8, slices, plane), vm(8, slices, LANES), vm(8, slices, LANES),
            vm(group, nb, 4, LANES), vm(group * nb + 1, 4, LANES), dma(nb), dma(rims + 2), dma(rims + 2),
            dma(UNITS, group), dma(UNITS, group), dma(group), dma(1),
            vm(group, plane // LANES, 4, LANES), vm(devices // 4 * (plane // LANES) + 1, 4, LANES),
            dma(rims, group), dma(rims, group // 2), dma(group), dma(1),
            vm(4, 8, plane), pltpu.VMEM((3, n, 3 * n), bf16), vm(2, LANES, LANES),
            vm(plane, LANES), vm(plane, LANES), vm(4 * planes, plane), vm(8, plane), vm(8, plane),
            vm(8, LANES), vm(8, LANES), vm(group * nb + 1, 4, LANES), vm(group, nb + plane // LANES, 4, LANES), vm(group, 1, 4, LANES),
            dma(PIECES + 1), dma(PIECES + 1), dma(UNITS + rims, group), dma(UNITS + rims, group), dma(2), dma(group),
        ],
        links,
        in_specs=[HBM],
        limit=GAUGE_KB,
    )
    new_links, total, shares = pl.pallas_call(
        place_kernel,
        out_shape=(shape(*links.shape), shape(1, 1), shape(1, slices)),
        in_specs=[VM, VM, VM],
        out_specs=(ANY, ANY, ANY),
        scratch_shapes=[dma(2), dma(nb)],
        compiler_params=pltpu.CompilerParams(vmem_limit_bytes=8 * 1024 * 1024),
    )(placed, total, shares)
    total = total.reshape(())
    if times > 1:
        total = lax.psum(total, "tm")
    return (new_links, total, shares.reshape(slices))


def solution(mesh):
    placed = (P("tm", None, None, None, None, "space"),)
    return jax.shard_map(
        body,
        mesh=mesh,
        in_specs=placed,
        out_specs=(P("tm", None, None, None, None, "space"), P(), P("tm")),
        check_vma=False,
    )
```
